32 devices in a mesh: sector: 8 (over y, x, core), block: 4 (over z).
Axes of the slice: x: 2, y: 2, z: 4, core: 2. Of those that a mesh axis runs over, the one named last changes fastest.
Arguments:
- source: float32 [125, 2, 128, 512], P(None, None, 'sector', 'block'), may hold values from -6 to 6
- jacobian: float32 [2, 128, 512], P(None, 'sector', 'block'), may hold values from 0.5 to 2
- stiff_fine: float32 [125, 125], replicated, may hold values from -1 to 2, as said below
- stiff_coarse: float32 [27, 27], replicated, may hold values from -1 to 2, as said below
- restrict_fine: float32 [27, 125], replicated, may hold values from -0.5 to 0.5
- restrict_coarse: float32 [8, 27], replicated, may hold values from -1.25 to 1.25
- mortar_proj: float32 [2, 5, 5], replicated, may hold values from -2.5 to 2.5
- rotor_trace: float32 [4, 25, 128, 512], P(None, None, 'sector', 'block'), may hold values from -6 to 6
- stator_trace: float32 [4, 25, 128, 512], P(None, None, 'sector', 'block'), may hold values from -6 to 6
- offsets: int32 [4], P('block'), may hold values from 0 to 127
Outputs:
- stator_flux: float32 [4, 25, 128, 512], P(None, None, 'sector', 'block')
- rotor_flux: float32 [4, 25, 128, 512], P(None, None, 'sector', 'block')
- fine_pressure: float32 [125, 2, 128, 512], P(None, None, 'sector', 'block')
- coarse_pressure: float32 [27, 2, 128, 512], P(None, None, 'sector', 'block')
- coarsest_residual: float32 [8, 2, 128, 512], P(None, None, 'sector', 'block')
The draws below stay inside these ranges and needn't reach their ends.
Inputs may be any that keep to these rules, and one draw needn't show every extreme that they name: `stiff_fine`: symmetric, positive diagonal. `stiff_coarse`: symmetric, positive diagonal.
All inputs are finite; a program needn't handle non-finite values.
Results may differ from the reference program's by a relative error of at most 0.00016.
Values sent between devices are 32-bit elements; how exact they have to be, the bound alone decides.
No kernel may reach another device: no remote copies, remote signals or barrier semaphores. Data moves between devices by JAX's collectives and lax.ppermute only.
A program may use at most 128 MiB of HBM per device.

```python
import math
import jax
import jax.numpy as jnp
from jax import lax

NP = 5
NPC = 3
COMPS = 4
ER = 2
NU = 3
ES = 16
EB = 128
NODES = 125
CNODES = 27
LNODES = 8
FNODES = 25
NSG = 128
NBG = 512


def stiffness_draw(draw_key, node_total):
    uniform_part = jax.random.uniform(draw_key, (node_total, node_total), jnp.float32, -1.0, 1.0)
    symmetric = 0.5 * (uniform_part + uniform_part.T)
    identity = jnp.eye(node_total, dtype=jnp.float32)
    off_part = symmetric * (1.0 - identity) * (1.2 / node_total)
    row_sums = jnp.sum(jnp.abs(off_part), axis=1)
    return off_part + identity * (1.25 * row_sums + 0.25)


def draw_stiff_fine(key, part):
    return stiffness_draw(jax.random.fold_in(key, 3), NODES)


def draw_stiff_coarse(key, part):
    return stiffness_draw(jax.random.fold_in(key, 5), CNODES)


def draw_offsets(key, part):
    rows_count = NBG // EB
    sectors_count = NSG // ES
    base_row = jax.random.randint(jax.random.fold_in(key, 13), (), 0, rows_count)
    ranks = jnp.mod(jnp.arange(rows_count, dtype=jnp.int32) + base_row, rows_count)
    spread_steps = jnp.mod(sectors_count // 2 - 1 - 3 * (ranks - 1), sectors_count)
    whole_steps = jnp.where(ranks == 0, sectors_count - 1, spread_steps)
    remainder = jax.random.randint(jax.random.fold_in(key, 11), (rows_count,), 0, ES)
    remainder = jnp.where(ranks == 0, ES - 1, remainder)
    return (whole_steps * ES + remainder).astype(jnp.int32)


def shard_levels(rng, shape, pieces, least, largest):
    level, own = 1.0, jax.random.fold_in(rng, 6)
    for dim, shards_of in pieces:
        draws = jnp.exp(jax.random.uniform(jax.random.fold_in(own, dim), (shards_of,), jnp.float32, least / len(pieces), largest / len(pieces)))
        level = level * jnp.repeat(draws, shape[dim] // shards_of).reshape([-1 if axis == dim else 1 for axis in range(len(shape))])
    return level


def bell_draw(rng, extent, scale, most, split=(), kind=jnp.bfloat16):
    entries = scale * jax.random.normal(rng, extent, jnp.float32)
    if split:
        entries = entries * shard_levels(rng, extent, split, -0.22, 0.18)
    return jnp.clip(entries, -most, most).astype(kind)


def setup_inputs(seed: int = 0) -> dict:
    keys = jax.random.split(jax.random.key(seed), 11)
    source = bell_draw(keys[0], (NODES, ER, NSG, NBG), 1.0, 6.0, ((2, 8), (3, 4)), jnp.float32)
    jacobian = jnp.clip(jnp.exp(math.log(2.0) - 1.3862944 * jax.random.uniform(keys[1], (ER, NSG, NBG), jnp.float32) ** shard_levels(keys[1], (ER, NSG, NBG), ((1, 8), (2, 4)), -0.2, 0.2)), 0.5, 2.0)
    stiff_fine = draw_stiff_fine(jax.random.fold_in(keys[10], 71), 0)
    stiff_coarse = draw_stiff_coarse(jax.random.fold_in(keys[10], 71), 0)
    restrict_fine = bell_draw(keys[4], (CNODES, NODES), NODES ** -0.5, 0.5, (), jnp.float32)
    restrict_coarse = bell_draw(keys[5], (LNODES, CNODES), CNODES ** -0.5, 1.25, (), jnp.float32)
    mortar_proj = bell_draw(keys[6], (2, NP, NP), NP ** -0.5, 2.5, (), jnp.float32)
    rotor_trace = bell_draw(keys[7], (COMPS, FNODES, NSG, NBG), 1.0, 6.0, ((2, 8), (3, 4)), jnp.float32)
    stator_trace = bell_draw(keys[8], (COMPS, FNODES, NSG, NBG), 1.0, 6.0, ((2, 8), (3, 4)), jnp.float32)
    offsets = draw_offsets(jax.random.fold_in(keys[10], 71), 0)
    return {"source": source, "jacobian": jacobian, "stiff_fine": stiff_fine, "stiff_coarse": stiff_coarse, "restrict_fine": restrict_fine, "restrict_coarse": restrict_coarse, "mortar_proj": mortar_proj, "rotor_trace": rotor_trace, "stator_trace": stator_trace, "offsets": offsets}


DAMPING = 0.6
PENALTY = 0.5


def project_along(matrix, traces):
    shaped = traces.reshape((traces.shape[0], NP, NP) + traces.shape[2:])
    turned = jnp.einsum("ij,cjbse->cibse", matrix, shaped, precision=lax.Precision.HIGHEST)
    return turned.reshape(traces.shape)


def pick_faces(traces, wanted):
    return jnp.take_along_axis(traces, jnp.broadcast_to(wanted[None, None], traces.shape), axis=2)


def node_diagonal(stiffness, jacobian, points):
    position = jnp.arange(points)
    rim_cells = ((position == 0) | (position == points - 1)).astype(jnp.float32)
    face_count = rim_cells[:, None, None] + rim_cells[None, :, None] + jnp.zeros((1, 1, points), jnp.float32)
    stiff_diag = jnp.diagonal(stiffness).reshape(points, points, points)
    return jacobian[None, None, None] * stiff_diag[:, :, :, None, None, None] + PENALTY * face_count[:, :, :, None, None, None]


def apply_global(pressure, stiffness, jacobian):
    points = pressure.shape[0]
    product = jnp.dot(stiffness, pressure.reshape(points ** 3, -1), precision=lax.Precision.HIGHEST)
    result = jacobian[None, None, None] * product.reshape(pressure.shape)
    below_circ = jnp.roll(pressure[points - 1], 1, axis=3)
    above_circ = jnp.roll(pressure[0], -1, axis=3)
    zeroes = jnp.zeros_like(pressure[:, 0, :, :, :, :1])
    below_axial = jnp.concatenate([zeroes, pressure[:, points - 1, :, :, :, :-1]], axis=4)
    above_axial = jnp.concatenate([pressure[:, 0, :, :, :, 1:], zeroes], axis=4)
    result = result.at[0].add(PENALTY * (pressure[0] - below_circ))
    result = result.at[points - 1].add(PENALTY * (pressure[points - 1] - above_circ))
    result = result.at[:, 0].add(PENALTY * (pressure[:, 0] - below_axial))
    result = result.at[:, points - 1].add(PENALTY * (pressure[:, points - 1] - above_axial))
    return result


def smooth_level(forcing, stiffness, jacobian):
    points = forcing.shape[0]
    diagonal = node_diagonal(stiffness, jacobian, points)
    pressure = DAMPING * forcing / diagonal
    for sweep_index in range(NU - 1):
        pressure = pressure + DAMPING * (forcing - apply_global(pressure, stiffness, jacobian)) / diagonal
    return pressure, forcing - apply_global(pressure, stiffness, jacobian)


def reference(source, jacobian, stiff_fine, stiff_coarse, restrict_fine, restrict_coarse, mortar_proj, rotor_trace, stator_trace, offsets):
    columns = jnp.repeat(offsets, EB).astype(jnp.int32)
    places = jnp.arange(NSG, dtype=jnp.int32)[:, None]
    current = pick_faces(rotor_trace, jnp.mod(places - columns[None, :], NSG).astype(jnp.int32))
    earlier = pick_faces(rotor_trace, jnp.mod(places - columns[None, :] - 1, NSG).astype(jnp.int32))
    projected = project_along(mortar_proj[0], current) + project_along(mortar_proj[1], earlier)
    stator_flux = stator_trace - projected
    forward_faces = pick_faces(stator_flux, jnp.mod(places + columns[None, :], NSG).astype(jnp.int32))
    further = pick_faces(stator_flux, jnp.mod(places + columns[None, :] + 1, NSG).astype(jnp.int32))
    rotor_flux = project_along(mortar_proj[0].T, forward_faces) + project_along(mortar_proj[1].T, further)
    forcing = source.reshape((NP, NP, NP) + source.shape[1:])
    inflow = (stator_flux[0] + stator_flux[3]).reshape((NP, NP) + stator_flux.shape[2:])
    outflow = (rotor_flux[0] + rotor_flux[3]).reshape((NP, NP) + rotor_flux.shape[2:])
    forcing = forcing.at[:, :, 0, 1].add(inflow)
    forcing = forcing.at[:, :, NP - 1, 0].add(-outflow)
    fine_field, fine_left = smooth_level(forcing, stiff_fine, jacobian)
    coarse_forcing = jnp.dot(restrict_fine, fine_left.reshape(NODES, -1), precision=lax.Precision.HIGHEST)
    coarse_forcing = coarse_forcing.reshape((NPC, NPC, NPC) + source.shape[1:])
    coarse_field, coarse_left = smooth_level(coarse_forcing, stiff_coarse, jacobian)
    coarsest = jnp.dot(restrict_coarse, coarse_left.reshape(CNODES, -1), precision=lax.Precision.HIGHEST)
    return (stator_flux, rotor_flux, fine_field.reshape((NODES,) + source.shape[1:]),
            coarse_field.reshape((CNODES,) + source.shape[1:]), coarsest.reshape((LNODES,) + source.shape[1:]))
```

```python
import functools
import numpy as np
import jax
import jax.numpy as jnp
from jax import lax
from jax.experimental import pallas as pl
from jax.experimental.pallas import tpu as pltpu
from jax.sharding import PartitionSpec as P

F32 = jnp.float32
BF16 = jnp.bfloat16
DAMPING = 0.6
PENALTY = 0.5
LANES = 128
NF = 5
NC = 3
LAST = 8
STEP = 4
VMEM_BYTES = 30 * 1024 * 1024


def up(value, unit):
    return (value + unit - 1) // unit * unit


def any_spec():
    return pl.BlockSpec(memory_space=pl.ANY)


def params(**extra):
    return pltpu.CompilerParams(vmem_limit_bytes=VMEM_BYTES, **extra)


def cost(flops, data):
    return pl.CostEstimate(flops=flops, bytes_accessed=data, transcendentals=0)


def parts_of(x):
    high = x.astype(BF16)
    low = (x - high.astype(F32)).astype(BF16)
    return high, low


def stacked(matrix):
    high, low = parts_of(matrix)
    top = jnp.concatenate([high, high], axis=1)
    bottom = jnp.concatenate([low, jnp.zeros_like(low)], axis=1)
    return jnp.concatenate([top, bottom], axis=0)


def times(weights, x):
    rows = weights.shape[0] // 2
    high, low = parts_of(x)
    both = jnp.dot(weights, jnp.concatenate([high, low], axis=0), preferred_element_type=F32)
    return both[:rows] + both[rows:]


def lane_ids(rows):
    return lax.broadcasted_iota(jnp.int32, (rows, LANES), 1)


def half_faces(n):
    rim = np.zeros(n)
    rim[0] = rim[-1] = 1.0
    count = rim[:, None, None] + rim[None, :, None] + np.zeros((1, 1, n))
    column = np.zeros((up(n**3, 16), 1), np.float32)
    column[: n**3, 0] = PENALTY * count.reshape(-1)
    return np.broadcast_to(column, (column.shape[0], LANES)).copy()


def add_halo(n, e_total, span, source_of, r_ref, c1, c2, z1, z2):
    nn = n * n
    odd = lax.rem(lax.axis_index("sector"), 2) == 1
    block = lax.axis_index("block")
    z_odd = lax.rem(block, 2) == 1
    lowest = block == 0
    highest = block == lax.axis_size("block") - 1
    lanes = lane_ids(8)

    def slab(e, carry):
        r_ref[e] = source_of(e)
        for a in range(n):
            first, second = z1[a], z2[a]
            below = jnp.where(z_odd, first, second)
            above = jnp.where(z_odd, second, first)
            below = pltpu.roll(below, lax.rem(LANES - e, LANES), 1)
            above = pltpu.roll(above, LANES - 1 - e, 1)
            below = jnp.where((lanes == 0) & jnp.logical_not(lowest), PENALTY * below, 0.0)
            above = jnp.where((lanes == LANES - 1) & jnp.logical_not(highest), PENALTY * above, 0.0)
            r_ref[e, pl.ds(a * nn, n), :] += below[:n]
            r_ref[e, pl.ds(a * nn + nn - n, n), :] += above[:n]
        return carry

    lax.fori_loop(0, e_total, slab, 0, unroll=4)
    for layer in range(e_total // span):
        first, second = c1[layer], c2[layer]
        r_ref[layer * span, pl.ds(0, nn), :] += PENALTY * jnp.where(odd, first, second)
        r_ref[layer * span + span - 1, pl.ds((n - 1) * nn, nn), :] += PENALTY * jnp.where(odd, second, first)


def correct(n, e_total, span, r_ref, u_ref, u_of, c1, c2, z1, z2):
    nn = n * n
    lanes = lane_ids(8)

    def slab(e, carry):
        lows, highs = carry
        u_ref[e] = u_of(e, r_ref[e])
        new_lows, new_highs = [], []
        for a in range(n):
            low = u_ref[e, pl.ds(a * nn, 8), :]
            high = u_ref[e, pl.ds(a * nn + nn - n, 8), :]
            here = lanes == e
            new_lows.append(jnp.where(here, pltpu.roll(low, e, 1), lows[a]))
            new_highs.append(jnp.where(here, pltpu.roll(high, e + 1, 1), highs[a]))
        return tuple(new_lows), tuple(new_highs)

    blank = tuple(jnp.zeros((8, LANES), F32) for _ in range(n))
    lows, highs = lax.fori_loop(0, e_total, slab, (blank, blank), unroll=4)
    odd = lax.rem(lax.axis_index("sector"), 2) == 1
    z_odd = lax.rem(lax.axis_index("block"), 2) == 1
    for a in range(n):
        z1[a] = jnp.where(z_odd, lows[a], highs[a])
        z2[a] = jnp.where(z_odd, highs[a], lows[a])
    for layer in range(e_total // span):
        low = u_ref[layer * span, pl.ds(0, nn), :]
        high = u_ref[layer * span + span - 1, pl.ds((n - 1) * nn, nn), :]
        c1[layer] = jnp.where(odd, low, high)
        c2[layer] = jnp.where(odd, high, low)


def subtract_operator(n, e_total, span, r_ref, u_ref, weights, jac_ref, count_ref):
    nn = n * n
    group = 4
    lanes = lane_ids(8)

    def some(i, carry):
        first = i * group
        wide = jnp.concatenate([u_ref[first + j] for j in range(group)], axis=1)
        product = times(weights[...], wide)
        for j in range(group):
            e = first + j
            own = product[:, j * LANES : (j + 1) * LANES]
            r_ref[e] = r_ref[e] - jac_ref[pl.ds(e, 1), :] * own - count_ref[...] * u_ref[e]
            s = lax.rem(e, span)
            before = jnp.where(s > 0, PENALTY, 0.0)
            after = jnp.where(s < span - 1, PENALTY, 0.0)
            previous = u_ref[jnp.maximum(e - 1, 0), pl.ds((n - 1) * nn, nn), :]
            following = u_ref[jnp.minimum(e + 1, e_total - 1), pl.ds(0, nn), :]
            r_ref[e, pl.ds(0, nn), :] += before * previous
            r_ref[e, pl.ds((n - 1) * nn, nn), :] += after * following
            for a in range(n):
                low = u_ref[e, pl.ds(a * nn, 8), :]
                high = u_ref[e, pl.ds(a * nn + nn - n, 8), :]
                from_below = jnp.where(lanes > 0, PENALTY * pltpu.roll(high, 1, 1), 0.0)
                from_above = jnp.where(lanes < LANES - 1, PENALTY * pltpu.roll(low, LANES - 1, 1), 0.0)
                r_ref[e, pl.ds(a * nn, n), :] += from_below[:n]
                r_ref[e, pl.ds(a * nn + nn - n, n), :] += from_above[:n]
        return carry

    lax.fori_loop(0, e_total // group, some, 0)


def face_shapes(n, layers):
    circ = jax.ShapeDtypeStruct((layers, n * n, LANES), F32)
    axial = jax.ShapeDtypeStruct((n, 8, LANES), F32)
    return [circ, circ, axial, axial]


def prepare(rotor, stator, mortar, stiff_fine, stiff_coarse, restrict_fine, restrict_coarse):
    rows, span = rotor.shape[0], rotor.shape[1]
    tall, wide = up(rows, 8), up(rows, 16)
    nodes = np.arange(rows)
    comp, a, b = nodes // (NF * NF), nodes // NF % NF, nodes % NF
    same = (comp[:, None] == comp[None]) & (b[:, None] == b[None])
    code = np.full((tall, LANES), -1, np.int32)
    code[:rows, :rows] = np.where(same, a[:, None] * NF + a[None], -1)
    flipped = np.full((tall, LANES), -1, np.int32)
    flipped[:rows, :rows] = np.where(same, a[None] * NF + a[:, None], -1)
    big, small = up(NF**3, 16), up(NC**3, 16)

    def body(
        rotor_ref, stator_ref, mortar_ref, code_ref, flipped_ref, kf_ref, kc_ref, rf_ref, rc_ref,
        rotor_out, stator_out, proj_out, back_out, wf_out, wc_out, rfs_out, rcs_out, df_out, dc_out,
        pad_ref, sem,
    ):
        copies = []
        for f in range(span):
            for source, target in ((rotor_ref, rotor_out), (stator_ref, stator_out)):
                if tall > rows:
                    target[f, pl.ds(rows, tall - rows), :] = jnp.zeros((tall - rows, LANES), F32)
                copies.append(pltpu.make_async_copy(source.at[:, f, :], target.at[f, pl.ds(0, rows), :], sem))
        for c in copies:
            c.start()
        for codes, out in ((code_ref, proj_out), (flipped_ref, back_out)):
            found = codes[...]
            pair = []
            for which in range(2):
                total = jnp.zeros((tall, LANES), F32)
                for i in range(NF):
                    for j in range(NF):
                        total = jnp.where(found == i * NF + j, mortar_ref[which, i, j], total)
                pair.append(total[:, :wide])
            highs, lows = zip(*[parts_of(m) for m in pair])
            out[...] = jnp.concatenate(
                [
                    jnp.concatenate([jnp.concatenate([h, h], axis=1) for h in highs], axis=0),
                    jnp.concatenate([jnp.concatenate([l, jnp.zeros_like(l)], axis=1) for l in lows], axis=0),
                ],
                axis=0,
            )

        def padded(ref, height, width):
            pad_ref[...] = jnp.zeros_like(pad_ref)
            pad_ref[pl.ds(0, ref.shape[0]), pl.ds(0, ref.shape[1])] = ref[...]
            return pad_ref[pl.ds(0, height), :][:, :width]

        for ref, out, diag_out, size in ((kf_ref, wf_out, df_out, big), (kc_ref, wc_out, dc_out, small)):
            matrix = padded(ref, size, size)
            out[...] = stacked(matrix)
            row = lax.broadcasted_iota(jnp.int32, (size, size), 0)
            col = lax.broadcasted_iota(jnp.int32, (size, size), 1)
            diag = jnp.sum(jnp.where(row == col, matrix, 0.0), axis=1, keepdims=True)
            diag = jnp.where(row[:, :1] < ref.shape[0], diag, 1.0)
            diag_out[...] = jnp.broadcast_to(diag, (size, LANES))
        rfs_out[...] = stacked(padded(rf_ref, small, big))
        rcs_out[...] = stacked(padded(rc_ref, 16, small))
        for c in copies:
            c.wait()

    whole = pl.BlockSpec()
    return pl.pallas_call(
        body,
        out_shape=[
            jax.ShapeDtypeStruct((span, tall, LANES), F32),
            jax.ShapeDtypeStruct((span, tall, LANES), F32),
            jax.ShapeDtypeStruct((4 * tall, 2 * wide), BF16),
            jax.ShapeDtypeStruct((4 * tall, 2 * wide), BF16),
            jax.ShapeDtypeStruct((2 * big, 2 * big), BF16),
            jax.ShapeDtypeStruct((2 * small, 2 * small), BF16),
            jax.ShapeDtypeStruct((2 * small, 2 * big), BF16),
            jax.ShapeDtypeStruct((32, 2 * small), BF16),
            jax.ShapeDtypeStruct((big, LANES), F32),
            jax.ShapeDtypeStruct((small, LANES), F32),
        ],
        in_specs=[any_spec(), any_spec(), pl.BlockSpec(memory_space=pltpu.SMEM)] + [whole] * 6,
        scratch_shapes=[pltpu.VMEM((big, LANES), F32), pltpu.SemaphoreType.DMA],
        compiler_params=params(),
        name="prepare",
    )(rotor, stator, mortar, code, flipped, stiff_fine, stiff_coarse, restrict_fine, restrict_coarse)


def fluxes_and_first(
    shift, rotor_win, stator_win, rotor, stator, near1, near2, proj, back, source, jac, weights, diag, layers,
):
    span, tall = rotor.shape[0], rotor.shape[1]
    rows = 4 * NF * NF
    wide = proj.shape[1] // 2
    e_total = jac.shape[0]
    n, nn = NF, NF * NF
    nodes = n**3
    height = weights.shape[0] // 2
    reach = rotor_win.shape[0]
    even_faces = up(span + 1, 2)

    def body(
        shift_ref, rw_ref, sw_ref, r_in, s_in, near1_ref, near2_ref, proj_ref, back_ref, source_ref, jac_ref,
        w_mat, diag_ref, count_ref,
        sflux_out, rflux_out, r_ref, u_ref, w_ref, c1, c2, z1, z2,
        y0, y1, sflux, rflux, jump, in_sem, out_sem,
    ):
        loads = [
            pltpu.make_async_copy(source_ref.at[:, e, :], r_ref.at[e, pl.ds(0, nodes), :], in_sem)
            for e in range(e_total)
        ]
        for c in loads:
            c.start()
        odd = lax.rem(lax.axis_index("sector"), 2) == 1
        inner = shift_ref[0]
        first_rotor = STEP - 1 - inner

        def apply(matrix_ref, slab_of, count):
            fill = jnp.zeros((wide - tall, 2 * LANES), F32)

            def two(i, carry):
                x = jnp.concatenate([slab_of(2 * i), slab_of(jnp.minimum(2 * i + 1, count - 1))], axis=1)
                x = jnp.concatenate([x, fill], axis=0)
                high, low = parts_of(x)
                y = jnp.dot(
                    matrix_ref[...], jnp.concatenate([high, low], axis=0), preferred_element_type=F32
                )
                a = y[:tall] + y[2 * tall : 3 * tall]
                b = y[tall : 2 * tall] + y[3 * tall :]
                for j in range(2):
                    y0[2 * i + j] = a[:, j * LANES : (j + 1) * LANES]
                    y1[2 * i + j] = b[:, j * LANES : (j + 1) * LANES]
                return carry

            lax.fori_loop(0, up(count, 2) // 2, two, 0)

        stores = []

        def send(buffer, out):
            for f in range(span):
                c = pltpu.make_async_copy(buffer.at[f, pl.ds(0, rows), :], out.at[:, f, :], out_sem)
                c.start()
                stores.append(c)

        apply(proj_ref, lambda f: rw_ref[first_rotor + f], span + 1)

        def stator_face(g, carry):
            sflux[g] = s_in[g] - (y0[g + 1] + y1[g])
            return carry

        lax.fori_loop(0, span, stator_face, 0, unroll=4)
        send(sflux, sflux_out)

        def rotor_slab(f):
            inside = r_in[jnp.clip(f - 1, 0, span - 1)]
            before = jnp.where(odd, near1_ref[0], near2_ref[0])
            after = jnp.where(odd, near2_ref[0], near1_ref[0])
            return jnp.where(f == 0, before, jnp.where(f == span + 1, after, inside))

        apply(proj_ref, rotor_slab, span + 2)

        def jump_face(g, carry):
            jump[g] = sw_ref[inner + g] - (y0[g + 1] + y1[g])
            return carry

        lax.fori_loop(0, span + 1, jump_face, 0)
        apply(back_ref, lambda f: jump[f], span + 1)

        def rotor_face(g, carry):
            rflux[g] = y0[g] + y1[g + 1]
            return carry

        lax.fori_loop(0, span, rotor_face, 0, unroll=4)
        send(rflux, rflux_out)

        for c in loads:
            c.wait()

        def force(s, carry):
            if height > nodes:
                for layer in range(layers):
                    r_ref[layer * span + s, pl.ds(nodes, height - nodes), :] = jnp.zeros((height - nodes, LANES), F32)
            inflow = sflux[s, pl.ds(0, nn), :] + sflux[s, pl.ds(3 * nn, nn), :]
            outflow = rflux[s, pl.ds(0, nn), :] + rflux[s, pl.ds(3 * nn, nn), :]
            r_ref[span + s, pl.ds(0, nn, stride=n), :] += inflow
            r_ref[s, pl.ds(n - 1, nn, stride=n), :] += -outflow
            return carry

        lax.fori_loop(0, span, force, 0)

        def u_of(e, r):
            w = DAMPING / (jac_ref[pl.ds(e, 1), :] * diag_ref[...] + count_ref[...])
            w_ref[e] = w
            return r * w

        correct(n, e_total, span, r_ref, u_ref, u_of, c1, c2, z1, z2)
        subtract_operator(n, e_total, span, r_ref, u_ref, w_mat, jac_ref, count_ref)
        for c in stores:
            c.wait()

    whole = pl.BlockSpec()
    field = jax.ShapeDtypeStruct((e_total, height, LANES), F32)
    trace = jax.ShapeDtypeStruct((rows, span, LANES), F32)
    return pl.pallas_call(
        body,
        out_shape=[trace, trace, field, field, field] + face_shapes(n, layers),
        in_specs=[pl.BlockSpec(memory_space=pltpu.SMEM)] + [whole] * 8 + [any_spec()] + [whole] * 4,
        out_specs=[any_spec(), any_spec()] + [whole] * 7,
        scratch_shapes=[
            pltpu.VMEM((even_faces + 2, tall, LANES), F32),
            pltpu.VMEM((even_faces + 2, tall, LANES), F32),
            pltpu.VMEM((span, tall, LANES), F32),
            pltpu.VMEM((span, tall, LANES), F32),
            pltpu.VMEM((span + 1, tall, LANES), F32),
            pltpu.SemaphoreType.DMA,
            pltpu.SemaphoreType.DMA,
        ],
        compiler_params=params(),
        cost_estimate=cost(2 * 10**9, 20 * 10**6),
        name="fluxes_and_first",
    )(
        shift, rotor_win, stator_win, rotor, stator, near1, near2, proj, back, source, jac, weights, diag,
        half_faces(n),
    )


def sweep(n, r, p, w, jac, weights, faces, layers, last):
    e_total, height = r.shape[0], r.shape[1]
    span = e_total // layers
    nodes = n**3

    def body(r_in, p_in, w_in, jac_ref, w_mat, count_ref, h1, h2, g1, g2, p_out, r_ref, c1, c2, z1, z2, u_ref, p_keep, sem):
        p_ref = p_keep if last else p_out
        add_halo(n, e_total, span, lambda e: r_in[e], r_ref, h1, h2, g1, g2)

        def u_of(e, r_here):
            u = r_here * w_in[e]
            p_ref[e] = p_in[e] + u
            return u

        correct(n, e_total, span, r_ref, u_ref, u_of, c1, c2, z1, z2)
        stores = []
        if last:
            for e in range(e_total):
                c = pltpu.make_async_copy(p_ref.at[e, pl.ds(0, nodes), :], p_out.at[:, e, :], sem)
                c.start()
                stores.append(c)
        subtract_operator(n, e_total, span, r_ref, u_ref, w_mat, jac_ref, count_ref)
        for c in stores:
            c.wait()

    whole = pl.BlockSpec()
    field = jax.ShapeDtypeStruct((e_total, height, LANES), F32)
    kept = jax.ShapeDtypeStruct((nodes, e_total, LANES), F32) if last else field
    return pl.pallas_call(
        body,
        out_shape=[kept, field] + face_shapes(n, layers),
        out_specs=[any_spec() if last else whole] + [whole] * 5,
        scratch_shapes=[
            pltpu.VMEM((e_total, height, LANES), F32),
            pltpu.VMEM((e_total, height, LANES) if last else (1, 8, LANES), F32),
            pltpu.SemaphoreType.DMA,
        ],
        compiler_params=params(),
        cost_estimate=cost(10**9 if n == NF else 10**8, 10 * 10**6),
        name="sweep%d%s" % (n, "_last" if last else ""),
    )(r, p, w, jac, weights, half_faces(n), *faces)


def to_coarse(r, faces, restrict, jac, weights, diag, layers):
    e_total = r.shape[0]
    span = e_total // layers
    small = weights.shape[0] // 2
    n = NC
    group = 4

    def body(r_in, h1, h2, g1, g2, rest_ref, jac_ref, w_mat, diag_ref, count_ref, rc_ref, u_ref, w_ref, c1, c2, z1, z2, r_fine):
        add_halo(NF, e_total, span, lambda e: r_in[e], r_fine, h1, h2, g1, g2)

        def some(i, carry):
            first = i * group
            wide = jnp.concatenate([r_fine[first + j] for j in range(group)], axis=1)
            product = times(rest_ref[...], wide)
            for j in range(group):
                rc_ref[first + j] = product[:, j * LANES : (j + 1) * LANES]
            return carry

        lax.fori_loop(0, e_total // group, some, 0)

        def u_of(e, r_here):
            w_here = DAMPING / (jac_ref[pl.ds(e, 1), :] * diag_ref[...] + count_ref[...])
            w_ref[e] = w_here
            return r_here * w_here

        correct(n, e_total, span, rc_ref, u_ref, u_of, c1, c2, z1, z2)
        subtract_operator(n, e_total, span, rc_ref, u_ref, w_mat, jac_ref, count_ref)

    field = jax.ShapeDtypeStruct((e_total, small, LANES), F32)
    return pl.pallas_call(
        body,
        out_shape=[field, field, field] + face_shapes(n, layers),
        scratch_shapes=[pltpu.VMEM(r.shape, F32)],
        compiler_params=params(),
        cost_estimate=cost(5 * 10**8, 5 * 10**6),
        name="to_coarse",
    )(r, *faces, restrict, jac, weights, diag, half_faces(n))


def to_coarsest(r, faces, restrict, layers):
    e_total = r.shape[0]
    span = e_total // layers
    group = 4

    def body(r_in, h1, h2, g1, g2, rest_ref, out_ref, r_done, kept, sem):
        add_halo(NC, e_total, span, lambda e: r_in[e], r_done, h1, h2, g1, g2)

        def some(i, carry):
            first = i * group
            wide = jnp.concatenate([r_done[first + j] for j in range(group)], axis=1)
            product = times(rest_ref[...], wide)
            for j in range(group):
                kept[first + j] = product[:LAST, j * LANES : (j + 1) * LANES]
            return carry

        lax.fori_loop(0, e_total // group, some, 0)
        stores = []
        for e in range(e_total):
            c = pltpu.make_async_copy(kept.at[e], out_ref.at[:, e, :], sem)
            c.start()
            stores.append(c)
        for c in stores:
            c.wait()

    whole = pl.BlockSpec()
    return pl.pallas_call(
        body,
        out_shape=jax.ShapeDtypeStruct((LAST, e_total, LANES), F32),
        in_specs=[whole] * 6,
        out_specs=any_spec(),
        scratch_shapes=[
            pltpu.VMEM(r.shape, F32),
            pltpu.VMEM((e_total, LAST, LANES), F32),
            pltpu.SemaphoreType.DMA,
        ],
        compiler_params=params(),
        cost_estimate=cost(5 * 10**7, 10**6),
        name="to_coarsest",
    )(r, *faces, restrict)


def move(x, axis, by):
    count = lax.axis_size(axis)
    return lax.ppermute(x, axis, [(i, (i + by) % count) for i in range(count)])


def swap(x, axis, odd_first):
    count = lax.axis_size(axis)
    pairs = []
    for i in range(count):
        ahead = (i % 2 == 0) != odd_first
        pairs.append((i, (i + 1) % count if ahead else (i - 1) % count))
    return lax.ppermute(x, axis, pairs)


def exchange(faces):
    c1, c2, z1, z2 = faces
    return (
        swap(c1, "sector", False),
        swap(c2, "sector", True),
        swap(z1, "block", False),
        swap(z2, "block", True),
    )


def windows(rotor, stator, offset):
    span = rotor.shape[0]
    sectors = lax.axis_size("sector")
    buckets = span // STEP
    device, rest = offset // span, offset % span

    def branch(number):
        by, bucket = number // buckets, number % buckets
        many, few = span - STEP * bucket, STEP * (bucket + 1)

        def run(rotor, stator):
            near = move(rotor[:many], "sector", by)
            far = move(rotor[span - few :], "sector", by + 1)
            near_s = move(stator[span - many :], "sector", -by)
            far_s = move(stator[:few], "sector", -by - 1)
            return jnp.concatenate([far, near], axis=0), jnp.concatenate([near_s, far_s], axis=0)

        return run

    choice = device * buckets + rest // STEP
    both = lax.switch(choice, [branch(i) for i in range(sectors * buckets)], rotor, stator)
    return both, (rest % STEP).reshape(1)


def per_device(
    source, jacobian, stiff_fine, stiff_coarse, restrict_fine, restrict_coarse, mortar_proj, rotor_trace,
    stator_trace, offsets,
):
    layers, span, axial = jacobian.shape
    e_total = layers * span
    source_rows = source.reshape(source.shape[0], e_total, axial)
    jac = jacobian.reshape(e_total, axial)
    rotor_rows = rotor_trace.reshape(-1, span, axial)
    stator_rows = stator_trace.reshape(-1, span, axial)
    rotor, stator, proj, back, wf, wc, rfs, rcs, df, dc = prepare(
        rotor_rows, stator_rows, mortar_proj, stiff_fine, stiff_coarse, restrict_fine, restrict_coarse
    )
    odd = lax.axis_index("sector") % 2 == 1
    first, final = rotor[:1], rotor[span - 1 :]
    near1 = swap(jnp.where(odd, first, final), "sector", False)
    near2 = swap(jnp.where(odd, final, first), "sector", True)
    (rotor_win, stator_win), shift = windows(rotor, stator, offsets[0])
    sflux, rflux, r, p, w, *faces = fluxes_and_first(
        shift, rotor_win, stator_win, rotor, stator, near1, near2, proj, back, source_rows, jac, wf, df, layers
    )
    p, r, *faces = sweep(NF, r, p, w, jac, wf, exchange(faces), layers, False)
    fine, r, *faces = sweep(NF, r, p, w, jac, wf, exchange(faces), layers, True)
    r, p, w, *faces = to_coarse(r, exchange(faces), rfs, jac, wc, dc, layers)
    p, r, *faces = sweep(NC, r, p, w, jac, wc, exchange(faces), layers, False)
    coarse, r, *faces = sweep(NC, r, p, w, jac, wc, exchange(faces), layers, True)
    coarsest = to_coarsest(r, exchange(faces), rcs, layers)
    shape = (layers, span, axial)
    return (
        sflux.reshape(stator_trace.shape),
        rflux.reshape(rotor_trace.shape),
        fine.reshape((-1,) + shape),
        coarse.reshape((-1,) + shape),
        coarsest.reshape((-1,) + shape),
    )


def solution(mesh):
    cell = P(None, None, "sector", "block")
    return jax.shard_map(
        per_device,
        mesh=mesh,
        in_specs=(cell, P(None, "sector", "block"), P(), P(), P(), P(), P(), cell, cell, P("block")),
        out_specs=(cell,) * 5,
        check_vma=False,
    )
```

```python
import jax
import jax.numpy as jnp
from jax import lax
from jax.experimental import pallas as pl
from jax.experimental.pallas import tpu as pltpu
from jax.sharding import PartitionSpec as P

F32 = jnp.float32
BF16 = jnp.bfloat16
DAMPING = 0.6
PENALTY = 0.5
LANES = 128
NF = 5
NC = 3
LAST = 8
STEP = 4
VMEM_BYTES = 12 * 1024 * 1024


def up(value, unit):
    return (value + unit - 1) // unit * unit


def any_spec():
    return pl.BlockSpec(memory_space=pl.ANY)


def hbm_spec():
    return pl.BlockSpec(memory_space=pltpu.HBM)


def in_hbm(*arrays):
    return tuple(pltpu.with_memory_space_constraint(x, pltpu.HBM) for x in arrays)


def params(**extra):
    return pltpu.CompilerParams(vmem_limit_bytes=VMEM_BYTES, **extra)


def cost(flops, data):
    return pl.CostEstimate(flops=flops, bytes_accessed=data, transcendentals=0)


def parts_of(x):
    high = x.astype(BF16)
    low = (x - high.astype(F32)).astype(BF16)
    return high, low


def stacked(matrix):
    high, low = parts_of(matrix)
    top = jnp.concatenate([high, high], axis=1)
    bottom = jnp.concatenate([low, jnp.zeros_like(low)], axis=1)
    return jnp.concatenate([top, bottom], axis=0)


def times(weights, x):
    rows = weights.shape[0] // 2
    high, low = parts_of(x)
    both = jnp.dot(weights, jnp.concatenate([high, low], axis=0), preferred_element_type=F32)
    return both[:rows] + both[rows:]


def lane_ids(rows):
    return lax.broadcasted_iota(jnp.int32, (rows, LANES), 1)


def node_rows(shape, axis):
    return lax.broadcasted_iota(jnp.int32, shape, axis)


def digit(index, unit, most):
    found = jnp.zeros_like(index)
    for k in range(1, most + 1):
        found += jnp.where(index >= k * unit, 1, 0)
    return found


def half_faces(n, height):
    row = node_rows((height, LANES), 0)
    a = digit(row, n * n, n)
    b = digit(row - n * n * a, n, n - 1)
    on_a = jnp.where((a == 0) | (a == n - 1), PENALTY, 0.0)
    on_b = jnp.where((b == 0) | (b == n - 1), PENALTY, 0.0)
    return jnp.where(row < n**3, on_a + on_b, 0.0)


def add_halo(n, e_total, span, source_of, r_ref, c1, c2, z1, z2):
    nn = n * n
    odd = lax.rem(lax.axis_index("sector"), 2) == 1
    block = lax.axis_index("block")
    z_odd = lax.rem(block, 2) == 1
    lowest = block == 0
    highest = block == lax.axis_size("block") - 1
    lanes = lane_ids(8)

    def slab(e, carry):
        r_ref[e] = source_of(e)
        for a in range(n):
            first, second = z1[a], z2[a]
            below = jnp.where(z_odd, first, second)
            above = jnp.where(z_odd, second, first)
            below = pltpu.roll(below, lax.rem(LANES - e, LANES), 1)
            above = pltpu.roll(above, LANES - 1 - e, 1)
            below = jnp.where((lanes == 0) & jnp.logical_not(lowest), PENALTY * below, 0.0)
            above = jnp.where((lanes == LANES - 1) & jnp.logical_not(highest), PENALTY * above, 0.0)
            r_ref[e, pl.ds(a * nn, n), :] += below[:n]
            r_ref[e, pl.ds(a * nn + nn - n, n), :] += above[:n]
        return carry

    lax.fori_loop(0, e_total, slab, 0, unroll=4)
    for layer in range(e_total // span):
        first, second = c1[layer], c2[layer]
        r_ref[layer * span, pl.ds(0, nn), :] += PENALTY * jnp.where(odd, first, second)
        r_ref[layer * span + span - 1, pl.ds((n - 1) * nn, nn), :] += PENALTY * jnp.where(odd, second, first)


def correct(n, e_total, span, r_ref, u_ref, u_of, c1, c2, z1, z2):
    nn = n * n
    lanes = lane_ids(8)

    def slab(e, carry):
        lows, highs = carry
        u_ref[e] = u_of(e, r_ref[e])
        new_lows, new_highs = [], []
        for a in range(n):
            low = u_ref[e, pl.ds(a * nn, 8), :]
            high = u_ref[e, pl.ds(a * nn + nn - n, 8), :]
            here = lanes == e
            new_lows.append(jnp.where(here, pltpu.roll(low, e, 1), lows[a]))
            new_highs.append(jnp.where(here, pltpu.roll(high, e + 1, 1), highs[a]))
        return tuple(new_lows), tuple(new_highs)

    blank = tuple(jnp.zeros((8, LANES), F32) for _ in range(n))
    lows, highs = lax.fori_loop(0, e_total, slab, (blank, blank), unroll=4)
    odd = lax.rem(lax.axis_index("sector"), 2) == 1
    z_odd = lax.rem(lax.axis_index("block"), 2) == 1
    for a in range(n):
        z1[a] = jnp.where(z_odd, lows[a], highs[a])
        z2[a] = jnp.where(z_odd, highs[a], lows[a])
    for layer in range(e_total // span):
        low = u_ref[layer * span, pl.ds(0, nn), :]
        high = u_ref[layer * span + span - 1, pl.ds((n - 1) * nn, nn), :]
        c1[layer] = jnp.where(odd, low, high)
        c2[layer] = jnp.where(odd, high, low)


def subtract_operator(n, e_total, span, r_ref, u_ref, weights, jac_ref, count_ref):
    nn = n * n
    group = 4
    lanes = lane_ids(8)

    def some(i, carry):
        first = i * group
        wide = jnp.concatenate([u_ref[first + j] for j in range(group)], axis=1)
        product = times(weights[...], wide)
        for j in range(group):
            e = first + j
            own = product[:, j * LANES : (j + 1) * LANES]
            r_ref[e] = r_ref[e] - jac_ref[pl.ds(e, 1), :] * own - count_ref[...] * u_ref[e]
            s = lax.rem(e, span)
            before = jnp.where(s > 0, PENALTY, 0.0)
            after = jnp.where(s < span - 1, PENALTY, 0.0)
            previous = u_ref[jnp.maximum(e - 1, 0), pl.ds((n - 1) * nn, nn), :]
            following = u_ref[jnp.minimum(e + 1, e_total - 1), pl.ds(0, nn), :]
            r_ref[e, pl.ds(0, nn), :] += before * previous
            r_ref[e, pl.ds((n - 1) * nn, nn), :] += after * following
            for a in range(n):
                low = u_ref[e, pl.ds(a * nn, 8), :]
                high = u_ref[e, pl.ds(a * nn + nn - n, 8), :]
                from_below = jnp.where(lanes > 0, PENALTY * pltpu.roll(high, 1, 1), 0.0)
                from_above = jnp.where(lanes < LANES - 1, PENALTY * pltpu.roll(low, LANES - 1, 1), 0.0)
                r_ref[e, pl.ds(a * nn, n), :] += from_below[:n]
                r_ref[e, pl.ds(a * nn + nn - n, n), :] += from_above[:n]
        return carry

    lax.fori_loop(0, e_total // group, some, 0)


def face_shapes(n, layers):
    circ = jax.ShapeDtypeStruct((layers, n * n, LANES), F32)
    axial = jax.ShapeDtypeStruct((n, 8, LANES), F32)
    return [circ, circ, axial, axial]


def prepare(rotor, stator, mortar, stiff_fine, stiff_coarse, restrict_fine, restrict_coarse):
    rows, span = rotor.shape[0], rotor.shape[1]
    tall, wide = up(rows, 8), up(rows, 16)
    big, small = up(NF**3, 16), up(NC**3, 16)
    smalls = (mortar, stiff_fine, stiff_coarse, restrict_fine, restrict_coarse)

    def body(
        rotor_ref, stator_ref, mortar_in, kf_in, kc_in, rf_in, rc_in,
        rotor_out, stator_out, proj_out, back_out, wf_out, wc_out, rfs_out, rcs_out, df_out, dc_out,
        mortar_ref, kf_ref, kc_ref, rf_ref, rc_ref, pad_ref, sem, small_sem,
    ):
        copies = []
        for f in range(span):
            for source, target in ((rotor_ref, rotor_out), (stator_ref, stator_out)):
                if tall > rows:
                    target[f, pl.ds(rows, tall - rows), :] = jnp.zeros((tall - rows, LANES), F32)
                copies.append(pltpu.make_async_copy(source.at[:, f, :], target.at[f, pl.ds(0, rows), :], sem))
        little = [
            pltpu.make_async_copy(source, target, small_sem)
            for source, target in (
                (mortar_in, mortar_ref), (kf_in, kf_ref), (kc_in, kc_ref), (rf_in, rf_ref), (rc_in, rc_ref)
            )
        ]
        for c in little + copies:
            c.start()
        row, col = node_rows((tall, LANES), 0), node_rows((tall, LANES), 1)
        comp_r, comp_c = digit(row, NF * NF, 4), digit(col, NF * NF, 5)
        rest_r, rest_c = row - NF * NF * comp_r, col - NF * NF * comp_c
        a_r, a_c = digit(rest_r, NF, NF - 1), digit(rest_c, NF, NF - 1)
        same = (comp_r == comp_c) & (rest_r - NF * a_r == rest_c - NF * a_c) & (row < rows) & (col < rows)
        ahead = jnp.where(same, a_r * NF + a_c, -1)
        flipped = jnp.where(same, a_c * NF + a_r, -1)
        for c in little:
            c.wait()
        for found, out in ((ahead, proj_out), (flipped, back_out)):
            pair = []
            for which in range(2):
                total = jnp.zeros((tall, LANES), F32)
                matrix = mortar_ref[which]
                for i in range(NF):
                    for j in range(NF):
                        total = jnp.where(found == i * NF + j, matrix[i : i + 1, j : j + 1], total)
                pair.append(total[:, :wide])
            highs, lows = zip(*[parts_of(m) for m in pair])
            out[...] = jnp.concatenate(
                [
                    jnp.concatenate([jnp.concatenate([h, h], axis=1) for h in highs], axis=0),
                    jnp.concatenate([jnp.concatenate([l, jnp.zeros_like(l)], axis=1) for l in lows], axis=0),
                ],
                axis=0,
            )

        def padded(ref, height, width):
            pad_ref[...] = jnp.zeros_like(pad_ref)
            pad_ref[pl.ds(0, ref.shape[0]), pl.ds(0, ref.shape[1])] = ref[...]
            return pad_ref[pl.ds(0, height), :][:, :width]

        for ref, out, diag_out, size in ((kf_ref, wf_out, df_out, big), (kc_ref, wc_out, dc_out, small)):
            matrix = padded(ref, size, size)
            out[...] = stacked(matrix)
            row = lax.broadcasted_iota(jnp.int32, (size, size), 0)
            col = lax.broadcasted_iota(jnp.int32, (size, size), 1)
            diag = jnp.sum(jnp.where(row == col, matrix, 0.0), axis=1, keepdims=True)
            diag = jnp.where(row[:, :1] < ref.shape[0], diag, 1.0)
            diag_out[...] = jnp.broadcast_to(diag, (size, LANES))
        rfs_out[...] = stacked(padded(rf_ref, small, big))
        rcs_out[...] = stacked(padded(rc_ref, 16, small))
        for c in copies:
            c.wait()

    return pl.pallas_call(
        body,
        out_shape=[
            jax.ShapeDtypeStruct((span, tall, LANES), F32),
            jax.ShapeDtypeStruct((span, tall, LANES), F32),
            jax.ShapeDtypeStruct((4 * tall, 2 * wide), BF16),
            jax.ShapeDtypeStruct((4 * tall, 2 * wide), BF16),
            jax.ShapeDtypeStruct((2 * big, 2 * big), BF16),
            jax.ShapeDtypeStruct((2 * small, 2 * small), BF16),
            jax.ShapeDtypeStruct((2 * small, 2 * big), BF16),
            jax.ShapeDtypeStruct((32, 2 * small), BF16),
            jax.ShapeDtypeStruct((big, LANES), F32),
            jax.ShapeDtypeStruct((small, LANES), F32),
        ],
        in_specs=[hbm_spec()] * 7,
        scratch_shapes=[pltpu.VMEM(m.shape, F32) for m in smalls]
        + [pltpu.VMEM((big, LANES), F32), pltpu.SemaphoreType.DMA, pltpu.SemaphoreType.DMA],
        compiler_params=params(),
        name="prepare",
    )(*in_hbm(rotor, stator, *smalls))


def apply_faces(matrix_ref, slab_of, count, tall, wide, y0, y1):
    group = 4
    fill = jnp.zeros((wide - tall, group * LANES), F32)

    def some(i, carry):
        first = group * i
        x = jnp.concatenate([slab_of(jnp.minimum(first + j, count - 1)) for j in range(group)], axis=1)
        if wide > tall:
            x = jnp.concatenate([x, fill], axis=0)
        high, low = parts_of(x)
        y = jnp.dot(matrix_ref[...], jnp.concatenate([high, low], axis=0), preferred_element_type=F32)
        a = y[:tall] + y[2 * tall : 3 * tall]
        b = y[tall : 2 * tall] + y[3 * tall :]
        for j in range(group):
            y0[first + j] = a[:, j * LANES : (j + 1) * LANES]
            y1[first + j] = b[:, j * LANES : (j + 1) * LANES]
        return carry

    lax.fori_loop(0, up(count, group) // group, some, 0)


def own_part(rotor, near1, near2, proj, source, jac, diag):
    span, tall = rotor.shape[0], rotor.shape[1]
    wide = proj.shape[1] // 2
    e_total, height = jac.shape[0], diag.shape[0]
    nodes = NF**3

    def body(r_in, near1_ref, near2_ref, proj_ref, source_ref, jac_ref, diag_ref, kept, w_ref, r_ref, y0, y1, sem):
        loads = [
            pltpu.make_async_copy(source_ref.at[:, e, :], r_ref.at[e, pl.ds(0, nodes), :], sem)
            for e in range(e_total)
        ]
        for c in loads:
            c.start()
        odd = lax.rem(lax.axis_index("sector"), 2) == 1
        before = jnp.where(odd, near1_ref[0], near2_ref[0])
        after = jnp.where(odd, near2_ref[0], near1_ref[0])

        def rotor_slab(f):
            inside = r_in[jnp.clip(f - 1, 0, span - 1)]
            return jnp.where(f == 0, before, jnp.where(f == span + 1, after, inside))

        apply_faces(proj_ref, rotor_slab, span + 2, tall, wide, y0, y1)

        def face(g, carry):
            kept[g] = y0[g + 1] + y1[g]
            return carry

        lax.fori_loop(0, span + 1, face, 0)
        count = half_faces(NF, height)

        def weight(e, carry):
            w_ref[e] = DAMPING / (jac_ref[pl.ds(e, 1), :] * diag_ref[...] + count)
            r_ref[e, pl.ds(nodes, height - nodes), :] = jnp.zeros((height - nodes, LANES), F32)
            return carry

        lax.fori_loop(0, e_total, weight, 0)
        for c in loads:
            c.wait()

    whole = pl.BlockSpec()
    field = jax.ShapeDtypeStruct((e_total, height, LANES), F32)
    return pl.pallas_call(
        body,
        out_shape=[jax.ShapeDtypeStruct((span + 1, tall, LANES), F32), field, field],
        in_specs=[whole] * 4 + [hbm_spec()] + [whole] * 2,
        scratch_shapes=[pltpu.VMEM((up(span + 2, 4), tall, LANES), F32)] * 2 + [pltpu.SemaphoreType.DMA],
        compiler_params=params(),
        cost_estimate=cost(2 * 10**9, 10 * 10**6),
        name="own_part",
    )(rotor, near1, near2, proj, *in_hbm(source), jac, diag)


def fluxes_and_first(shift, rotor_win, stator_win, stator, kept, proj, back, r_source, w, jac, weights, layers):
    span, tall = stator.shape[0], stator.shape[1]
    rows = 4 * NF * NF
    wide = proj.shape[1] // 2
    e_total = jac.shape[0]
    n, nn = NF, NF * NF
    height = weights.shape[0] // 2

    def body(
        shift_ref, rw_ref, sw_ref, s_in, kept_ref, proj_ref, back_ref, source_ref, w_ref, jac_ref, w_mat,
        sflux_out, rflux_out, r_ref, u_ref, c1, c2, z1, z2,
        y0, y1, sflux, rflux, jump, count_ref, out_sem,
    ):
        inner = shift_ref[0]
        first_rotor = STEP - 1 - inner
        count_ref[...] = half_faces(n, height)
        stores = []

        def send(buffer, out):
            for f in range(span):
                c = pltpu.make_async_copy(buffer.at[f, pl.ds(0, rows), :], out.at[:, f, :], out_sem)
                c.start()
                stores.append(c)

        apply_faces(proj_ref, lambda f: rw_ref[first_rotor + f], span + 1, tall, wide, y0, y1)

        def stator_face(g, carry):
            sflux[g] = s_in[g] - (y0[g + 1] + y1[g])
            return carry

        lax.fori_loop(0, span, stator_face, 0, unroll=2)
        send(sflux, sflux_out)

        def jump_face(g, carry):
            jump[g] = sw_ref[inner + g] - kept_ref[g]
            return carry

        lax.fori_loop(0, span + 1, jump_face, 0)
        apply_faces(back_ref, lambda f: jump[f], span + 1, tall, wide, y0, y1)

        def rotor_face(g, carry):
            rflux[g] = y0[g] + y1[g + 1]
            return carry

        lax.fori_loop(0, span, rotor_face, 0, unroll=2)
        send(rflux, rflux_out)

        def force(s, carry):
            for layer in range(layers):
                r_ref[layer * span + s] = source_ref[layer * span + s]
            inflow = sflux[s, pl.ds(0, nn), :] + sflux[s, pl.ds(3 * nn, nn), :]
            outflow = rflux[s, pl.ds(0, nn), :] + rflux[s, pl.ds(3 * nn, nn), :]
            r_ref[span + s, pl.ds(0, nn, stride=n), :] += inflow
            r_ref[s, pl.ds(n - 1, nn, stride=n), :] += -outflow
            return carry

        lax.fori_loop(0, span, force, 0, unroll=2)
        correct(n, e_total, span, r_ref, u_ref, lambda e, r: r * w_ref[e], c1, c2, z1, z2)
        subtract_operator(n, e_total, span, r_ref, u_ref, w_mat, jac_ref, count_ref)
        for c in stores:
            c.wait()

    whole = pl.BlockSpec()
    field = jax.ShapeDtypeStruct((e_total, height, LANES), F32)
    trace = jax.ShapeDtypeStruct((rows, span, LANES), F32)
    slabs = pltpu.VMEM((up(span + 1, 4), tall, LANES), F32)
    return pl.pallas_call(
        body,
        out_shape=[trace, trace, field, field] + face_shapes(n, layers),
        in_specs=[pl.BlockSpec(memory_space=pltpu.SMEM)] + [whole] * 10,
        out_specs=[any_spec(), any_spec()] + [whole] * 6,
        scratch_shapes=[
            slabs,
            slabs,
            pltpu.VMEM((span, tall, LANES), F32),
            pltpu.VMEM((span, tall, LANES), F32),
            pltpu.VMEM((span + 1, tall, LANES), F32),
            pltpu.VMEM((height, LANES), F32),
            pltpu.SemaphoreType.DMA,
        ],
        compiler_params=params(),
        cost_estimate=cost(2 * 10**9, 20 * 10**6),
        name="fluxes_and_first",
    )(shift, rotor_win, stator_win, stator, kept, proj, back, r_source, w, jac, weights)


def sweep(n, r, p, w, jac, weights, faces, layers, last):
    e_total, height = r.shape[0], r.shape[1]
    span = e_total // layers
    nodes = n**3

    def body(r_in, p_in, w_in, jac_ref, w_mat, h1, h2, g1, g2, p_out, r_ref, c1, c2, z1, z2, u_ref, p_keep, count_ref, sem):
        count_ref[...] = half_faces(n, height)
        p_ref = p_keep if last else p_out
        add_halo(n, e_total, span, lambda e: r_in[e], r_ref, h1, h2, g1, g2)

        def u_of(e, r_here):
            u = r_here * w_in[e]
            p_ref[e] = p_in[e] + u
            return u

        correct(n, e_total, span, r_ref, u_ref, u_of, c1, c2, z1, z2)
        stores = []
        if last:
            for e in range(e_total):
                c = pltpu.make_async_copy(p_ref.at[e, pl.ds(0, nodes), :], p_out.at[:, e, :], sem)
                c.start()
                stores.append(c)
        subtract_operator(n, e_total, span, r_ref, u_ref, w_mat, jac_ref, count_ref)
        for c in stores:
            c.wait()

    whole = pl.BlockSpec()
    field = jax.ShapeDtypeStruct((e_total, height, LANES), F32)
    kept = jax.ShapeDtypeStruct((nodes, e_total, LANES), F32) if last else field
    return pl.pallas_call(
        body,
        out_shape=[kept, field] + face_shapes(n, layers),
        out_specs=[any_spec() if last else whole] + [whole] * 5,
        scratch_shapes=[
            pltpu.VMEM((e_total, height, LANES), F32),
            pltpu.VMEM((e_total, height, LANES) if last else (1, 8, LANES), F32),
            pltpu.VMEM((height, LANES), F32),
            pltpu.SemaphoreType.DMA,
        ],
        compiler_params=params(),
        cost_estimate=cost(10**9 if n == NF else 10**8, 10 * 10**6),
        name="sweep%d%s" % (n, "_last" if last else ""),
    )(r, p, w, jac, weights, *faces)


def to_coarse(r, faces, restrict, jac, weights, diag, layers):
    e_total = r.shape[0]
    span = e_total // layers
    small = weights.shape[0] // 2
    n = NC
    group = 4

    def body(r_in, h1, h2, g1, g2, rest_ref, jac_ref, w_mat, diag_ref, rc_ref, u_ref, w_ref, c1, c2, z1, z2, r_fine, count_ref):
        count_ref[...] = half_faces(n, small)
        add_halo(NF, e_total, span, lambda e: r_in[e], r_fine, h1, h2, g1, g2)

        def some(i, carry):
            first = i * group
            wide = jnp.concatenate([r_fine[first + j] for j in range(group)], axis=1)
            product = times(rest_ref[...], wide)
            for j in range(group):
                rc_ref[first + j] = product[:, j * LANES : (j + 1) * LANES]
            return carry

        lax.fori_loop(0, e_total // group, some, 0)

        def u_of(e, r_here):
            w_here = DAMPING / (jac_ref[pl.ds(e, 1), :] * diag_ref[...] + count_ref[...])
            w_ref[e] = w_here
            return r_here * w_here

        correct(n, e_total, span, rc_ref, u_ref, u_of, c1, c2, z1, z2)
        subtract_operator(n, e_total, span, rc_ref, u_ref, w_mat, jac_ref, count_ref)

    field = jax.ShapeDtypeStruct((e_total, small, LANES), F32)
    return pl.pallas_call(
        body,
        out_shape=[field, field, field] + face_shapes(n, layers),
        scratch_shapes=[pltpu.VMEM(r.shape, F32), pltpu.VMEM((small, LANES), F32)],
        compiler_params=params(),
        cost_estimate=cost(5 * 10**8, 5 * 10**6),
        name="to_coarse",
    )(r, *faces, restrict, jac, weights, diag)


def to_coarsest(r, faces, restrict, layers):
    e_total = r.shape[0]
    span = e_total // layers
    group = 4

    def body(r_in, h1, h2, g1, g2, rest_ref, out_ref, r_done, kept, sem):
        add_halo(NC, e_total, span, lambda e: r_in[e], r_done, h1, h2, g1, g2)

        def some(i, carry):
            first = i * group
            wide = jnp.concatenate([r_done[first + j] for j in range(group)], axis=1)
            product = times(rest_ref[...], wide)
            for j in range(group):
                kept[first + j] = product[:LAST, j * LANES : (j + 1) * LANES]
            return carry

        lax.fori_loop(0, e_total // group, some, 0)
        stores = []
        for e in range(e_total):
            c = pltpu.make_async_copy(kept.at[e], out_ref.at[:, e, :], sem)
            c.start()
            stores.append(c)
        for c in stores:
            c.wait()

    whole = pl.BlockSpec()
    return pl.pallas_call(
        body,
        out_shape=jax.ShapeDtypeStruct((LAST, e_total, LANES), F32),
        in_specs=[whole] * 6,
        out_specs=any_spec(),
        scratch_shapes=[
            pltpu.VMEM(r.shape, F32),
            pltpu.VMEM((e_total, LAST, LANES), F32),
            pltpu.SemaphoreType.DMA,
        ],
        compiler_params=params(),
        cost_estimate=cost(5 * 10**7, 10**6),
        name="to_coarsest",
    )(r, *faces, restrict)


def move(x, axis, by):
    count = lax.axis_size(axis)
    return lax.ppermute(x, axis, [(i, (i + by) % count) for i in range(count)])


def swap(x, axis, odd_first):
    count = lax.axis_size(axis)
    pairs = []
    for i in range(count):
        ahead = (i % 2 == 0) != odd_first
        pairs.append((i, (i + 1) % count if ahead else (i - 1) % count))
    return lax.ppermute(x, axis, pairs)


def swap_inner(x, axis, other):
    count, beside = lax.axis_size(axis), lax.axis_size(other)
    pairs = []
    for j in range(beside):
        for i in range(count):
            to = i + 1 if i % 2 else i - 1
            target = (j, to) if 0 <= to < count else (j ^ 1, i)
            pairs.append((j * count + i, target[0] * count + target[1]))
    return lax.ppermute(x, (other, axis), pairs)


def exchange(faces):
    c1, c2, z1, z2 = faces
    return (
        swap(c1, "sector", False),
        swap(c2, "sector", True),
        swap(z1, "block", False),
        swap_inner(z2, "block", "sector"),
    )


def windows(rotor, stator, offset, own):
    span = rotor.shape[0]
    sectors = lax.axis_size("sector")
    buckets = span // STEP
    device, rest = offset // span, offset % span

    def branch(number):
        by, bucket = number // buckets, number % buckets
        many, few = span - STEP * bucket, STEP * (bucket + 1)

        def run(rotor, stator, own):
            near = move(rotor[:many], "sector", by)
            far = move(rotor[span - few :], "sector", by + 1)
            near_s = move(stator[span - many :], "sector", -by)
            far_s = move(stator[:few], "sector", -by - 1)
            wins = jnp.concatenate([far, near], axis=0), jnp.concatenate([near_s, far_s], axis=0)
            return wins + tuple(own_part(rotor, *own))

        return run

    choice = device * buckets + rest // STEP
    found = lax.switch(choice, [branch(i) for i in range(sectors * buckets)], rotor, stator, own)
    return found, (rest % STEP).reshape(1)


def per_device(
    source, jacobian, stiff_fine, stiff_coarse, restrict_fine, restrict_coarse, mortar_proj, rotor_trace,
    stator_trace, offsets,
):
    layers, span, axial = jacobian.shape
    e_total = layers * span
    source_rows = source.reshape(source.shape[0], e_total, axial)
    jac = jacobian.reshape(e_total, axial)
    rotor_rows = rotor_trace.reshape(-1, span, axial)
    stator_rows = stator_trace.reshape(-1, span, axial)
    rotor, stator, proj, back, wf, wc, rfs, rcs, df, dc = prepare(
        rotor_rows, stator_rows, mortar_proj, stiff_fine, stiff_coarse, restrict_fine, restrict_coarse
    )
    odd = lax.axis_index("sector") % 2 == 1
    first, final = rotor[:1], rotor[span - 1 :]
    near1 = swap(jnp.where(odd, first, final), "sector", False)
    near2 = swap(jnp.where(odd, final, first), "sector", True)
    own = (near1, near2, proj, source_rows, jac, df)
    (rotor_win, stator_win, kept, w, r), shift = windows(rotor, stator, offsets[0], own)
    sflux, rflux, r, p, *faces = fluxes_and_first(
        shift, rotor_win, stator_win, stator, kept, proj, back, r, w, jac, wf, layers
    )
    p, r, *faces = sweep(NF, r, p, w, jac, wf, exchange(faces), layers, False)
    fine, r, *faces = sweep(NF, r, p, w, jac, wf, exchange(faces), layers, True)
    r, p, w, *faces = to_coarse(r, exchange(faces), rfs, jac, wc, dc, layers)
    p, r, *faces = sweep(NC, r, p, w, jac, wc, exchange(faces), layers, False)
    coarse, r, *faces = sweep(NC, r, p, w, jac, wc, exchange(faces), layers, True)
    coarsest = to_coarsest(r, exchange(faces), rcs, layers)
    shape = (layers, span, axial)
    return (
        sflux.reshape(stator_trace.shape),
        rflux.reshape(rotor_trace.shape),
        fine.reshape((-1,) + shape),
        coarse.reshape((-1,) + shape),
        coarsest.reshape((-1,) + shape),
    )


def solution(mesh):
    cell = P(None, None, "sector", "block")
    return jax.shard_map(
        per_device,
        mesh=mesh,
        in_specs=(cell, P(None, "sector", "block"), P(), P(), P(), P(), P(), cell, cell, P("block")),
        out_specs=(cell,) * 5,
        check_vma=False,
    )
```

```python
import jax
import jax.numpy as jnp
from jax import lax
from jax.experimental import pallas as pl
from jax.experimental.pallas import tpu as pltpu
from jax.sharding import PartitionSpec as P


F32 = jnp.float32
BF16 = jnp.bfloat16
DAMPING = 0.6
PENALTY = 0.5
LANES = 128
NF = 5
NC = 3
LAST = 8
STEP = 4
HALO_UNROLL = 32
GROUP = {NF: 4, NC: 16}
GROUP_UNROLL = {NF: 4, NC: 1}
VMEM_BYTES = 12 * 1024 * 1024


def up(value, unit):
    return (value + unit - 1) // unit * unit


def any_spec():
    return pl.BlockSpec(memory_space=pl.ANY)


def hbm_spec():
    return pl.BlockSpec(memory_space=pltpu.HBM)


def in_hbm(*arrays):
    return tuple(pltpu.with_memory_space_constraint(x, pltpu.HBM) for x in arrays)


def params(**extra):
    return pltpu.CompilerParams(vmem_limit_bytes=VMEM_BYTES, **extra)


def cost(flops, data):
    return pl.CostEstimate(flops=flops, bytes_accessed=data, transcendentals=0)


def parts_of(x):
    high = x.astype(BF16)
    low = (x - high.astype(F32)).astype(BF16)
    return high, low


def stacked(matrix):
    high, low = parts_of(matrix)
    top = jnp.concatenate([high, high], axis=1)
    bottom = jnp.concatenate([low, jnp.zeros_like(low)], axis=1)
    return jnp.concatenate([top, bottom], axis=0)


def times(weights, x):
    rows = weights.shape[0] // 2
    high, low = parts_of(x)
    both = jnp.dot(weights, jnp.concatenate([high, low], axis=0), preferred_element_type=F32)
    return both[:rows] + both[rows:]


def lane_ids(rows):
    return lax.broadcasted_iota(jnp.int32, (rows, LANES), 1)


def node_rows(shape, axis):
    return lax.broadcasted_iota(jnp.int32, shape, axis)


def digit(index, unit, most):
    found = jnp.zeros_like(index)
    for k in range(1, most + 1):
        found += jnp.where(index >= k * unit, 1, 0)
    return found


def half_faces(n, height):
    row = node_rows((height, LANES), 0)
    a = digit(row, n * n, n)
    b = digit(row - n * n * a, n, n - 1)
    on_a = jnp.where((a == 0) | (a == n - 1), PENALTY, 0.0)
    on_b = jnp.where((b == 0) | (b == n - 1), PENALTY, 0.0)
    return jnp.where(row < n**3, on_a + on_b, 0.0)


def add_halo(n, e_total, span, source_of, r_ref, c1, c2, z1, z2):
    nn = n * n
    odd = lax.rem(lax.axis_index("sector"), 2) == 1
    block = lax.axis_index("block")
    z_odd = lax.rem(block, 2) == 1
    lowest = block == 0
    highest = block == lax.axis_size("block") - 1
    lanes = lane_ids(8)

    def slab(e, carry):
        r_ref[e] = source_of(e)
        for a in range(n):
            first, second = z1[a], z2[a]
            below = jnp.where(z_odd, first, second)
            above = jnp.where(z_odd, second, first)
            below = pltpu.roll(below, lax.rem(LANES - e, LANES), 1)
            above = pltpu.roll(above, LANES - 1 - e, 1)
            below = jnp.where((lanes == 0) & jnp.logical_not(lowest), PENALTY * below, 0.0)
            above = jnp.where((lanes == LANES - 1) & jnp.logical_not(highest), PENALTY * above, 0.0)
            r_ref[e, pl.ds(a * nn, n), :] += below[:n]
            r_ref[e, pl.ds(a * nn + nn - n, n), :] += above[:n]
        return carry

    lax.fori_loop(0, e_total, slab, 0, unroll=HALO_UNROLL)
    for layer in range(e_total // span):
        first, second = c1[layer], c2[layer]
        r_ref[layer * span, pl.ds(0, nn), :] += PENALTY * jnp.where(odd, first, second)
        r_ref[layer * span + span - 1, pl.ds((n - 1) * nn, nn), :] += PENALTY * jnp.where(odd, second, first)


def correct(n, e_total, span, r_ref, u_ref, u_of, c1, c2, z1, z2):
    nn = n * n
    lanes = lane_ids(8)

    def slab(e, carry):
        lows, highs = carry
        u_ref[e] = u_of(e, r_ref[e])
        new_lows, new_highs = [], []
        for a in range(n):
            low = u_ref[e, pl.ds(a * nn, 8), :]
            high = u_ref[e, pl.ds(a * nn + nn - n, 8), :]
            here = lanes == e
            new_lows.append(jnp.where(here, pltpu.roll(low, e, 1), lows[a]))
            new_highs.append(jnp.where(here, pltpu.roll(high, e + 1, 1), highs[a]))
        return tuple(new_lows), tuple(new_highs)

    blank = tuple(jnp.zeros((8, LANES), F32) for _ in range(n))
    lows, highs = lax.fori_loop(0, e_total, slab, (blank, blank), unroll=HALO_UNROLL)
    odd = lax.rem(lax.axis_index("sector"), 2) == 1
    z_odd = lax.rem(lax.axis_index("block"), 2) == 1
    for a in range(n):
        z1[a] = jnp.where(z_odd, lows[a], highs[a])
        z2[a] = jnp.where(z_odd, highs[a], lows[a])
    for layer in range(e_total // span):
        low = u_ref[layer * span, pl.ds(0, nn), :]
        high = u_ref[layer * span + span - 1, pl.ds((n - 1) * nn, nn), :]
        c1[layer] = jnp.where(odd, low, high)
        c2[layer] = jnp.where(odd, high, low)


def subtract_operator(n, e_total, span, r_ref, u_ref, weights, jac_ref, count_ref):
    nn = n * n
    group = GROUP[n]
    lanes = lane_ids(8)

    def some(i, carry):
        first = i * group
        wide = jnp.concatenate([u_ref[first + j] for j in range(group)], axis=1)
        product = times(weights[...], wide)
        for j in range(group):
            e = first + j
            own = product[:, j * LANES : (j + 1) * LANES]
            r_ref[e] = r_ref[e] - jac_ref[pl.ds(e, 1), :] * own - count_ref[...] * u_ref[e]
            s = lax.rem(e, span)
            before = jnp.where(s > 0, PENALTY, 0.0)
            after = jnp.where(s < span - 1, PENALTY, 0.0)
            previous = u_ref[jnp.maximum(e - 1, 0), pl.ds((n - 1) * nn, nn), :]
            following = u_ref[jnp.minimum(e + 1, e_total - 1), pl.ds(0, nn), :]
            r_ref[e, pl.ds(0, nn), :] += before * previous
            r_ref[e, pl.ds((n - 1) * nn, nn), :] += after * following
            for a in range(n):
                low = u_ref[e, pl.ds(a * nn, 8), :]
                high = u_ref[e, pl.ds(a * nn + nn - n, 8), :]
                from_below = jnp.where(lanes > 0, PENALTY * pltpu.roll(high, 1, 1), 0.0)
                from_above = jnp.where(lanes < LANES - 1, PENALTY * pltpu.roll(low, LANES - 1, 1), 0.0)
                r_ref[e, pl.ds(a * nn, n), :] += from_below[:n]
                r_ref[e, pl.ds(a * nn + nn - n, n), :] += from_above[:n]
        return carry

    lax.fori_loop(0, e_total // group, some, 0, unroll=GROUP_UNROLL[n])


def face_shapes(n, layers):
    circ = jax.ShapeDtypeStruct((layers, n * n, LANES), F32)
    axial = jax.ShapeDtypeStruct((n, 8, LANES), F32)
    return [circ, circ, axial, axial]


def prepare(rotor, stator, mortar, stiff_fine, stiff_coarse, restrict_fine, restrict_coarse):
    rows, span = rotor.shape[0], rotor.shape[1]
    tall, wide = up(rows, 8), up(rows, 16)
    big, small = up(NF**3, 16), up(NC**3, 16)
    smalls = (mortar, stiff_fine, stiff_coarse, restrict_fine, restrict_coarse)

    def body(
        rotor_ref, stator_ref, mortar_in, kf_in, kc_in, rf_in, rc_in,
        rotor_out, stator_out, proj_out, back_out, wf_out, wc_out, rfs_out, rcs_out, df_out, dc_out,
        mortar_ref, kf_ref, kc_ref, rf_ref, rc_ref, pad_ref, sem, small_sem,
    ):
        copies = []
        for f in range(span):
            for source, target in ((rotor_ref, rotor_out), (stator_ref, stator_out)):
                if tall > rows:
                    target[f, pl.ds(rows, tall - rows), :] = jnp.zeros((tall - rows, LANES), F32)
                copies.append(pltpu.make_async_copy(source.at[:, f, :], target.at[f, pl.ds(0, rows), :], sem))
        little = [
            pltpu.make_async_copy(source, target, small_sem)
            for source, target in (
                (mortar_in, mortar_ref), (kf_in, kf_ref), (kc_in, kc_ref), (rf_in, rf_ref), (rc_in, rc_ref)
            )
        ]
        for c in little + copies:
            c.start()
        row, col = node_rows((tall, LANES), 0), node_rows((tall, LANES), 1)
        comp_r, comp_c = digit(row, NF * NF, 4), digit(col, NF * NF, 5)
        rest_r, rest_c = row - NF * NF * comp_r, col - NF * NF * comp_c
        a_r, a_c = digit(rest_r, NF, NF - 1), digit(rest_c, NF, NF - 1)
        same = (comp_r == comp_c) & (rest_r - NF * a_r == rest_c - NF * a_c) & (row < rows) & (col < rows)
        ahead = jnp.where(same, a_r * NF + a_c, -1)
        flipped = jnp.where(same, a_c * NF + a_r, -1)
        for c in little:
            c.wait()
        for found, out in ((ahead, proj_out), (flipped, back_out)):
            pair = []
            for which in range(2):
                total = jnp.zeros((tall, LANES), F32)
                matrix = mortar_ref[:, which, :]
                for i in range(NF):
                    for j in range(NF):
                        total = jnp.where(found == i * NF + j, matrix[i : i + 1, j : j + 1], total)
                pair.append(total[:, :wide])
            highs, lows = zip(*[parts_of(m) for m in pair])
            out[...] = jnp.concatenate(
                [
                    jnp.concatenate([jnp.concatenate([h, h], axis=1) for h in highs], axis=0),
                    jnp.concatenate([jnp.concatenate([l, jnp.zeros_like(l)], axis=1) for l in lows], axis=0),
                ],
                axis=0,
            )

        def padded(ref, height, width):
            pad_ref[...] = jnp.zeros_like(pad_ref)
            pad_ref[pl.ds(0, ref.shape[0]), pl.ds(0, ref.shape[1])] = ref[...]
            return pad_ref[pl.ds(0, height), :][:, :width]

        for ref, out, diag_out, size in ((kf_ref, wf_out, df_out, big), (kc_ref, wc_out, dc_out, small)):
            matrix = padded(ref, size, size)
            out[...] = stacked(matrix)
            row = lax.broadcasted_iota(jnp.int32, (size, size), 0)
            col = lax.broadcasted_iota(jnp.int32, (size, size), 1)
            diag = jnp.sum(jnp.where(row == col, matrix, 0.0), axis=1, keepdims=True)
            diag = jnp.where(row[:, :1] < ref.shape[0], diag, 1.0)
            diag_out[...] = jnp.broadcast_to(diag, (size, LANES))
        rfs_out[...] = stacked(padded(rf_ref, small, big))
        rcs_out[...] = stacked(padded(rc_ref, 16, small))
        for c in copies:
            c.wait()

    return pl.pallas_call(
        body,
        out_shape=[
            jax.ShapeDtypeStruct((span, tall, LANES), F32),
            jax.ShapeDtypeStruct((span, tall, LANES), F32),
            jax.ShapeDtypeStruct((4 * tall, 2 * wide), BF16),
            jax.ShapeDtypeStruct((4 * tall, 2 * wide), BF16),
            jax.ShapeDtypeStruct((2 * big, 2 * big), BF16),
            jax.ShapeDtypeStruct((2 * small, 2 * small), BF16),
            jax.ShapeDtypeStruct((2 * small, 2 * big), BF16),
            jax.ShapeDtypeStruct((32, 2 * small), BF16),
            jax.ShapeDtypeStruct((big, LANES), F32),
            jax.ShapeDtypeStruct((small, LANES), F32),
        ],
        in_specs=[hbm_spec()] * 7,
        scratch_shapes=[pltpu.VMEM(m.shape, F32) for m in smalls]
        + [pltpu.VMEM((big, LANES), F32), pltpu.SemaphoreType.DMA, pltpu.SemaphoreType.DMA],
        compiler_params=params(),
        name="prepare",
    )(*in_hbm(rotor, stator, *smalls))


def apply_faces(matrix_ref, slab_of, count, tall, wide, y0, y1, unroll=1):
    group = 4
    fill = jnp.zeros((wide - tall, group * LANES), F32)

    def some(i, carry):
        first = group * i
        x = jnp.concatenate([slab_of(jnp.minimum(first + j, count - 1)) for j in range(group)], axis=1)
        if wide > tall:
            x = jnp.concatenate([x, fill], axis=0)
        high, low = parts_of(x)
        y = jnp.dot(matrix_ref[...], jnp.concatenate([high, low], axis=0), preferred_element_type=F32)
        a = y[:tall] + y[2 * tall : 3 * tall]
        b = y[tall : 2 * tall] + y[3 * tall :]
        for j in range(group):
            y0[first + j] = a[:, j * LANES : (j + 1) * LANES]
            y1[first + j] = b[:, j * LANES : (j + 1) * LANES]
        return carry

    lax.fori_loop(0, up(count, group) // group, some, 0, unroll=unroll)


def rotor_part(shift, far, near, stator, rotor, near1, near2, proj, jac, diag):
    span, tall = rotor.shape[0], rotor.shape[1]
    wide = proj.shape[1] // 2
    rows, nn = 4 * NF * NF, NF * NF
    e_total, height = jac.shape[0], diag.shape[0]
    offset = up(span + 1, 4)
    few, many = far.shape[0], near.shape[0]

    def body(
        shift_ref, far_ref, near_ref, s_in, r_in, near1_ref, near2_ref, proj_ref, jac_ref, diag_ref,
        sflux_out, inflow, kept, w_ref, y0, y1, sflux, sem,
    ):
        odd = lax.rem(lax.axis_index("sector"), 2) == 1
        before = jnp.where(odd, near1_ref[0], near2_ref[0])
        after = jnp.where(odd, near2_ref[0], near1_ref[0])
        first_rotor = STEP - 1 - shift_ref[0]

        def rotor_slab(f):
            f_win = jnp.minimum(f, span)
            f_own = jnp.maximum(f - offset, 0)
            inside = r_in[jnp.clip(f_own - 1, 0, span - 1)]
            own = jnp.where(f_own == 0, before, jnp.where(f_own == span + 1, after, inside))
            w = first_rotor + f_win
            a, b = far_ref[jnp.minimum(w, few - 1)], near_ref[jnp.clip(w - few, 0, many - 1)]
            return jnp.where(f < offset, jnp.where(w < few, a, b), own)

        apply_faces(proj_ref, rotor_slab, offset + span + 2, tall, wide, y0, y1)

        def face(g, carry):
            jump = s_in[g] - (y0[g + 1] + y1[g])
            sflux[g] = jump
            inflow[g, pl.ds(0, nn), :] = jump[:nn] + jump[3 * nn : 4 * nn]
            c = pltpu.make_async_copy(sflux.at[g, pl.ds(0, rows), :], sflux_out.at[:, g, 0, :], sem)
            c.start()
            return carry

        lax.fori_loop(0, span, face, 0)

        def own_face(g, carry):
            kept[g] = y0[offset + g + 1] + y1[offset + g]
            return carry

        lax.fori_loop(0, span + 1, own_face, 0)
        count = half_faces(NF, height)

        def weight(e, carry):
            w_ref[e] = DAMPING / (jac_ref[pl.ds(e, 1), :] * diag_ref[...] + count)
            return carry

        lax.fori_loop(0, e_total, weight, 0)

        def finish(g, carry):
            pltpu.make_async_copy(sflux.at[g, pl.ds(0, rows), :], sflux_out.at[:, g, 0, :], sem).wait()
            return carry

        lax.fori_loop(0, span, finish, 0)

    whole = pl.BlockSpec()
    buffer = pltpu.VMEM((offset + up(span + 2, 4), tall, LANES), F32)
    return pl.pallas_call(
        body,
        out_shape=[
            jax.ShapeDtypeStruct((rows, span, 1, LANES), F32),
            jax.ShapeDtypeStruct((span, up(nn, 8), LANES), F32),
            jax.ShapeDtypeStruct((span + 1, tall, LANES), F32),
            jax.ShapeDtypeStruct((e_total, height, LANES), F32),
        ],
        in_specs=[pl.BlockSpec(memory_space=pltpu.SMEM)] + [whole] * 9,
        out_specs=[hbm_spec()] + [whole] * 3,
        scratch_shapes=[buffer, buffer, pltpu.VMEM((span, tall, LANES), F32), pltpu.SemaphoreType.DMA],
        compiler_params=params(),
        cost_estimate=cost(2 * 10**9, 10 * 10**6),
        name="rotor_part",
    )(shift, far, near, stator, rotor, near1, near2, proj, jac, diag)


def first_sweep(shift, stator_win, kept, inflow, back, source, w, jac, weights, layers):
    span, tall = inflow.shape[0], kept.shape[1]
    wide = back.shape[1] // 2
    rows = 4 * NF * NF
    e_total = jac.shape[0]
    n, nn = NF, NF * NF
    nodes = n**3
    height = weights.shape[0] // 2

    def body(
        shift_ref, sw_ref, kept_ref, inflow_ref, back_ref, source_ref, w_ref, jac_ref, w_mat,
        rflux_out, r_ref, u_ref, c1, c2, z1, z2,
        y0, y1, rflux, count_ref, in_sem, out_sem,
    ):
        loads = [
            pltpu.make_async_copy(source_ref.at[:, e, :], r_ref.at[e, pl.ds(0, nodes), :], in_sem)
            for e in range(e_total)
        ]
        for c in loads:
            c.start()
        inner = shift_ref[0]
        count_ref[...] = half_faces(n, height)
        apply_faces(
            back_ref, lambda f: sw_ref[inner + f] - kept_ref[f], span + 1, tall, wide, y0, y1, unroll=5
        )
        for c in loads:
            c.wait()
        stores = []
        for s in range(span):
            back_flux = y0[s] + y1[s + 1]
            rflux[s] = back_flux
            c = pltpu.make_async_copy(rflux.at[s, pl.ds(0, rows), :], rflux_out.at[:, s, :], out_sem)
            c.start()
            stores.append(c)
            if height > nodes:
                for layer in range(layers):
                    r_ref[layer * span + s, pl.ds(nodes, height - nodes), :] = jnp.zeros((height - nodes, LANES), F32)
            outflow = back_flux[:nn] + rflux[s, pl.ds(3 * nn, nn), :]
            r_ref[span + s, pl.ds(0, nn, stride=n), :] += inflow_ref[s, pl.ds(0, nn), :]
            r_ref[s, pl.ds(n - 1, nn, stride=n), :] += -outflow
        correct(n, e_total, span, r_ref, u_ref, lambda e, r: r * w_ref[e], c1, c2, z1, z2)
        subtract_operator(n, e_total, span, r_ref, u_ref, w_mat, jac_ref, count_ref)
        for c in stores:
            c.wait()

    whole = pl.BlockSpec()
    field = jax.ShapeDtypeStruct((e_total, height, LANES), F32)
    slabs = pltpu.VMEM((up(span + 1, 4), tall, LANES), F32)
    return pl.pallas_call(
        body,
        out_shape=[jax.ShapeDtypeStruct((rows, span, LANES), F32), field, field] + face_shapes(n, layers),
        in_specs=[pl.BlockSpec(memory_space=pltpu.SMEM)] + [whole] * 4 + [hbm_spec()] + [whole] * 3,
        out_specs=[hbm_spec()] + [whole] * 6,
        scratch_shapes=[
            slabs,
            slabs,
            pltpu.VMEM((span, tall, LANES), F32),
            pltpu.VMEM((height, LANES), F32),
            pltpu.SemaphoreType.DMA,
            pltpu.SemaphoreType.DMA,
        ],
        compiler_params=params(),
        cost_estimate=cost(2 * 10**9, 20 * 10**6),
        name="first_sweep",
    )(shift, stator_win, kept, inflow, back, *in_hbm(source), w, jac, weights)


def sweep(n, r, p, w, jac, weights, faces, layers, last):
    e_total, height = r.shape[0], r.shape[1]
    span = e_total // layers
    nodes = n**3

    def body(r_in, p_in, w_in, jac_ref, w_mat, h1, h2, g1, g2, p_out, r_ref, c1, c2, z1, z2, u_ref, p_keep, count_ref, sem):
        count_ref[...] = half_faces(n, height)
        p_ref = p_keep if last else p_out
        add_halo(n, e_total, span, lambda e: r_in[e], r_ref, h1, h2, g1, g2)

        def u_of(e, r_here):
            u = r_here * w_in[e]
            p_ref[e] = p_in[e] + u
            return u

        correct(n, e_total, span, r_ref, u_ref, u_of, c1, c2, z1, z2)
        stores = []
        if last:
            for e in range(e_total):
                c = pltpu.make_async_copy(p_ref.at[e, pl.ds(0, nodes), :], p_out.at[:, e, :], sem)
                c.start()
                stores.append(c)
        subtract_operator(n, e_total, span, r_ref, u_ref, w_mat, jac_ref, count_ref)
        for c in stores:
            c.wait()

    whole = pl.BlockSpec()
    field = jax.ShapeDtypeStruct((e_total, height, LANES), F32)
    kept = jax.ShapeDtypeStruct((nodes, e_total, LANES), F32) if last else field
    return pl.pallas_call(
        body,
        out_shape=[kept, field] + face_shapes(n, layers),
        out_specs=[any_spec() if last else whole] + [whole] * 5,
        scratch_shapes=[
            pltpu.VMEM((e_total, height, LANES), F32),
            pltpu.VMEM((e_total, height, LANES) if last else (1, 8, LANES), F32),
            pltpu.VMEM((height, LANES), F32),
            pltpu.SemaphoreType.DMA,
        ],
        compiler_params=params(),
        cost_estimate=cost(10**9 if n == NF else 10**8, 10 * 10**6),
    )(r, p, w, jac, weights, *faces)


def to_coarse(r, faces, restrict, jac, weights, diag, layers):
    e_total = r.shape[0]
    span = e_total // layers
    small = weights.shape[0] // 2
    n = NC
    group = 4

    def body(r_in, h1, h2, g1, g2, rest_ref, jac_ref, w_mat, diag_ref, rc_ref, u_ref, w_ref, c1, c2, z1, z2, r_fine, count_ref):
        count_ref[...] = half_faces(n, small)
        add_halo(NF, e_total, span, lambda e: r_in[e], r_fine, h1, h2, g1, g2)

        def some(i, carry):
            first = i * group
            wide = jnp.concatenate([r_fine[first + j] for j in range(group)], axis=1)
            product = times(rest_ref[...], wide)
            for j in range(group):
                rc_ref[first + j] = product[:, j * LANES : (j + 1) * LANES]
            return carry

        lax.fori_loop(0, e_total // group, some, 0, unroll=2)

        def u_of(e, r_here):
            w_here = DAMPING / (jac_ref[pl.ds(e, 1), :] * diag_ref[...] + count_ref[...])
            w_ref[e] = w_here
            return r_here * w_here

        correct(n, e_total, span, rc_ref, u_ref, u_of, c1, c2, z1, z2)
        subtract_operator(n, e_total, span, rc_ref, u_ref, w_mat, jac_ref, count_ref)

    field = jax.ShapeDtypeStruct((e_total, small, LANES), F32)
    return pl.pallas_call(
        body,
        out_shape=[field, field, field] + face_shapes(n, layers),
        scratch_shapes=[pltpu.VMEM(r.shape, F32), pltpu.VMEM((small, LANES), F32)],
        compiler_params=params(),
        cost_estimate=cost(5 * 10**8, 5 * 10**6),
        name="to_coarse",
    )(r, *faces, restrict, jac, weights, diag)


def to_coarsest(r, faces, restrict, layers):
    e_total = r.shape[0]
    span = e_total // layers
    group = 4

    def body(r_in, h1, h2, g1, g2, rest_ref, out_ref, r_done, kept, sem):
        add_halo(NC, e_total, span, lambda e: r_in[e], r_done, h1, h2, g1, g2)

        def some(i, carry):
            first = i * group
            wide = jnp.concatenate([r_done[first + j] for j in range(group)], axis=1)
            product = times(rest_ref[...], wide)
            for j in range(group):
                kept[first + j] = product[:LAST, j * LANES : (j + 1) * LANES]
            return carry

        lax.fori_loop(0, e_total // group, some, 0, unroll=8)
        stores = []
        for e in range(e_total):
            c = pltpu.make_async_copy(kept.at[e], out_ref.at[:, e, :], sem)
            c.start()
            stores.append(c)
        for c in stores:
            c.wait()

    whole = pl.BlockSpec()
    return pl.pallas_call(
        body,
        out_shape=jax.ShapeDtypeStruct((LAST, e_total, LANES), F32),
        in_specs=[whole] * 6,
        out_specs=any_spec(),
        scratch_shapes=[
            pltpu.VMEM(r.shape, F32),
            pltpu.VMEM((e_total, LAST, LANES), F32),
            pltpu.SemaphoreType.DMA,
        ],
        compiler_params=params(),
        cost_estimate=cost(5 * 10**7, 10**6),
        name="to_coarsest",
    )(r, *faces, restrict)


def move(x, axis, by):
    count = lax.axis_size(axis)
    return lax.ppermute(x, axis, [(i, (i + by) % count) for i in range(count)])


def swap(x, axis, odd_first):
    count = lax.axis_size(axis)
    pairs = []
    for i in range(count):
        ahead = (i % 2 == 0) != odd_first
        pairs.append((i, (i + 1) % count if ahead else (i - 1) % count))
    return lax.ppermute(x, axis, pairs)


def swap_inner(x, axis, other):
    count, beside = lax.axis_size(axis), lax.axis_size(other)
    pairs = []
    for j in range(beside):
        for i in range(count):
            to = i + 1 if i % 2 else i - 1
            target = (j, to) if 0 <= to < count else (j ^ 1, i)
            pairs.append((j * count + i, target[0] * count + target[1]))
    return lax.ppermute(x, (other, axis), pairs)


def exchange(faces):
    c1, c2, z1, z2 = faces
    c2 = swap(c2, "sector", True)
    z2 = swap_inner(z2, "block", "sector")
    z1 = swap(z1, "block", False)
    c1 = swap(c1, "sector", False)
    return c1, c2, z1, z2


def windows(rotor, stator, offset, own):
    span = rotor.shape[0]
    sectors = lax.axis_size("sector")
    buckets = span // STEP
    device, rest = offset // span, offset % span

    def branch(number):
        by, bucket = number // buckets, number % buckets
        many, few = span - STEP * bucket, STEP * (bucket + 1)

        def run(shift, rotor, stator, own):
            near = move(rotor[:many], "sector", by)
            far = move(rotor[span - few :], "sector", by + 1)
            near_s = move(stator[span - many :], "sector", -by)
            far_s = move(stator[:few], "sector", -by - 1)
            done = rotor_part(shift, far, near, stator, rotor, *own)
            return jnp.concatenate([near_s, far_s], axis=0), *done

        return run

    choice = device * buckets + rest // STEP
    shift = (rest % STEP).reshape(1)
    return shift, lax.switch(choice, [branch(i) for i in range(sectors * buckets)], shift, rotor, stator, own)


def per_device(
    source, jacobian, stiff_fine, stiff_coarse, restrict_fine, restrict_coarse, mortar_proj, rotor_trace,
    stator_trace, offsets,
):
    layers, span, axial = jacobian.shape
    e_total = layers * span
    source_rows = source.reshape(source.shape[0], e_total, axial)
    jac = jacobian.reshape(e_total, axial)
    rotor_rows = rotor_trace.reshape(-1, span, axial)
    stator_rows = stator_trace.reshape(-1, span, axial)
    rotor, stator, proj, back, wf, wc, rfs, rcs, df, dc = prepare(
        rotor_rows, stator_rows, mortar_proj.transpose(1, 0, 2), stiff_fine, stiff_coarse, restrict_fine, restrict_coarse
    )
    odd = lax.axis_index("sector") % 2 == 1
    first, final = rotor[:1], rotor[span - 1 :]
    near1 = swap(jnp.where(odd, first, final), "sector", False)
    near2 = swap(jnp.where(odd, final, first), "sector", True)
    own = (near1, near2, proj, jac, df)
    shift, (stator_win, sflux, inflow, kept, w) = windows(rotor, stator, offsets[0], own)
    rflux, r, p, *faces = first_sweep(shift, stator_win, kept, inflow, back, source_rows, w, jac, wf, layers)
    p, r, *faces = sweep(NF, r, p, w, jac, wf, exchange(faces), layers, False)
    fine, r, *faces = sweep(NF, r, p, w, jac, wf, exchange(faces), layers, True)
    r, p, w, *faces = to_coarse(r, exchange(faces), rfs, jac, wc, dc, layers)
    p, r, *faces = sweep(NC, r, p, w, jac, wc, exchange(faces), layers, False)
    coarse, r, *faces = sweep(NC, r, p, w, jac, wc, exchange(faces), layers, True)
    coarsest = to_coarsest(r, exchange(faces), rcs, layers)
    shape = (layers, span, axial)
    return (
        sflux.reshape(stator_trace.shape),
        rflux.reshape(rotor_trace.shape),
        fine.reshape((-1,) + shape),
        coarse.reshape((-1,) + shape),
        coarsest.reshape((-1,) + shape),
    )


def solution(mesh):
    cell = P(None, None, "sector", "block")

    return jax.shard_map(
        per_device,
        mesh=mesh,
        in_specs=(cell, P(None, "sector", "block"), P(), P(), P(), P(), P(), cell, cell, P("block")),
        out_specs=(cell,) * 5,
        check_vma=False,
    )
```

```python
import jax
import jax.numpy as jnp
from jax import lax
from jax.experimental import pallas as pl
from jax.experimental.pallas import tpu as pltpu
from jax.sharding import PartitionSpec as P


F32 = jnp.float32
BF16 = jnp.bfloat16
DAMPING = 0.6
PENALTY = 0.5
LANES = 128
NF = 5
NC = 3
LAST = 8
STEP = 4
FACE_UNROLL = 5
HALO_UNROLL = 32
GROUP = {NF: 4, NC: 16}
GROUP_UNROLL = {NF: 4, NC: 1}
VMEM_BYTES = 12 * 1024 * 1024


def up(value, unit):
    return (value + unit - 1) // unit * unit


def any_spec():
    return pl.BlockSpec(memory_space=pl.ANY)


def hbm_spec():
    return pl.BlockSpec(memory_space=pltpu.HBM)


def in_hbm(*arrays):
    return tuple(pltpu.with_memory_space_constraint(x, pltpu.HBM) for x in arrays)


def params(**extra):
    return pltpu.CompilerParams(vmem_limit_bytes=VMEM_BYTES, **extra)


def cost(flops, data):
    return pl.CostEstimate(flops=flops, bytes_accessed=data, transcendentals=0)


def parts_of(x):
    high = x.astype(BF16)
    low = (x - high.astype(F32)).astype(BF16)
    return high, low


def stacked(matrix):
    high, low = parts_of(matrix)
    top = jnp.concatenate([high, high], axis=1)
    bottom = jnp.concatenate([low, jnp.zeros_like(low)], axis=1)
    return jnp.concatenate([top, bottom], axis=0)


def times(weights, x):
    rows = weights.shape[0] // 2
    high, low = parts_of(x)
    both = jnp.dot(weights, jnp.concatenate([high, low], axis=0), preferred_element_type=F32)
    return both[:rows] + both[rows:]


def lane_ids(rows):
    return lax.broadcasted_iota(jnp.int32, (rows, LANES), 1)


def node_rows(shape, axis):
    return lax.broadcasted_iota(jnp.int32, shape, axis)


def digit(index, unit, most):
    found = jnp.zeros_like(index)
    for k in range(1, most + 1):
        found += jnp.where(index >= k * unit, 1, 0)
    return found


def half_faces(n, height):
    row = node_rows((height, LANES), 0)
    a = digit(row, n * n, n)
    b = digit(row - n * n * a, n, n - 1)
    on_a = jnp.where((a == 0) | (a == n - 1), PENALTY, 0.0)
    on_b = jnp.where((b == 0) | (b == n - 1), PENALTY, 0.0)
    return jnp.where(row < n**3, on_a + on_b, 0.0)


def add_halo(n, e_total, span, source_of, r_ref, c1, c2, z1, z2):
    nn = n * n
    odd = lax.rem(lax.axis_index("sector"), 2) == 1
    block = lax.axis_index("block")
    z_odd = lax.rem(block, 2) == 1
    lowest = block == 0
    highest = block == lax.axis_size("block") - 1
    lanes = lane_ids(8)

    def slab(e, carry):
        r_ref[e] = source_of(e)
        for a in range(n):
            first, second = z1[a], z2[a]
            below = jnp.where(z_odd, first, second)
            above = jnp.where(z_odd, second, first)
            below = pltpu.roll(below, lax.rem(LANES - e, LANES), 1)
            above = pltpu.roll(above, LANES - 1 - e, 1)
            below = jnp.where((lanes == 0) & jnp.logical_not(lowest), PENALTY * below, 0.0)
            above = jnp.where((lanes == LANES - 1) & jnp.logical_not(highest), PENALTY * above, 0.0)
            r_ref[e, pl.ds(a * nn, n), :] += below[:n]
            r_ref[e, pl.ds(a * nn + nn - n, n), :] += above[:n]
        return carry

    lax.fori_loop(0, e_total, slab, 0, unroll=HALO_UNROLL)
    for layer in range(e_total // span):
        first, second = c1[layer], c2[layer]
        r_ref[layer * span, pl.ds(0, nn), :] += PENALTY * jnp.where(odd, first, second)
        r_ref[layer * span + span - 1, pl.ds((n - 1) * nn, nn), :] += PENALTY * jnp.where(odd, second, first)


def correct(n, e_total, span, r_ref, u_ref, u_of, c1, c2, z1, z2):
    nn = n * n
    lanes = lane_ids(8)

    def slab(e, carry):
        lows, highs = carry
        u_ref[e] = u_of(e, r_ref[e])
        new_lows, new_highs = [], []
        for a in range(n):
            low = u_ref[e, pl.ds(a * nn, 8), :]
            high = u_ref[e, pl.ds(a * nn + nn - n, 8), :]
            here = lanes == e
            new_lows.append(jnp.where(here, pltpu.roll(low, e, 1), lows[a]))
            new_highs.append(jnp.where(here, pltpu.roll(high, e + 1, 1), highs[a]))
        return tuple(new_lows), tuple(new_highs)

    blank = tuple(jnp.zeros((8, LANES), F32) for _ in range(n))
    lows, highs = lax.fori_loop(0, e_total, slab, (blank, blank), unroll=HALO_UNROLL)
    odd = lax.rem(lax.axis_index("sector"), 2) == 1
    z_odd = lax.rem(lax.axis_index("block"), 2) == 1
    for a in range(n):
        z1[a] = jnp.where(z_odd, lows[a], highs[a])
        z2[a] = jnp.where(z_odd, highs[a], lows[a])
    for layer in range(e_total // span):
        low = u_ref[layer * span, pl.ds(0, nn), :]
        high = u_ref[layer * span + span - 1, pl.ds((n - 1) * nn, nn), :]
        c1[layer] = jnp.where(odd, low, high)
        c2[layer] = jnp.where(odd, high, low)


def subtract_operator(n, e_total, span, r_ref, u_ref, weights, jac_ref, count_ref):
    nn = n * n
    group = GROUP[n]
    lanes = lane_ids(8)

    def some(i, carry):
        first = i * group
        wide = jnp.concatenate([u_ref[first + j] for j in range(group)], axis=1)
        product = times(weights[...], wide)
        for j in range(group):
            e = first + j
            own = product[:, j * LANES : (j + 1) * LANES]
            r_ref[e] = r_ref[e] - jac_ref[pl.ds(e, 1), :] * own - count_ref[...] * u_ref[e]
            s = lax.rem(e, span)
            before = jnp.where(s > 0, PENALTY, 0.0)
            after = jnp.where(s < span - 1, PENALTY, 0.0)
            previous = u_ref[jnp.maximum(e - 1, 0), pl.ds((n - 1) * nn, nn), :]
            following = u_ref[jnp.minimum(e + 1, e_total - 1), pl.ds(0, nn), :]
            r_ref[e, pl.ds(0, nn), :] += before * previous
            r_ref[e, pl.ds((n - 1) * nn, nn), :] += after * following
            for a in range(n):
                low = u_ref[e, pl.ds(a * nn, 8), :]
                high = u_ref[e, pl.ds(a * nn + nn - n, 8), :]
                from_below = jnp.where(lanes > 0, PENALTY * pltpu.roll(high, 1, 1), 0.0)
                from_above = jnp.where(lanes < LANES - 1, PENALTY * pltpu.roll(low, LANES - 1, 1), 0.0)
                r_ref[e, pl.ds(a * nn, n), :] += from_below[:n]
                r_ref[e, pl.ds(a * nn + nn - n, n), :] += from_above[:n]
        return carry

    lax.fori_loop(0, e_total // group, some, 0, unroll=GROUP_UNROLL[n])


def face_shapes(n, layers):
    circ = jax.ShapeDtypeStruct((layers, n * n, LANES), F32)
    axial = jax.ShapeDtypeStruct((n, 8, LANES), F32)
    return [circ, circ, axial, axial]


def prepare(rotor, stator, mortar, stiff_fine, stiff_coarse, restrict_fine, restrict_coarse):
    rows, span = rotor.shape[0], rotor.shape[1]
    tall, wide = up(rows, 8), up(rows, 16)
    big, small = up(NF**3, 16), up(NC**3, 16)
    smalls = (mortar, stiff_fine, stiff_coarse, restrict_fine, restrict_coarse)

    def body(
        rotor_ref, stator_ref, mortar_in, kf_in, kc_in, rf_in, rc_in,
        rotor_out, stator_out, proj_out, back_out, wf_out, wc_out, rfs_out, rcs_out, df_out, dc_out,
        mortar_ref, kf_ref, kc_ref, rf_ref, rc_ref, pad_ref, sem, small_sem,
    ):
        copies = []
        for f in range(span):
            for source, target in ((rotor_ref, rotor_out), (stator_ref, stator_out)):
                if tall > rows:
                    target[f, pl.ds(rows, tall - rows), :] = jnp.zeros((tall - rows, LANES), F32)
                copies.append(pltpu.make_async_copy(source.at[:, f, :], target.at[f, pl.ds(0, rows), :], sem))
        little = [
            pltpu.make_async_copy(source, target, small_sem)
            for source, target in (
                (mortar_in, mortar_ref), (kf_in, kf_ref), (kc_in, kc_ref), (rf_in, rf_ref), (rc_in, rc_ref)
            )
        ]
        for c in little + copies:
            c.start()
        row, col = node_rows((tall, LANES), 0), node_rows((tall, LANES), 1)
        comp_r, comp_c = digit(row, NF * NF, 4), digit(col, NF * NF, 5)
        rest_r, rest_c = row - NF * NF * comp_r, col - NF * NF * comp_c
        a_r, a_c = digit(rest_r, NF, NF - 1), digit(rest_c, NF, NF - 1)
        same = (comp_r == comp_c) & (rest_r - NF * a_r == rest_c - NF * a_c) & (row < rows) & (col < rows)
        ahead = jnp.where(same, a_r * NF + a_c, -1)
        flipped = jnp.where(same, a_c * NF + a_r, -1)
        for c in little:
            c.wait()
        for found, out in ((ahead, proj_out), (flipped, back_out)):
            pair = []
            for which in range(2):
                total = jnp.zeros((tall, LANES), F32)
                matrix = mortar_ref[:, which, :]
                for i in range(NF):
                    for j in range(NF):
                        total = jnp.where(found == i * NF + j, matrix[i : i + 1, j : j + 1], total)
                pair.append(total[:, :wide])
            highs, lows = zip(*[parts_of(m) for m in pair])
            out[...] = jnp.concatenate(
                [
                    jnp.concatenate([jnp.concatenate([h, h], axis=1) for h in highs], axis=0),
                    jnp.concatenate([jnp.concatenate([l, jnp.zeros_like(l)], axis=1) for l in lows], axis=0),
                ],
                axis=0,
            )

        def padded(ref, height, width):
            pad_ref[...] = jnp.zeros_like(pad_ref)
            pad_ref[pl.ds(0, ref.shape[0]), pl.ds(0, ref.shape[1])] = ref[...]
            return pad_ref[pl.ds(0, height), :][:, :width]

        for ref, out, diag_out, size in ((kf_ref, wf_out, df_out, big), (kc_ref, wc_out, dc_out, small)):
            matrix = padded(ref, size, size)
            out[...] = stacked(matrix)
            row = lax.broadcasted_iota(jnp.int32, (size, size), 0)
            col = lax.broadcasted_iota(jnp.int32, (size, size), 1)
            diag = jnp.sum(jnp.where(row == col, matrix, 0.0), axis=1, keepdims=True)
            diag = jnp.where(row[:, :1] < ref.shape[0], diag, 1.0)
            diag_out[...] = jnp.broadcast_to(diag, (size, LANES))
        rfs_out[...] = stacked(padded(rf_ref, small, big))
        rcs_out[...] = stacked(padded(rc_ref, 16, small))
        for c in copies:
            c.wait()

    return pl.pallas_call(
        body,
        out_shape=[
            jax.ShapeDtypeStruct((span, tall, LANES), F32),
            jax.ShapeDtypeStruct((span, tall, LANES), F32),
            jax.ShapeDtypeStruct((4 * tall, 2 * wide), BF16),
            jax.ShapeDtypeStruct((4 * tall, 2 * wide), BF16),
            jax.ShapeDtypeStruct((2 * big, 2 * big), BF16),
            jax.ShapeDtypeStruct((2 * small, 2 * small), BF16),
            jax.ShapeDtypeStruct((2 * small, 2 * big), BF16),
            jax.ShapeDtypeStruct((32, 2 * small), BF16),
            jax.ShapeDtypeStruct((big, LANES), F32),
            jax.ShapeDtypeStruct((small, LANES), F32),
        ],
        in_specs=[hbm_spec()] * 7,
        scratch_shapes=[pltpu.VMEM(m.shape, F32) for m in smalls]
        + [pltpu.VMEM((big, LANES), F32), pltpu.SemaphoreType.DMA, pltpu.SemaphoreType.DMA],
        compiler_params=params(),
        name="prepare",
    )(*in_hbm(rotor, stator, *smalls))


def apply_faces(matrix_ref, slab_of, count, tall, wide, y0, y1, unroll=1):
    group = 4
    fill = jnp.zeros((wide - tall, group * LANES), F32)

    def some(i, carry):
        first = group * i
        x = jnp.concatenate([slab_of(jnp.minimum(first + j, count - 1)) for j in range(group)], axis=1)
        if wide > tall:
            x = jnp.concatenate([x, fill], axis=0)
        high, low = parts_of(x)
        y = jnp.dot(matrix_ref[...], jnp.concatenate([high, low], axis=0), preferred_element_type=F32)
        a = y[:tall] + y[2 * tall : 3 * tall]
        b = y[tall : 2 * tall] + y[3 * tall :]
        for j in range(group):
            y0[first + j] = a[:, j * LANES : (j + 1) * LANES]
            y1[first + j] = b[:, j * LANES : (j + 1) * LANES]
        return carry

    lax.fori_loop(0, up(count, group) // group, some, 0, unroll=unroll)


def own_part(rotor, near1, near2, proj, jac, diag):
    span, tall = rotor.shape[0], rotor.shape[1]
    wide = proj.shape[1] // 2
    e_total, height = jac.shape[0], diag.shape[0]

    def body(r_in, near1_ref, near2_ref, proj_ref, jac_ref, diag_ref, kept, w_ref, y0, y1):
        odd = lax.rem(lax.axis_index("sector"), 2) == 1
        before = jnp.where(odd, near1_ref[0], near2_ref[0])
        after = jnp.where(odd, near2_ref[0], near1_ref[0])

        def rotor_slab(f):
            inside = r_in[jnp.clip(f - 1, 0, span - 1)]
            return jnp.where(f == 0, before, jnp.where(f == span + 1, after, inside))

        apply_faces(proj_ref, rotor_slab, span + 2, tall, wide, y0, y1)

        def face(g, carry):
            kept[g] = y0[g + 1] + y1[g]
            return carry

        lax.fori_loop(0, span + 1, face, 0)
        count = half_faces(NF, height)

        def weight(e, carry):
            w_ref[e] = DAMPING / (jac_ref[pl.ds(e, 1), :] * diag_ref[...] + count)
            return carry

        lax.fori_loop(0, e_total, weight, 0)

    return pl.pallas_call(
        body,
        out_shape=[
            jax.ShapeDtypeStruct((span + 1, tall, LANES), F32),
            jax.ShapeDtypeStruct((e_total, height, LANES), F32),
        ],
        scratch_shapes=[pltpu.VMEM((up(span + 2, 4), tall, LANES), F32)] * 2,
        compiler_params=params(),
        cost_estimate=cost(2 * 10**9, 10 * 10**6),
        name="own_part",
    )(rotor, near1, near2, proj, jac, diag)


def join(far, near, near_s, far_s):
    few, many = far.shape[0], near.shape[0]
    window = jax.ShapeDtypeStruct((few + many,) + far.shape[1:], F32)

    def body(far_ref, near_ref, near_s_ref, far_s_ref, rotor_out, stator_out):
        def copy(source, out, first):
            def one(f, carry):
                out[first + f] = source[f]
                return carry

            lax.fori_loop(0, source.shape[0], one, 0)

        copy(far_ref, rotor_out, 0)
        copy(near_ref, rotor_out, few)
        copy(near_s_ref, stator_out, 0)
        copy(far_s_ref, stator_out, many)

    return pl.pallas_call(body, out_shape=[window, window], compiler_params=params(), name="join")(
        far, near, near_s, far_s
    )


def first_sweep(shift, rotor_win, stator_win, stator, kept, proj, back, source, w, jac, weights, layers):
    span, tall = stator.shape[0], stator.shape[1]
    wide = back.shape[1] // 2
    rows = 4 * NF * NF
    e_total = jac.shape[0]
    n, nn = NF, NF * NF
    nodes = n**3
    height = weights.shape[0] // 2

    def body(
        shift_ref, rw_ref, sw_ref, s_in, kept_ref, proj_ref, back_ref, source_ref, w_ref, jac_ref, w_mat,
        sflux_out, rflux_out, r_ref, u_ref, c1, c2, z1, z2,
        y0, y1, x0, x1, sflux, rflux, count_ref, in_sem, out_sem,
    ):
        loads = [
            pltpu.make_async_copy(source_ref.at[:, e, :], r_ref.at[e, pl.ds(0, nodes), :], in_sem)
            for e in range(e_total)
        ]
        for c in loads:
            c.start()
        inner = shift_ref[0]
        first_rotor = STEP - 1 - inner
        count_ref[...] = half_faces(n, height)
        apply_faces(proj_ref, lambda f: rw_ref[first_rotor + f], span + 1, tall, wide, x0, x1, unroll=FACE_UNROLL)
        apply_faces(
            back_ref, lambda f: sw_ref[inner + f] - kept_ref[f], span + 1, tall, wide, y0, y1, unroll=FACE_UNROLL
        )
        stores = []
        for s in range(span):
            sflux[s] = s_in[s] - (x0[s + 1] + x1[s])
            rflux[s] = y0[s] + y1[s + 1]
            for buffer, out in ((sflux, sflux_out), (rflux, rflux_out)):
                c = pltpu.make_async_copy(buffer.at[s, pl.ds(0, rows), :], out.at[:, s, :], out_sem)
                c.start()
                stores.append(c)
        for c in loads:
            c.wait()
        for s in range(span):
            if height > nodes:
                for layer in range(layers):
                    r_ref[layer * span + s, pl.ds(nodes, height - nodes), :] = jnp.zeros((height - nodes, LANES), F32)
            inflow = sflux[s, pl.ds(0, nn), :] + sflux[s, pl.ds(3 * nn, nn), :]
            outflow = rflux[s, pl.ds(0, nn), :] + rflux[s, pl.ds(3 * nn, nn), :]
            r_ref[span + s, pl.ds(0, nn, stride=n), :] += inflow
            r_ref[s, pl.ds(n - 1, nn, stride=n), :] += -outflow
        correct(n, e_total, span, r_ref, u_ref, lambda e, r: r * w_ref[e], c1, c2, z1, z2)
        subtract_operator(n, e_total, span, r_ref, u_ref, w_mat, jac_ref, count_ref)
        for c in stores:
            c.wait()

    whole = pl.BlockSpec()
    field = jax.ShapeDtypeStruct((e_total, height, LANES), F32)
    trace = jax.ShapeDtypeStruct((rows, span, LANES), F32)
    slabs = pltpu.VMEM((up(span + 1, 4), tall, LANES), F32)
    return pl.pallas_call(
        body,
        out_shape=[trace, trace, field, field] + face_shapes(n, layers),
        in_specs=[pl.BlockSpec(memory_space=pltpu.SMEM)] + [whole] * 6 + [hbm_spec()] + [whole] * 3,
        out_specs=[hbm_spec()] * 2 + [whole] * 6,
        scratch_shapes=[slabs] * 4
        + [
            pltpu.VMEM((span, tall, LANES), F32),
            pltpu.VMEM((span, tall, LANES), F32),
            pltpu.VMEM((height, LANES), F32),
            pltpu.SemaphoreType.DMA,
            pltpu.SemaphoreType.DMA,
        ],
        compiler_params=params(),
        cost_estimate=cost(2 * 10**9, 20 * 10**6),
        name="first_sweep",
    )(shift, rotor_win, stator_win, stator, kept, proj, back, *in_hbm(source), w, jac, weights)


def sweep(n, r, p, w, jac, weights, faces, layers, last):
    e_total, height = r.shape[0], r.shape[1]
    span = e_total // layers
    nodes = n**3

    def body(r_in, p_in, w_in, jac_ref, w_mat, h1, h2, g1, g2, p_out, r_ref, c1, c2, z1, z2, u_ref, p_keep, count_ref, sem):
        count_ref[...] = half_faces(n, height)
        p_ref = p_keep if last else p_out
        add_halo(n, e_total, span, lambda e: r_in[e], r_ref, h1, h2, g1, g2)

        def u_of(e, r_here):
            u = r_here * w_in[e]
            p_ref[e] = p_in[e] + u
            return u

        correct(n, e_total, span, r_ref, u_ref, u_of, c1, c2, z1, z2)
        stores = []
        if last:
            for e in range(e_total):
                c = pltpu.make_async_copy(p_ref.at[e, pl.ds(0, nodes), :], p_out.at[:, e, :], sem)
                c.start()
                stores.append(c)
        subtract_operator(n, e_total, span, r_ref, u_ref, w_mat, jac_ref, count_ref)
        for c in stores:
            c.wait()

    whole = pl.BlockSpec()
    field = jax.ShapeDtypeStruct((e_total, height, LANES), F32)
    kept = jax.ShapeDtypeStruct((nodes, e_total, LANES), F32) if last else field
    return pl.pallas_call(
        body,
        out_shape=[kept, field] + face_shapes(n, layers),
        out_specs=[any_spec() if last else whole] + [whole] * 5,
        scratch_shapes=[
            pltpu.VMEM((e_total, height, LANES), F32),
            pltpu.VMEM((e_total, height, LANES) if last else (1, 8, LANES), F32),
            pltpu.VMEM((height, LANES), F32),
            pltpu.SemaphoreType.DMA,
        ],
        compiler_params=params(),
        cost_estimate=cost(10**9 if n == NF else 10**8, 10 * 10**6),
    )(r, p, w, jac, weights, *faces)


def to_coarse(r, faces, restrict, jac, weights, diag, layers):
    e_total = r.shape[0]
    span = e_total // layers
    small = weights.shape[0] // 2
    n = NC
    group = 4

    def body(r_in, h1, h2, g1, g2, rest_ref, jac_ref, w_mat, diag_ref, rc_ref, u_ref, w_ref, c1, c2, z1, z2, r_fine, count_ref):
        count_ref[...] = half_faces(n, small)
        add_halo(NF, e_total, span, lambda e: r_in[e], r_fine, h1, h2, g1, g2)

        def some(i, carry):
            first = i * group
            wide = jnp.concatenate([r_fine[first + j] for j in range(group)], axis=1)
            product = times(rest_ref[...], wide)
            for j in range(group):
                rc_ref[first + j] = product[:, j * LANES : (j + 1) * LANES]
            return carry

        lax.fori_loop(0, e_total // group, some, 0, unroll=2)

        def u_of(e, r_here):
            w_here = DAMPING / (jac_ref[pl.ds(e, 1), :] * diag_ref[...] + count_ref[...])
            w_ref[e] = w_here
            return r_here * w_here

        correct(n, e_total, span, rc_ref, u_ref, u_of, c1, c2, z1, z2)
        subtract_operator(n, e_total, span, rc_ref, u_ref, w_mat, jac_ref, count_ref)

    field = jax.ShapeDtypeStruct((e_total, small, LANES), F32)
    return pl.pallas_call(
        body,
        out_shape=[field, field, field] + face_shapes(n, layers),
        scratch_shapes=[pltpu.VMEM(r.shape, F32), pltpu.VMEM((small, LANES), F32)],
        compiler_params=params(),
        cost_estimate=cost(5 * 10**8, 5 * 10**6),
        name="to_coarse",
    )(r, *faces, restrict, jac, weights, diag)


def to_coarsest(r, faces, restrict, layers):
    e_total = r.shape[0]
    span = e_total // layers
    group = 4

    def body(r_in, h1, h2, g1, g2, rest_ref, out_ref, r_done, kept, sem):
        add_halo(NC, e_total, span, lambda e: r_in[e], r_done, h1, h2, g1, g2)

        def some(i, carry):
            first = i * group
            wide = jnp.concatenate([r_done[first + j] for j in range(group)], axis=1)
            product = times(rest_ref[...], wide)
            for j in range(group):
                kept[first + j] = product[:LAST, j * LANES : (j + 1) * LANES]
            return carry

        lax.fori_loop(0, e_total // group, some, 0, unroll=8)
        stores = []
        for e in range(e_total):
            c = pltpu.make_async_copy(kept.at[e], out_ref.at[:, e, :], sem)
            c.start()
            stores.append(c)
        for c in stores:
            c.wait()

    whole = pl.BlockSpec()
    return pl.pallas_call(
        body,
        out_shape=jax.ShapeDtypeStruct((LAST, e_total, LANES), F32),
        in_specs=[whole] * 6,
        out_specs=any_spec(),
        scratch_shapes=[
            pltpu.VMEM(r.shape, F32),
            pltpu.VMEM((e_total, LAST, LANES), F32),
            pltpu.SemaphoreType.DMA,
        ],
        compiler_params=params(),
        cost_estimate=cost(5 * 10**7, 10**6),
        name="to_coarsest",
    )(r, *faces, restrict)


def move(x, axis, by):
    count = lax.axis_size(axis)
    return lax.ppermute(x, axis, [(i, (i + by) % count) for i in range(count)])


def swap(x, axis, odd_first):
    count = lax.axis_size(axis)
    pairs = []
    for i in range(count):
        ahead = (i % 2 == 0) != odd_first
        pairs.append((i, (i + 1) % count if ahead else (i - 1) % count))
    return lax.ppermute(x, axis, pairs)


def swap_inner(x, axis, other):
    count, beside = lax.axis_size(axis), lax.axis_size(other)
    pairs = []
    for j in range(beside):
        for i in range(count):
            to = i + 1 if i % 2 else i - 1
            target = (j, to) if 0 <= to < count else (j ^ 1, i)
            pairs.append((j * count + i, target[0] * count + target[1]))
    return lax.ppermute(x, (other, axis), pairs)


def exchange(faces):
    c1, c2, z1, z2 = faces
    c2 = swap(c2, "sector", True)
    z2 = swap_inner(z2, "block", "sector")
    z1 = swap(z1, "block", False)
    c1 = swap(c1, "sector", False)
    return c1, c2, z1, z2


def windows(rotor, stator, offset, own):
    span = rotor.shape[0]
    sectors = lax.axis_size("sector")
    buckets = span // STEP
    device, rest = offset // span, offset % span

    def branch(number):
        by, bucket = number // buckets, number % buckets
        many, few = span - STEP * bucket, STEP * (bucket + 1)

        def run(rotor, stator, own):
            near = move(rotor[:many], "sector", by)
            far = move(rotor[span - few :], "sector", by + 1)
            near_s = move(stator[span - many :], "sector", -by)
            far_s = move(stator[:few], "sector", -by - 1)
            kept, w = own_part(rotor, *own)
            return *join(far, near, near_s, far_s), kept, w

        return run

    choice = device * buckets + rest // STEP
    shift = (rest % STEP).reshape(1)
    return shift, lax.switch(choice, [branch(i) for i in range(sectors * buckets)], rotor, stator, own)


def per_device(
    source, jacobian, stiff_fine, stiff_coarse, restrict_fine, restrict_coarse, mortar_proj, rotor_trace,
    stator_trace, offsets,
):
    layers, span, axial = jacobian.shape
    e_total = layers * span
    source_rows = source.reshape(source.shape[0], e_total, axial)
    jac = jacobian.reshape(e_total, axial)
    rotor_rows = rotor_trace.reshape(-1, span, axial)
    stator_rows = stator_trace.reshape(-1, span, axial)
    rotor, stator, proj, back, wf, wc, rfs, rcs, df, dc = prepare(
        rotor_rows, stator_rows, mortar_proj.transpose(1, 0, 2), stiff_fine, stiff_coarse, restrict_fine, restrict_coarse
    )
    odd = lax.axis_index("sector") % 2 == 1
    first, final = rotor[:1], rotor[span - 1 :]
    near1 = swap(jnp.where(odd, first, final), "sector", False)
    near2 = swap(jnp.where(odd, final, first), "sector", True)
    own = (near1, near2, proj, jac, df)
    shift, (rotor_win, stator_win, kept, w) = windows(rotor, stator, offsets[0], own)
    sflux, rflux, r, p, *faces = first_sweep(
        shift, rotor_win, stator_win, stator, kept, proj, back, source_rows, w, jac, wf, layers
    )
    p, r, *faces = sweep(NF, r, p, w, jac, wf, exchange(faces), layers, False)
    fine, r, *faces = sweep(NF, r, p, w, jac, wf, exchange(faces), layers, True)
    r, p, w, *faces = to_coarse(r, exchange(faces), rfs, jac, wc, dc, layers)
    p, r, *faces = sweep(NC, r, p, w, jac, wc, exchange(faces), layers, False)
    coarse, r, *faces = sweep(NC, r, p, w, jac, wc, exchange(faces), layers, True)
    coarsest = to_coarsest(r, exchange(faces), rcs, layers)
    shape = (layers, span, axial)
    return (
        sflux.reshape(stator_trace.shape),
        rflux.reshape(rotor_trace.shape),
        fine.reshape((-1,) + shape),
        coarse.reshape((-1,) + shape),
        coarsest.reshape((-1,) + shape),
    )


def solution(mesh):
    cell = P(None, None, "sector", "block")

    return jax.shard_map(
        per_device,
        mesh=mesh,
        in_specs=(cell, P(None, "sector", "block"), P(), P(), P(), P(), P(), cell, cell, P("block")),
        out_specs=(cell,) * 5,
        check_vma=False,
    )
```

```python
import jax
import jax.numpy as jnp
from jax import lax
from jax.experimental import pallas as pl
from jax.experimental.pallas import tpu as pltpu
from jax.sharding import PartitionSpec as P


F32 = jnp.float32
BF16 = jnp.bfloat16
DAMPING = 0.6
PENALTY = 0.5
LANES = 128
NF = 5
NC = 3
LAST = 8
STEP = 4
SUM_ROWS = 32
HALO_UNROLL = 32
GROUP = {NF: 4, NC: 16}
GROUP_UNROLL = {NF: 4, NC: 1}
VMEM_BYTES = 12 * 1024 * 1024


def up(value, unit):
    return (value + unit - 1) // unit * unit


def any_spec():
    return pl.BlockSpec(memory_space=pl.ANY)


def hbm_spec():
    return pl.BlockSpec(memory_space=pltpu.HBM)


def in_hbm(*arrays):
    return tuple(pltpu.with_memory_space_constraint(x, pltpu.HBM) for x in arrays)


def params(**extra):
    return pltpu.CompilerParams(vmem_limit_bytes=VMEM_BYTES, **extra)


def cost(flops, data):
    return pl.CostEstimate(flops=flops, bytes_accessed=data, transcendentals=0)


def parts_of(x):
    high = x.astype(BF16)
    low = (x - high.astype(F32)).astype(BF16)
    return high, low


def stacked(matrix):
    high, low = parts_of(matrix)
    top = jnp.concatenate([high, high], axis=1)
    bottom = jnp.concatenate([low, jnp.zeros_like(low)], axis=1)
    return jnp.concatenate([top, bottom], axis=0)


def times(weights, x):
    rows = weights.shape[0] // 2
    high, low = parts_of(x)
    both = jnp.dot(weights, jnp.concatenate([high, low], axis=0), preferred_element_type=F32)
    return both[:rows] + both[rows:]


def lane_ids(rows):
    return lax.broadcasted_iota(jnp.int32, (rows, LANES), 1)


def node_rows(shape, axis):
    return lax.broadcasted_iota(jnp.int32, shape, axis)


def digit(index, unit, most):
    found = jnp.zeros_like(index)
    for k in range(1, most + 1):
        found += jnp.where(index >= k * unit, 1, 0)
    return found


def half_faces(n, height):
    row = node_rows((height, LANES), 0)
    a = digit(row, n * n, n)
    b = digit(row - n * n * a, n, n - 1)
    on_a = jnp.where((a == 0) | (a == n - 1), PENALTY, 0.0)
    on_b = jnp.where((b == 0) | (b == n - 1), PENALTY, 0.0)
    return jnp.where(row < n**3, on_a + on_b, 0.0)


def add_halo(n, e_total, span, source_of, r_ref, c1, c2, z1, z2):
    nn = n * n
    odd = lax.rem(lax.axis_index("sector"), 2) == 1
    block = lax.axis_index("block")
    z_odd = lax.rem(block, 2) == 1
    lowest = block == 0
    highest = block == lax.axis_size("block") - 1
    lanes = lane_ids(8)

    def slab(e, carry):
        r_ref[e] = source_of(e)
        for a in range(n):
            first, second = z1[a], z2[a]
            below = jnp.where(z_odd, first, second)
            above = jnp.where(z_odd, second, first)
            below = pltpu.roll(below, lax.rem(LANES - e, LANES), 1)
            above = pltpu.roll(above, LANES - 1 - e, 1)
            below = jnp.where((lanes == 0) & jnp.logical_not(lowest), PENALTY * below, 0.0)
            above = jnp.where((lanes == LANES - 1) & jnp.logical_not(highest), PENALTY * above, 0.0)
            r_ref[e, pl.ds(a * nn, n), :] += below[:n]
            r_ref[e, pl.ds(a * nn + nn - n, n), :] += above[:n]
        return carry

    lax.fori_loop(0, e_total, slab, 0, unroll=HALO_UNROLL)
    for layer in range(e_total // span):
        first, second = c1[layer], c2[layer]
        r_ref[layer * span, pl.ds(0, nn), :] += PENALTY * jnp.where(odd, first, second)
        r_ref[layer * span + span - 1, pl.ds((n - 1) * nn, nn), :] += PENALTY * jnp.where(odd, second, first)


def correct(n, e_total, span, r_ref, u_ref, u_of, c1, c2, z1, z2):
    nn = n * n
    lanes = lane_ids(8)

    def slab(e, carry):
        lows, highs = carry
        u_ref[e] = u_of(e, r_ref[e])
        new_lows, new_highs = [], []
        for a in range(n):
            low = u_ref[e, pl.ds(a * nn, 8), :]
            high = u_ref[e, pl.ds(a * nn + nn - n, 8), :]
            here = lanes == e
            new_lows.append(jnp.where(here, pltpu.roll(low, e, 1), lows[a]))
            new_highs.append(jnp.where(here, pltpu.roll(high, e + 1, 1), highs[a]))
        return tuple(new_lows), tuple(new_highs)

    blank = tuple(jnp.zeros((8, LANES), F32) for _ in range(n))
    lows, highs = lax.fori_loop(0, e_total, slab, (blank, blank), unroll=HALO_UNROLL)
    odd = lax.rem(lax.axis_index("sector"), 2) == 1
    z_odd = lax.rem(lax.axis_index("block"), 2) == 1
    for a in range(n):
        z1[a] = jnp.where(z_odd, lows[a], highs[a])
        z2[a] = jnp.where(z_odd, highs[a], lows[a])
    for layer in range(e_total // span):
        low = u_ref[layer * span, pl.ds(0, nn), :]
        high = u_ref[layer * span + span - 1, pl.ds((n - 1) * nn, nn), :]
        c1[layer] = jnp.where(odd, low, high)
        c2[layer] = jnp.where(odd, high, low)


def subtract_operator(n, e_total, span, r_ref, u_ref, weights, jac_ref, count_ref):
    nn = n * n
    group = GROUP[n]
    lanes = lane_ids(8)

    def some(i, carry):
        first = i * group
        wide = jnp.concatenate([u_ref[first + j] for j in range(group)], axis=1)
        product = times(weights[...], wide)
        for j in range(group):
            e = first + j
            own = product[:, j * LANES : (j + 1) * LANES]
            r_ref[e] = r_ref[e] - jac_ref[pl.ds(e, 1), :] * own - count_ref[...] * u_ref[e]
            s = lax.rem(e, span)
            before = jnp.where(s > 0, PENALTY, 0.0)
            after = jnp.where(s < span - 1, PENALTY, 0.0)
            previous = u_ref[jnp.maximum(e - 1, 0), pl.ds((n - 1) * nn, nn), :]
            following = u_ref[jnp.minimum(e + 1, e_total - 1), pl.ds(0, nn), :]
            r_ref[e, pl.ds(0, nn), :] += before * previous
            r_ref[e, pl.ds((n - 1) * nn, nn), :] += after * following
            for a in range(n):
                low = u_ref[e, pl.ds(a * nn, 8), :]
                high = u_ref[e, pl.ds(a * nn + nn - n, 8), :]
                from_below = jnp.where(lanes > 0, PENALTY * pltpu.roll(high, 1, 1), 0.0)
                from_above = jnp.where(lanes < LANES - 1, PENALTY * pltpu.roll(low, LANES - 1, 1), 0.0)
                r_ref[e, pl.ds(a * nn, n), :] += from_below[:n]
                r_ref[e, pl.ds(a * nn + nn - n, n), :] += from_above[:n]
        return carry

    lax.fori_loop(0, e_total // group, some, 0, unroll=GROUP_UNROLL[n])


def face_shapes(n, layers):
    circ = jax.ShapeDtypeStruct((layers, n * n, LANES), F32)
    axial = jax.ShapeDtypeStruct((n, 8, LANES), F32)
    return [circ, circ, axial, axial]


def prepare(rotor, stator, mortar, stiff_fine, stiff_coarse, restrict_fine, restrict_coarse):
    rows, span = rotor.shape[0], rotor.shape[1]
    tall, wide = up(rows, 8), up(rows, 16)
    big, small = up(NF**3, 16), up(NC**3, 16)
    smalls = (mortar, stiff_fine, stiff_coarse, restrict_fine, restrict_coarse)

    def body(
        rotor_ref, stator_ref, mortar_in, kf_in, kc_in, rf_in, rc_in,
        rotor_out, stator_out, near1_out, near2_out, proj_out, back_out, proj_sum_out, back_sum_out,
        wf_out, wc_out, rfs_out, rcs_out, df_out, dc_out, mortar_ref, kf_ref, kc_ref, rf_ref, rc_ref, pad_ref, sem, small_sem,
    ):
        copies = []
        for f in range(span):
            for source, target in ((rotor_ref, rotor_out), (stator_ref, stator_out)):
                if tall > rows:
                    target[f, pl.ds(rows, tall - rows), :] = jnp.zeros((tall - rows, LANES), F32)
                copies.append(pltpu.make_async_copy(source.at[:, f, :], target.at[f, pl.ds(0, rows), :], sem))
        little = [
            pltpu.make_async_copy(source, target, small_sem)
            for source, target in (
                (mortar_in, mortar_ref), (kf_in, kf_ref), (kc_in, kc_ref), (rf_in, rf_ref), (rc_in, rc_ref)
            )
        ]
        for c in little + copies:
            c.start()
        row, col = node_rows((tall, LANES), 0), node_rows((tall, LANES), 1)
        comp_r, comp_c = digit(row, NF * NF, 4), digit(col, NF * NF, 5)
        rest_r, rest_c = row - NF * NF * comp_r, col - NF * NF * comp_c
        a_r, a_c = digit(rest_r, NF, NF - 1), digit(rest_c, NF, NF - 1)
        same = (comp_r == comp_c) & (rest_r - NF * a_r == rest_c - NF * a_c) & (row < rows) & (col < rows)
        ahead = jnp.where(same, a_r * NF + a_c, -1)
        flipped = jnp.where(same, a_c * NF + a_r, -1)
        for c in little:
            c.wait()

        def both_terms(pair):
            highs, lows = zip(*[parts_of(m) for m in pair])
            return jnp.concatenate(
                [jnp.concatenate([h, h], axis=1) for h in highs]
                + [jnp.concatenate([l, jnp.zeros_like(l)], axis=1) for l in lows],
                axis=0,
            )

        first_comp = (row < NF * NF) & (col < NF * NF)
        for found, out, sum_out in ((ahead, proj_out, proj_sum_out), (flipped, back_out, back_sum_out)):
            pair = []
            for which in range(2):
                total = jnp.zeros((tall, LANES), F32)
                matrix = mortar_ref[:, which, :]
                for i in range(NF):
                    for j in range(NF):
                        total = jnp.where(found == i * NF + j, matrix[i : i + 1, j : j + 1], total)
                pair.append(total)
            out[...] = both_terms([m[:, :wide] for m in pair])
            sum_out[...] = both_terms([jnp.where(first_comp, m, 0.0)[:SUM_ROWS, :SUM_ROWS] for m in pair])

        def padded(ref, height, width):
            pad_ref[...] = jnp.zeros_like(pad_ref)
            pad_ref[pl.ds(0, ref.shape[0]), pl.ds(0, ref.shape[1])] = ref[...]
            return pad_ref[pl.ds(0, height), :][:, :width]

        for ref, out, diag_out, size in ((kf_ref, wf_out, df_out, big), (kc_ref, wc_out, dc_out, small)):
            matrix = padded(ref, size, size)
            out[...] = stacked(matrix)
            row = lax.broadcasted_iota(jnp.int32, (size, size), 0)
            col = lax.broadcasted_iota(jnp.int32, (size, size), 1)
            diag = jnp.sum(jnp.where(row == col, matrix, 0.0), axis=1, keepdims=True)
            diag = jnp.where(row[:, :1] < ref.shape[0], diag, 1.0)
            diag_out[...] = jnp.broadcast_to(diag, (size, LANES))
        rfs_out[...] = stacked(padded(rf_ref, small, big))
        rcs_out[...] = stacked(padded(rc_ref, 16, small))
        for c in copies:
            c.wait()
        odd = lax.rem(lax.axis_index("sector"), 2) == 1
        near1_out[0] = jnp.where(odd, rotor_out[0], rotor_out[span - 1])
        near2_out[0] = jnp.where(odd, rotor_out[span - 1], rotor_out[0])

    return pl.pallas_call(
        body,
        out_shape=[
            jax.ShapeDtypeStruct((span, tall, LANES), F32),
            jax.ShapeDtypeStruct((span, tall, LANES), F32),
            jax.ShapeDtypeStruct((1, tall, LANES), F32),
            jax.ShapeDtypeStruct((1, tall, LANES), F32),
            jax.ShapeDtypeStruct((4 * tall, 2 * wide), BF16),
            jax.ShapeDtypeStruct((4 * tall, 2 * wide), BF16),
            jax.ShapeDtypeStruct((4 * SUM_ROWS, 2 * SUM_ROWS), BF16),
            jax.ShapeDtypeStruct((4 * SUM_ROWS, 2 * SUM_ROWS), BF16),
            jax.ShapeDtypeStruct((2 * big, 2 * big), BF16),
            jax.ShapeDtypeStruct((2 * small, 2 * small), BF16),
            jax.ShapeDtypeStruct((2 * small, 2 * big), BF16),
            jax.ShapeDtypeStruct((32, 2 * small), BF16),
            jax.ShapeDtypeStruct((big, LANES), F32),
            jax.ShapeDtypeStruct((small, LANES), F32),
        ],
        in_specs=[hbm_spec()] * 7,
        scratch_shapes=[pltpu.VMEM(m.shape, F32) for m in smalls]
        + [pltpu.VMEM((big, LANES), F32), pltpu.SemaphoreType.DMA, pltpu.SemaphoreType.DMA],
        compiler_params=params(),
        name="prepare",
    )(*in_hbm(rotor, stator, *smalls))


def apply_faces(matrix_ref, slab_of, count, tall, wide, y0, y1, unroll=1):
    group = 4
    fill = jnp.zeros((wide - tall, group * LANES), F32)

    def some(i, carry):
        first = group * i
        x = jnp.concatenate([slab_of(jnp.minimum(first + j, count - 1)) for j in range(group)], axis=1)
        if wide > tall:
            x = jnp.concatenate([x, fill], axis=0)
        high, low = parts_of(x)
        y = jnp.dot(matrix_ref[...], jnp.concatenate([high, low], axis=0), preferred_element_type=F32)
        a = y[:tall] + y[2 * tall : 3 * tall]
        b = y[tall : 2 * tall] + y[3 * tall :]
        for j in range(group):
            y0[first + j] = a[:, j * LANES : (j + 1) * LANES]
            y1[first + j] = b[:, j * LANES : (j + 1) * LANES]
        return carry

    lax.fori_loop(0, up(count, group) // group, some, 0, unroll=unroll)


def own_part(rotor, proj, jac, diag):
    span, tall = rotor.shape[0], rotor.shape[1]
    wide = proj.shape[1] // 2
    e_total, height = jac.shape[0], diag.shape[0]

    def body(r_in, proj_ref, jac_ref, diag_ref, kept, w_ref, y0, y1):
        apply_faces(proj_ref, lambda f: r_in[f], span, tall, wide, y0, y1)
        kept[0] = y0[0]
        kept[span] = y1[span - 1]

        def face(g, carry):
            kept[g] = y0[g] + y1[g - 1]
            return carry

        lax.fori_loop(1, span, face, 0)
        count = half_faces(NF, height)

        def weight(e, carry):
            w_ref[e] = DAMPING / (jac_ref[pl.ds(e, 1), :] * diag_ref[...] + count)
            return carry

        lax.fori_loop(0, e_total, weight, 0)

    return pl.pallas_call(
        body,
        out_shape=[
            jax.ShapeDtypeStruct((span + 1, tall, LANES), F32),
            jax.ShapeDtypeStruct((e_total, height, LANES), F32),
        ],
        scratch_shapes=[pltpu.VMEM((up(span, 4), tall, LANES), F32)] * 2,
        compiler_params=params(),
        cost_estimate=cost(2 * 10**9, 10 * 10**6),
        name="own_part",
    )(rotor, proj, jac, diag)


def join(far, near, near_s, far_s):
    few, many = far.shape[0], near.shape[0]
    window = jax.ShapeDtypeStruct((few + many,) + far.shape[1:], F32)

    def body(far_ref, near_ref, near_s_ref, far_s_ref, rotor_out, stator_out):
        def copy(source, out, first):
            def one(f, carry):
                out[first + f] = source[f]
                return carry

            lax.fori_loop(0, source.shape[0], one, 0)

        copy(far_ref, rotor_out, 0)
        copy(near_ref, rotor_out, few)
        copy(near_s_ref, stator_out, 0)
        copy(far_s_ref, stator_out, many)

    return pl.pallas_call(body, out_shape=[window, window], compiler_params=params(), name="join")(
        far, near, near_s, far_s
    )


def beside(near1_ref, near2_ref):
    odd = lax.rem(lax.axis_index("sector"), 2) == 1
    before = jnp.where(odd, near1_ref[0], near2_ref[0])
    after = jnp.where(odd, near2_ref[0], near1_ref[0])
    return before, after


def stator_out(shift, rotor_win, stator, proj):
    span, tall = stator.shape[0], stator.shape[1]
    wide = proj.shape[1] // 2
    rows = 4 * NF * NF

    def body(shift_ref, rw_ref, s_in, proj_ref, out, y0, y1, flux, sem):
        first = STEP - 1 - shift_ref[0]
        apply_faces(proj_ref, lambda f: rw_ref[first + f], span + 1, tall, wide, y0, y1)
        stores = []
        for g in range(span):
            flux[g] = s_in[g] - (y0[g + 1] + y1[g])
            c = pltpu.make_async_copy(flux.at[g, pl.ds(0, rows), :], out.at[:, g, :], sem)
            c.start()
            stores.append(c)
        for c in stores:
            c.wait()

    slabs = pltpu.VMEM((up(span + 1, 4), tall, LANES), F32)
    return pl.pallas_call(
        body,
        out_shape=jax.ShapeDtypeStruct((rows, span, LANES), F32),
        in_specs=[pl.BlockSpec(memory_space=pltpu.SMEM)] + [pl.BlockSpec()] * 3,
        out_specs=hbm_spec(),
        scratch_shapes=[slabs, slabs, pltpu.VMEM((span, tall, LANES), F32), pltpu.SemaphoreType.DMA],
        compiler_params=params(),
        cost_estimate=cost(10**9, 2 * 10**6),
        name="stator_out",
    )(shift, rotor_win, stator, proj)


def rotor_out(shift, stator_win, kept, near1, near2, proj, back):
    span, tall = kept.shape[0] - 1, kept.shape[1]
    wide = proj.shape[1] // 2
    rows = 4 * NF * NF

    def body(shift_ref, sw_ref, kept_ref, near1_ref, near2_ref, proj_ref, back_ref, out, y0, y1, flux, sides, sem):
        inner = shift_ref[0]
        before, after = beside(near1_ref, near2_ref)
        apply_faces(proj_ref, lambda f: jnp.where(f == 0, before, after), 2, tall, wide, y0, y1)
        sides[0] = y1[0]
        sides[1] = y0[1]

        def jump(f):
            own = kept_ref[f] + jnp.where(f == 0, sides[0], 0.0) + jnp.where(f == span, sides[1], 0.0)
            return sw_ref[inner + f] - own

        apply_faces(back_ref, jump, span + 1, tall, wide, y0, y1)
        stores = []
        for g in range(span):
            flux[g] = y0[g] + y1[g + 1]
            c = pltpu.make_async_copy(flux.at[g, pl.ds(0, rows), :], out.at[:, g, :], sem)
            c.start()
            stores.append(c)
        for c in stores:
            c.wait()

    slabs = pltpu.VMEM((up(span + 1, 4), tall, LANES), F32)
    return pl.pallas_call(
        body,
        out_shape=jax.ShapeDtypeStruct((rows, span, LANES), F32),
        in_specs=[pl.BlockSpec(memory_space=pltpu.SMEM)] + [pl.BlockSpec()] * 6,
        out_specs=hbm_spec(),
        scratch_shapes=[
            slabs, slabs, pltpu.VMEM((span, tall, LANES), F32), pltpu.VMEM((2, tall, LANES), F32), pltpu.SemaphoreType.DMA
        ],
        compiler_params=params(),
        cost_estimate=cost(10**9, 2 * 10**6),
        name="rotor_out",
    )(shift, stator_win, kept, near1, near2, proj, back)


def first_sweep(shift, rotor_win, stator_win, stator, kept, near1, near2, proj, back, source, w, jac, weights, layers):
    span = stator.shape[0]
    e_total = jac.shape[0]
    n, nn = NF, NF * NF
    nodes = n**3
    height = weights.shape[0] // 2
    group = 4

    def body(
        shift_ref, rw_ref, sw_ref, s_in, kept_ref, near1_ref, near2_ref, proj_ref, back_ref, source_ref, w_ref,
        jac_ref, w_mat, r_ref, u_ref, c1, c2, z1, z2, x, y0, y1, count_ref, in_sem,
    ):
        loads = [
            pltpu.make_async_copy(source_ref.at[:, e, :], r_ref.at[e, pl.ds(0, nodes), :], in_sem)
            for e in range(e_total)
        ]
        for c in loads:
            c.start()
        inner = shift_ref[0]
        first_rotor = STEP - 1 - inner
        count_ref[...] = half_faces(n, height)

        def summed(slab):
            return slab[:nn] + slab[3 * nn : 4 * nn]

        def sum_of(ref, f):
            return ref[f, pl.ds(0, nn), :] + ref[f, pl.ds(3 * nn, nn), :]

        def apply(matrix_ref, count):
            for i in range(0, count, group):
                high, low = parts_of(jnp.concatenate([x[i + j] for j in range(group)], axis=1))
                y = jnp.dot(matrix_ref[...], jnp.concatenate([high, low], axis=0), preferred_element_type=F32)
                a = y[:SUM_ROWS] + y[2 * SUM_ROWS : 3 * SUM_ROWS]
                b = y[SUM_ROWS : 2 * SUM_ROWS] + y[3 * SUM_ROWS :]
                for j in range(group):
                    y0[i + j] = a[:, j * LANES : (j + 1) * LANES]
                    y1[i + j] = b[:, j * LANES : (j + 1) * LANES]

        x[...] = jnp.zeros_like(x)
        for f in range(span + 1):
            x[f, pl.ds(0, nn), :] = sum_of(rw_ref, first_rotor + f)
        before, after = beside(near1_ref, near2_ref)
        x[span + 1, pl.ds(0, nn), :] = summed(before)
        x[span + 2, pl.ds(0, nn), :] = summed(after)
        apply(proj_ref, up(span + 3, group))
        inflow = [sum_of(s_in, g) - (y0[g + 1] + y1[g])[:nn] for g in range(span)]
        for c in loads:
            c.wait()
        for s in range(span):
            if height > nodes:
                for layer in range(layers):
                    r_ref[layer * span + s, pl.ds(nodes, height - nodes), :] = jnp.zeros((height - nodes, LANES), F32)
            r_ref[span + s, pl.ds(0, nn, stride=n), :] += inflow[s]
        for f in range(span + 1):
            own = sum_of(kept_ref, f)
            if f == 0:
                own = own + y1[span + 1, pl.ds(0, nn), :]
            if f == span:
                own = own + y0[span + 2, pl.ds(0, nn), :]
            x[f, pl.ds(0, nn), :] = sum_of(sw_ref, inner + f) - own
        apply(back_ref, up(span + 1, group))
        for s in range(span):
            r_ref[s, pl.ds(n - 1, nn, stride=n), :] += -(y0[s] + y1[s + 1])[:nn]
        correct(n, e_total, span, r_ref, u_ref, lambda e, r: r * w_ref[e], c1, c2, z1, z2)
        subtract_operator(n, e_total, span, r_ref, u_ref, w_mat, jac_ref, count_ref)

    whole = pl.BlockSpec()
    field = jax.ShapeDtypeStruct((e_total, height, LANES), F32)
    slabs = pltpu.VMEM((up(span + 3, group), SUM_ROWS, LANES), F32)
    return pl.pallas_call(
        body,
        out_shape=[field, field] + face_shapes(n, layers),
        in_specs=[pl.BlockSpec(memory_space=pltpu.SMEM)] + [whole] * 8 + [hbm_spec()] + [whole] * 3,
        scratch_shapes=[slabs] * 3 + [pltpu.VMEM((height, LANES), F32), pltpu.SemaphoreType.DMA],
        compiler_params=params(),
        cost_estimate=cost(2 * 10**9, 20 * 10**6),
        name="first_sweep",
    )(shift, rotor_win, stator_win, stator, kept, near1, near2, proj, back, *in_hbm(source), w, jac, weights)


def sweep(n, r, p, w, jac, weights, faces, layers, last):
    e_total, height = r.shape[0], r.shape[1]
    span = e_total // layers
    nodes = n**3

    def body(r_in, p_in, w_in, jac_ref, w_mat, h1, h2, g1, g2, p_out, r_ref, c1, c2, z1, z2, u_ref, p_keep, count_ref, sem):
        count_ref[...] = half_faces(n, height)
        p_ref = p_keep if last else p_out
        add_halo(n, e_total, span, lambda e: r_in[e], r_ref, h1, h2, g1, g2)

        def u_of(e, r_here):
            u = r_here * w_in[e]
            p_ref[e] = p_in[e] + u
            return u

        correct(n, e_total, span, r_ref, u_ref, u_of, c1, c2, z1, z2)
        stores = []
        if last:
            for e in range(e_total):
                c = pltpu.make_async_copy(p_ref.at[e, pl.ds(0, nodes), :], p_out.at[:, e, :], sem)
                c.start()
                stores.append(c)
        subtract_operator(n, e_total, span, r_ref, u_ref, w_mat, jac_ref, count_ref)
        for c in stores:
            c.wait()

    whole = pl.BlockSpec()
    field = jax.ShapeDtypeStruct((e_total, height, LANES), F32)
    kept = jax.ShapeDtypeStruct((nodes, e_total, LANES), F32) if last else field
    return pl.pallas_call(
        body,
        out_shape=[kept, field] + face_shapes(n, layers),
        out_specs=[any_spec() if last else whole] + [whole] * 5,
        scratch_shapes=[
            pltpu.VMEM((e_total, height, LANES), F32),
            pltpu.VMEM((e_total, height, LANES) if last else (1, 8, LANES), F32),
            pltpu.VMEM((height, LANES), F32),
            pltpu.SemaphoreType.DMA,
        ],
        compiler_params=params(),
        cost_estimate=cost(10**9 if n == NF else 10**8, 10 * 10**6),
    )(r, p, w, jac, weights, *faces)


def to_coarse(r, faces, restrict, jac, weights, diag, layers):
    e_total = r.shape[0]
    span = e_total // layers
    small = weights.shape[0] // 2
    n = NC
    group = 4

    def body(r_in, h1, h2, g1, g2, rest_ref, jac_ref, w_mat, diag_ref, rc_ref, u_ref, w_ref, c1, c2, z1, z2, r_fine, count_ref):
        count_ref[...] = half_faces(n, small)
        add_halo(NF, e_total, span, lambda e: r_in[e], r_fine, h1, h2, g1, g2)

        def some(i, carry):
            first = i * group
            wide = jnp.concatenate([r_fine[first + j] for j in range(group)], axis=1)
            product = times(rest_ref[...], wide)
            for j in range(group):
                rc_ref[first + j] = product[:, j * LANES : (j + 1) * LANES]
            return carry

        lax.fori_loop(0, e_total // group, some, 0, unroll=2)

        def u_of(e, r_here):
            w_here = DAMPING / (jac_ref[pl.ds(e, 1), :] * diag_ref[...] + count_ref[...])
            w_ref[e] = w_here
            return r_here * w_here

        correct(n, e_total, span, rc_ref, u_ref, u_of, c1, c2, z1, z2)
        subtract_operator(n, e_total, span, rc_ref, u_ref, w_mat, jac_ref, count_ref)

    field = jax.ShapeDtypeStruct((e_total, small, LANES), F32)
    return pl.pallas_call(
        body,
        out_shape=[field, field, field] + face_shapes(n, layers),
        scratch_shapes=[pltpu.VMEM(r.shape, F32), pltpu.VMEM((small, LANES), F32)],
        compiler_params=params(),
        cost_estimate=cost(5 * 10**8, 5 * 10**6),
        name="to_coarse",
    )(r, *faces, restrict, jac, weights, diag)


def to_coarsest(r, faces, restrict, layers):
    e_total = r.shape[0]
    span = e_total // layers
    group = 4

    def body(r_in, h1, h2, g1, g2, rest_ref, out_ref, r_done, kept, sem):
        add_halo(NC, e_total, span, lambda e: r_in[e], r_done, h1, h2, g1, g2)

        def some(i, carry):
            first = i * group
            wide = jnp.concatenate([r_done[first + j] for j in range(group)], axis=1)
            product = times(rest_ref[...], wide)
            for j in range(group):
                kept[first + j] = product[:LAST, j * LANES : (j + 1) * LANES]
            return carry

        lax.fori_loop(0, e_total // group, some, 0, unroll=8)
        stores = []
        for e in range(e_total):
            c = pltpu.make_async_copy(kept.at[e], out_ref.at[:, e, :], sem)
            c.start()
            stores.append(c)
        for c in stores:
            c.wait()

    whole = pl.BlockSpec()
    return pl.pallas_call(
        body,
        out_shape=jax.ShapeDtypeStruct((LAST, e_total, LANES), F32),
        in_specs=[whole] * 6,
        out_specs=any_spec(),
        scratch_shapes=[
            pltpu.VMEM(r.shape, F32),
            pltpu.VMEM((e_total, LAST, LANES), F32),
            pltpu.SemaphoreType.DMA,
        ],
        compiler_params=params(),
        cost_estimate=cost(5 * 10**7, 10**6),
        name="to_coarsest",
    )(r, *faces, restrict)


def move(x, axis, by):
    count = lax.axis_size(axis)
    return lax.ppermute(x, axis, [(i, (i + by) % count) for i in range(count)])


def swap(x, axis, odd_first):
    count = lax.axis_size(axis)
    pairs = []
    for i in range(count):
        ahead = (i % 2 == 0) != odd_first
        pairs.append((i, (i + 1) % count if ahead else (i - 1) % count))
    return lax.ppermute(x, axis, pairs)


def swap_inner(x, axis, other):
    count, beside = lax.axis_size(axis), lax.axis_size(other)
    pairs = []
    for j in range(beside):
        for i in range(count):
            to = i + 1 if i % 2 else i - 1
            target = (j, to) if 0 <= to < count else (j ^ 1, i)
            pairs.append((j * count + i, target[0] * count + target[1]))
    return lax.ppermute(x, (other, axis), pairs)


def exchange(faces):
    c1, c2, z1, z2 = faces
    c2 = swap(c2, "sector", True)
    z2 = swap_inner(z2, "block", "sector")
    z1 = swap(z1, "block", False)
    c1 = swap(c1, "sector", False)
    return c1, c2, z1, z2


def windows(rotor, stator, offset, own):
    span = rotor.shape[0]
    sectors = lax.axis_size("sector")
    buckets = span // STEP
    device, rest = lax.div(offset, span), lax.rem(offset, span)

    def branch(number):
        by, bucket = number // buckets, number % buckets
        many, few = span - STEP * bucket, STEP * (bucket + 1)

        def run(rotor, stator, own):
            near = move(rotor[:many], "sector", by)
            far = move(rotor[span - few :], "sector", by + 1)
            near_s = move(stator[span - many :], "sector", -by)
            far_s = move(stator[:few], "sector", -by - 1)
            kept, w = own_part(rotor, *own)
            return *join(far, near, near_s, far_s), kept, w

        return run

    choice = device * buckets + lax.div(rest, STEP)
    shift = lax.rem(rest, STEP).reshape(1)
    return shift, lax.switch(choice, [branch(i) for i in range(sectors * buckets)], rotor, stator, own)


def per_device(
    source, jacobian, stiff_fine, stiff_coarse, restrict_fine, restrict_coarse, mortar_proj, rotor_trace,
    stator_trace, offsets,
):
    layers, span, axial = jacobian.shape
    e_total = layers * span
    source_rows = source.reshape(source.shape[0], e_total, axial)
    jac = jacobian.reshape(e_total, axial)
    rotor_rows = rotor_trace.reshape(-1, span, axial)
    stator_rows = stator_trace.reshape(-1, span, axial)
    rotor, stator, near1, near2, proj, back, proj_sum, back_sum, wf, wc, rfs, rcs, df, dc = prepare(
        rotor_rows, stator_rows, mortar_proj.transpose(1, 0, 2), stiff_fine, stiff_coarse, restrict_fine, restrict_coarse
    )
    near2 = swap(near2, "sector", True)
    near1 = swap(near1, "sector", False)
    shift, (rotor_win, stator_win, kept, w) = windows(rotor, stator, offsets[0], (proj, jac, df))
    r, p, *faces = first_sweep(
        shift, rotor_win, stator_win, stator, kept, near1, near2, proj_sum, back_sum, source_rows, w, jac, wf, layers
    )
    sflux = stator_out(shift, rotor_win, stator, proj)
    rflux = rotor_out(shift, stator_win, kept, near1, near2, proj, back)
    p, r, *faces = sweep(NF, r, p, w, jac, wf, exchange(faces), layers, False)
    fine, r, *faces = sweep(NF, r, p, w, jac, wf, exchange(faces), layers, True)
    r, p, w, *faces = to_coarse(r, exchange(faces), rfs, jac, wc, dc, layers)
    p, r, *faces = sweep(NC, r, p, w, jac, wc, exchange(faces), layers, False)
    coarse, r, *faces = sweep(NC, r, p, w, jac, wc, exchange(faces), layers, True)
    coarsest = to_coarsest(r, exchange(faces), rcs, layers)
    shape = (layers, span, axial)
    return (
        sflux.reshape(stator_trace.shape),
        rflux.reshape(rotor_trace.shape),
        fine.reshape((-1,) + shape),
        coarse.reshape((-1,) + shape),
        coarsest.reshape((-1,) + shape),
    )


def solution(mesh):
    cell = P(None, None, "sector", "block")

    return jax.shard_map(
        per_device,
        mesh=mesh,
        in_specs=(cell, P(None, "sector", "block"), P(), P(), P(), P(), P(), cell, cell, P("block")),
        out_specs=(cell,) * 5,
        check_vma=False,
    )
```

```python
import jax
import jax.numpy as jnp
from jax import lax
from jax.experimental import pallas as pl
from jax.experimental.pallas import tpu as pltpu
from jax.sharding import PartitionSpec as P


F32 = jnp.float32
BF16 = jnp.bfloat16
DAMPING = 0.6
PENALTY = 0.5
LANES = 128
NF = 5
NC = 3
LAST = 8
STEP = 2
HALO_UNROLL = 32
GROUP = {NF: 4, NC: 16}
GROUP_UNROLL = {NF: 4, NC: 1}
VMEM_BYTES = 12 * 1024 * 1024


def up(value, unit):
    return (value + unit - 1) // unit * unit


def any_spec():
    return pl.BlockSpec(memory_space=pl.ANY)


def hbm_spec():
    return pl.BlockSpec(memory_space=pltpu.HBM)


def in_vmem(array):
    return pltpu.with_memory_space_constraint(array, pltpu.VMEM)


def in_hbm(*arrays):
    return tuple(pltpu.with_memory_space_constraint(x, pltpu.HBM) for x in arrays)


def params(**extra):
    return pltpu.CompilerParams(vmem_limit_bytes=VMEM_BYTES, **extra)


def cost(flops, data):
    return pl.CostEstimate(flops=flops, bytes_accessed=data, transcendentals=0)


def parts_of(x):
    high = x.astype(BF16)
    low = (x - high.astype(F32)).astype(BF16)
    return high, low


def stacked(matrix):
    high, low = parts_of(matrix)
    top = jnp.concatenate([high, high], axis=1)
    bottom = jnp.concatenate([low, jnp.zeros_like(low)], axis=1)
    return jnp.concatenate([top, bottom], axis=0)


def times(weights, x):
    rows = weights.shape[0] // 2
    high, low = parts_of(x)
    both = jnp.dot(weights, jnp.concatenate([high, low], axis=0), preferred_element_type=F32)
    return both[:rows] + both[rows:]


def lane_ids(rows):
    return lax.broadcasted_iota(jnp.int32, (rows, LANES), 1)


def node_rows(shape, axis):
    return lax.broadcasted_iota(jnp.int32, shape, axis)


def digit(index, unit, most):
    found = jnp.zeros_like(index)
    for k in range(1, most + 1):
        found += jnp.where(index >= k * unit, 1, 0)
    return found


def half_faces(n, height):
    row = node_rows((height, LANES), 0)
    a = digit(row, n * n, n)
    b = digit(row - n * n * a, n, n - 1)
    on_a = jnp.where((a == 0) | (a == n - 1), PENALTY, 0.0)
    on_b = jnp.where((b == 0) | (b == n - 1), PENALTY, 0.0)
    return jnp.where(row < n**3, on_a + on_b, 0.0)


def turn_plan(offset, span):
    total = span * lax.axis_size("sector")
    flipped = jnp.where(offset >= total // 2, 1, 0)
    return flipped, jnp.where(flipped == 1, total - 1 - offset, offset)


def smem_spec():
    return pl.BlockSpec(memory_space=pltpu.SMEM)


def add_halo(n, e_total, span, source_of, r_ref, c1, c2, z1, z2):
    nn = n * n
    odd = lax.rem(lax.axis_index("sector"), 2) == 1
    block = lax.axis_index("block")
    z_odd = lax.rem(block, 2) == 1
    lowest = block == 0
    highest = block == lax.axis_size("block") - 1
    lanes = lane_ids(8)

    def slab(e, carry):
        r_ref[e] = source_of(e)
        for a in range(n):
            first, second = z1[a], z2[a]
            below = jnp.where(z_odd, first, second)
            above = jnp.where(z_odd, second, first)
            below = pltpu.roll(below, lax.rem(LANES - e, LANES), 1)
            above = pltpu.roll(above, LANES - 1 - e, 1)
            below = jnp.where((lanes == 0) & jnp.logical_not(lowest), PENALTY * below, 0.0)
            above = jnp.where((lanes == LANES - 1) & jnp.logical_not(highest), PENALTY * above, 0.0)
            r_ref[e, pl.ds(a * nn, n), :] += below[:n]
            r_ref[e, pl.ds(a * nn + nn - n, n), :] += above[:n]
        return carry

    lax.fori_loop(0, e_total, slab, 0, unroll=HALO_UNROLL)
    for layer in range(e_total // span):
        first, second = c1[layer], c2[layer]
        r_ref[layer * span, pl.ds(0, nn), :] += PENALTY * jnp.where(odd, first, second)
        r_ref[layer * span + span - 1, pl.ds((n - 1) * nn, nn), :] += PENALTY * jnp.where(odd, second, first)


def correct(n, e_total, span, r_ref, u_ref, u_of, c1, c2, z1, z2):
    nn = n * n
    lanes = lane_ids(8)

    def slab(e, carry):
        lows, highs = carry
        u_ref[e] = u_of(e, r_ref[e])
        new_lows, new_highs = [], []
        for a in range(n):
            low = u_ref[e, pl.ds(a * nn, 8), :]
            high = u_ref[e, pl.ds(a * nn + nn - n, 8), :]
            here = lanes == e
            new_lows.append(jnp.where(here, pltpu.roll(low, e, 1), lows[a]))
            new_highs.append(jnp.where(here, pltpu.roll(high, e + 1, 1), highs[a]))
        return tuple(new_lows), tuple(new_highs)

    blank = tuple(jnp.zeros((8, LANES), F32) for _ in range(n))
    lows, highs = lax.fori_loop(0, e_total, slab, (blank, blank), unroll=HALO_UNROLL)
    odd = lax.rem(lax.axis_index("sector"), 2) == 1
    z_odd = lax.rem(lax.axis_index("block"), 2) == 1
    for a in range(n):
        z1[a] = jnp.where(z_odd, lows[a], highs[a])
        z2[a] = jnp.where(z_odd, highs[a], lows[a])
    for layer in range(e_total // span):
        low = u_ref[layer * span, pl.ds(0, nn), :]
        high = u_ref[layer * span + span - 1, pl.ds((n - 1) * nn, nn), :]
        c1[layer] = jnp.where(odd, low, high)
        c2[layer] = jnp.where(odd, high, low)


def subtract_operator(n, e_total, span, r_ref, u_ref, weights, jac_ref, count_ref):
    nn = n * n
    group = GROUP[n]
    lanes = lane_ids(8)

    def some(i, carry):
        first = i * group
        wide = jnp.concatenate([u_ref[first + j] for j in range(group)], axis=1)
        product = times(weights[...], wide)
        for j in range(group):
            e = first + j
            own = product[:, j * LANES : (j + 1) * LANES]
            r_ref[e] = r_ref[e] - jac_ref[pl.ds(e, 1), :] * own - count_ref[...] * u_ref[e]
            s = lax.rem(e, span)
            before = jnp.where(s > 0, PENALTY, 0.0)
            after = jnp.where(s < span - 1, PENALTY, 0.0)
            previous = u_ref[jnp.maximum(e - 1, 0), pl.ds((n - 1) * nn, nn), :]
            following = u_ref[jnp.minimum(e + 1, e_total - 1), pl.ds(0, nn), :]
            r_ref[e, pl.ds(0, nn), :] += before * previous
            r_ref[e, pl.ds((n - 1) * nn, nn), :] += after * following
            for a in range(n):
                low = u_ref[e, pl.ds(a * nn, 8), :]
                high = u_ref[e, pl.ds(a * nn + nn - n, 8), :]
                from_below = jnp.where(lanes > 0, PENALTY * pltpu.roll(high, 1, 1), 0.0)
                from_above = jnp.where(lanes < LANES - 1, PENALTY * pltpu.roll(low, LANES - 1, 1), 0.0)
                r_ref[e, pl.ds(a * nn, n), :] += from_below[:n]
                r_ref[e, pl.ds(a * nn + nn - n, n), :] += from_above[:n]
        return carry

    lax.fori_loop(0, e_total // group, some, 0, unroll=GROUP_UNROLL[n])


def face_shapes(n, layers):
    circ = jax.ShapeDtypeStruct((layers, n * n, LANES), F32)
    axial = jax.ShapeDtypeStruct((n, 8, LANES), F32)
    return [circ, circ, axial, axial]


def prepare(offsets, rotor, stator, mortar, stiff_fine, stiff_coarse, restrict_fine, restrict_coarse):
    rows, span = rotor.shape[0], rotor.shape[1]
    tall, wide = up(rows, 8), up(rows, 16)
    big, small = up(NF**3, 16), up(NC**3, 16)
    smalls = (mortar, stiff_fine, stiff_coarse, restrict_fine, restrict_coarse)

    def body(
        offset_ref, rotor_ref, stator_ref, mortar_in, kf_in, kc_in, rf_in, rc_in,
        pair_out, near1_out, near2_out, proj_out, back_out, wf_out, wc_out, rfs_out, rcs_out, df_out, dc_out,
        mortar_ref, kf_ref, kc_ref, rf_ref, rc_ref, pad_ref, sem, small_sem,
    ):
        flipped, _ = turn_plan(offset_ref[0], span)
        copies = []
        for f in range(span):
            for source, first in ((rotor_ref, span * flipped), (stator_ref, span - span * flipped)):
                if tall > rows:
                    pair_out[first + f, pl.ds(rows, tall - rows), :] = jnp.zeros((tall - rows, LANES), F32)
                copies.append(
                    pltpu.make_async_copy(source.at[:, f, :], pair_out.at[first + f, pl.ds(0, rows), :], sem)
                )
        little = [
            pltpu.make_async_copy(source, target, small_sem)
            for source, target in (
                (mortar_in, mortar_ref), (kf_in, kf_ref), (kc_in, kc_ref), (rf_in, rf_ref), (rc_in, rc_ref)
            )
        ]
        for c in little + copies:
            c.start()
        row, col = node_rows((tall, LANES), 0), node_rows((tall, LANES), 1)
        comp_r, comp_c = digit(row, NF * NF, 4), digit(col, NF * NF, 5)
        rest_r, rest_c = row - NF * NF * comp_r, col - NF * NF * comp_c
        a_r, a_c = digit(rest_r, NF, NF - 1), digit(rest_c, NF, NF - 1)
        same = (comp_r == comp_c) & (rest_r - NF * a_r == rest_c - NF * a_c) & (row < rows) & (col < rows)
        ahead = jnp.where(same, a_r * NF + a_c, -1)
        turned = jnp.where(same, a_c * NF + a_r, -1)
        for c in little:
            c.wait()

        def both_terms(pair):
            highs, lows = zip(*[parts_of(m) for m in pair])
            return jnp.concatenate(
                [jnp.concatenate([h, h], axis=1) for h in highs]
                + [jnp.concatenate([l, jnp.zeros_like(l)], axis=1) for l in lows],
                axis=0,
            )

        for found, out in ((ahead, proj_out), (turned, back_out)):
            pair = []
            for which in range(2):
                total = jnp.zeros((tall, LANES), F32)
                matrix = mortar_ref[:, which, :]
                for i in range(NF):
                    for j in range(NF):
                        total = jnp.where(found == i * NF + j, matrix[i : i + 1, j : j + 1], total)
                pair.append(total)
            out[...] = both_terms([m[:, :wide] for m in pair])

        def padded(ref, height, width):
            pad_ref[...] = jnp.zeros_like(pad_ref)
            pad_ref[pl.ds(0, ref.shape[0]), pl.ds(0, ref.shape[1])] = ref[...]
            return pad_ref[pl.ds(0, height), :][:, :width]

        for ref, out, diag_out, size in ((kf_ref, wf_out, df_out, big), (kc_ref, wc_out, dc_out, small)):
            matrix = padded(ref, size, size)
            out[...] = stacked(matrix)
            row = lax.broadcasted_iota(jnp.int32, (size, size), 0)
            col = lax.broadcasted_iota(jnp.int32, (size, size), 1)
            diag = jnp.sum(jnp.where(row == col, matrix, 0.0), axis=1, keepdims=True)
            diag = jnp.where(row[:, :1] < ref.shape[0], diag, 1.0)
            diag_out[...] = jnp.broadcast_to(diag, (size, LANES))
        rfs_out[...] = stacked(padded(rf_ref, small, big))
        rcs_out[...] = stacked(padded(rc_ref, 16, small))
        for c in copies:
            c.wait()
        odd = lax.rem(lax.axis_index("sector"), 2) == 1
        lowest, highest = pair_out[span * flipped], pair_out[span * flipped + span - 1]
        near1_out[0] = jnp.where(odd, lowest, highest)
        near2_out[0] = jnp.where(odd, highest, lowest)

    return pl.pallas_call(
        body,
        out_shape=[
            jax.ShapeDtypeStruct((2 * span, tall, LANES), F32),
            jax.ShapeDtypeStruct((1, tall, LANES), F32),
            jax.ShapeDtypeStruct((1, tall, LANES), F32),
            jax.ShapeDtypeStruct((4 * tall, 2 * wide), BF16),
            jax.ShapeDtypeStruct((4 * tall, 2 * wide), BF16),
            jax.ShapeDtypeStruct((2 * big, 2 * big), BF16),
            jax.ShapeDtypeStruct((2 * small, 2 * small), BF16),
            jax.ShapeDtypeStruct((2 * small, 2 * big), BF16),
            jax.ShapeDtypeStruct((32, 2 * small), BF16),
            jax.ShapeDtypeStruct((big, LANES), F32),
            jax.ShapeDtypeStruct((small, LANES), F32),
        ],
        in_specs=[smem_spec()] + [hbm_spec()] * 7,
        scratch_shapes=[pltpu.VMEM(m.shape, F32) for m in smalls]
        + [pltpu.VMEM((big, LANES), F32), pltpu.SemaphoreType.DMA, pltpu.SemaphoreType.DMA],
        compiler_params=params(),
        name="prepare",
    )(offsets, *in_hbm(rotor, stator, *smalls))


def apply_faces(matrix_ref, slab_of, count, tall, wide, y0, y1, unrolled):
    group = 4
    fill = jnp.zeros((wide - tall, group * LANES), F32)

    def some(i, carry):
        first = group * i
        least = min if unrolled else jnp.minimum
        x = jnp.concatenate([slab_of(least(first + j, count - 1)) for j in range(group)], axis=1)
        if wide > tall:
            x = jnp.concatenate([x, fill], axis=0)
        high, low = parts_of(x)
        y = jnp.dot(matrix_ref[...], jnp.concatenate([high, low], axis=0), preferred_element_type=F32)
        a = y[:tall] + y[2 * tall : 3 * tall]
        b = y[tall : 2 * tall] + y[3 * tall :]
        for j in range(group):
            y0[first + j] = a[:, j * LANES : (j + 1) * LANES]
            y1[first + j] = b[:, j * LANES : (j + 1) * LANES]
        return carry

    if unrolled:
        for i in range(up(count, group) // group):
            some(i, 0)
    else:
        lax.fori_loop(0, up(count, group) // group, some, 0)


def own_part(offsets, pair, proj, jac, diag):
    span, tall = pair.shape[0] // 2, pair.shape[1]
    wide = proj.shape[1] // 2
    e_total, height = jac.shape[0], diag.shape[0]

    def body(offset_ref, pair_ref, proj_ref, jac_ref, diag_ref, kept, w_ref, y0, y1):
        first = span * turn_plan(offset_ref[0], span)[0]
        apply_faces(proj_ref, lambda f: pair_ref[first + f], span, tall, wide, y0, y1, False)
        kept[0] = y0[0]
        kept[span] = y1[span - 1]

        def face(g, carry):
            kept[g] = y0[g] + y1[g - 1]
            return carry

        lax.fori_loop(1, span, face, 0)
        count = half_faces(NF, height)

        def weight(e, carry):
            w_ref[e] = DAMPING / (jac_ref[pl.ds(e, 1), :] * diag_ref[...] + count)
            return carry

        lax.fori_loop(0, e_total, weight, 0)

    return pl.pallas_call(
        body,
        out_shape=[
            jax.ShapeDtypeStruct((span + 1, tall, LANES), F32),
            jax.ShapeDtypeStruct((e_total, height, LANES), F32),
        ],
        in_specs=[smem_spec()] + [pl.BlockSpec()] * 4,
        scratch_shapes=[pltpu.VMEM((up(span, 4), tall, LANES), F32)] * 2,
        compiler_params=params(),
        cost_estimate=cost(2 * 10**9, 10 * 10**6),
        name="own_part",
    )(offsets, pair, proj, jac, diag)


def join(far, near, near_back, far_back):
    few, many = far.shape[0], near.shape[0]
    reach = few + many

    def body(far_ref, near_ref, near_back_ref, far_back_ref, out):
        def copy(source, first):
            def one(f, carry):
                out[first + f] = source[f]
                return carry

            lax.fori_loop(0, source.shape[0], one, 0)

        copy(far_ref, 0)
        copy(near_ref, few)
        copy(near_back_ref, reach)
        copy(far_back_ref, reach + many)

    return pl.pallas_call(
        body,
        out_shape=jax.ShapeDtypeStruct((2 * reach,) + far.shape[1:], F32),
        compiler_params=params(),
        name="join",
    )(far, near, near_back, far_back)


def first_sweep(offsets, wins, pair, kept, near1, near2, proj, back, source, w, jac, weights, layers):
    span, tall = pair.shape[0] // 2, pair.shape[1]
    reach = wins.shape[0] // 2
    wide = back.shape[1] // 2
    rows = 4 * NF * NF
    e_total = jac.shape[0]
    n, nn = NF, NF * NF
    nodes = n**3
    height = weights.shape[0] // 2

    def body(
        offset_ref, wins_ref, pair_ref, kept_ref, near1_ref, near2_ref, proj_ref, back_ref, source_ref, w_ref,
        jac_ref, w_mat, sflux_out, rflux_out, r_ref, u_ref, c1, c2, z1, z2,
        y0, y1, x0, x1, sflux, rflux, count_ref, in_sem, out_sem,
    ):
        loads = [
            pltpu.make_async_copy(source_ref.at[:, e, :], r_ref.at[e, pl.ds(0, nodes), :], in_sem)
            for e in range(e_total)
        ]
        for c in loads:
            c.start()
        flipped, steps = turn_plan(offset_ref[0], span)
        inner = lax.rem(steps, STEP)
        ahead, behind = STEP - 1 - inner, reach + inner
        first_rotor = jnp.where(flipped == 1, behind, ahead)
        first_stator = jnp.where(flipped == 1, ahead, behind)
        own_stator = span - span * flipped
        count_ref[...] = half_faces(n, height)
        odd = lax.rem(lax.axis_index("sector"), 2) == 1

        def rotor_slab(f):
            if f <= span:
                return wins_ref[first_rotor + f]
            one, two = near1_ref[0], near2_ref[0]
            return jnp.where(odd, one, two) if f == span + 1 else jnp.where(odd, two, one)

        def jump(f):
            own = kept_ref[f]
            if f == 0:
                own = own + x1[span + 1]
            if f == span:
                own = own + x0[span + 2]
            return wins_ref[first_stator + f] - own

        apply_faces(proj_ref, rotor_slab, span + 3, tall, wide, x0, x1, True)
        apply_faces(back_ref, jump, span + 1, tall, wide, y0, y1, True)
        stores = []
        for s in range(span):
            sflux[s] = pair_ref[own_stator + s] - (x0[s + 1] + x1[s])
            rflux[s] = y0[s] + y1[s + 1]
            for buffer, out in ((sflux, sflux_out), (rflux, rflux_out)):
                c = pltpu.make_async_copy(buffer.at[s, pl.ds(0, rows), :], out.at[:, s, :], out_sem)
                c.start()
                stores.append(c)
        for c in loads:
            c.wait()
        for s in range(span):
            if height > nodes:
                for layer in range(layers):
                    r_ref[layer * span + s, pl.ds(nodes, height - nodes), :] = jnp.zeros((height - nodes, LANES), F32)
            inflow = sflux[s, pl.ds(0, nn), :] + sflux[s, pl.ds(3 * nn, nn), :]
            outflow = rflux[s, pl.ds(0, nn), :] + rflux[s, pl.ds(3 * nn, nn), :]
            r_ref[span + s, pl.ds(0, nn, stride=n), :] += inflow
            r_ref[s, pl.ds(n - 1, nn, stride=n), :] += -outflow
        correct(n, e_total, span, r_ref, u_ref, lambda e, r: r * w_ref[e], c1, c2, z1, z2)
        subtract_operator(n, e_total, span, r_ref, u_ref, w_mat, jac_ref, count_ref)
        for c in stores:
            c.wait()

    whole = pl.BlockSpec()
    field = jax.ShapeDtypeStruct((e_total, height, LANES), F32)
    trace = jax.ShapeDtypeStruct((rows, span, LANES), F32)
    slabs = pltpu.VMEM((up(span + 3, 4), tall, LANES), F32)
    return pl.pallas_call(
        body,
        out_shape=[trace, trace, field, field] + face_shapes(n, layers),
        in_specs=[smem_spec()] + [whole] * 7 + [hbm_spec()] + [whole] * 3,
        out_specs=[hbm_spec()] * 2 + [whole] * 6,
        scratch_shapes=[slabs] * 4
        + [
            pltpu.VMEM((span, tall, LANES), F32),
            pltpu.VMEM((span, tall, LANES), F32),
            pltpu.VMEM((height, LANES), F32),
            pltpu.SemaphoreType.DMA,
            pltpu.SemaphoreType.DMA,
        ],
        compiler_params=params(),
        cost_estimate=cost(2 * 10**9, 20 * 10**6),
        name="first_sweep",
    )(offsets, in_vmem(wins), pair, kept, near1, near2, proj, back, *in_hbm(source), in_vmem(w), jac, weights)


def sweep(n, r, p, w, jac, weights, faces, layers, last):
    e_total, height = r.shape[0], r.shape[1]
    span = e_total // layers
    nodes = n**3

    def body(r_in, p_in, w_in, jac_ref, w_mat, h1, h2, g1, g2, p_out, r_ref, c1, c2, z1, z2, u_ref, p_keep, count_ref, sem):
        count_ref[...] = half_faces(n, height)
        p_ref = p_keep if last else p_out
        add_halo(n, e_total, span, lambda e: r_in[e], r_ref, h1, h2, g1, g2)

        def u_of(e, r_here):
            u = r_here * w_in[e]
            p_ref[e] = p_in[e] + u
            return u

        correct(n, e_total, span, r_ref, u_ref, u_of, c1, c2, z1, z2)
        stores = []
        if last:
            for e in range(e_total):
                c = pltpu.make_async_copy(p_ref.at[e, pl.ds(0, nodes), :], p_out.at[:, e, :], sem)
                c.start()
                stores.append(c)
        subtract_operator(n, e_total, span, r_ref, u_ref, w_mat, jac_ref, count_ref)
        for c in stores:
            c.wait()

    whole = pl.BlockSpec()
    field = jax.ShapeDtypeStruct((e_total, height, LANES), F32)
    kept = jax.ShapeDtypeStruct((nodes, e_total, LANES), F32) if last else field
    return pl.pallas_call(
        body,
        out_shape=[kept, field] + face_shapes(n, layers),
        out_specs=[any_spec() if last else whole] + [whole] * 5,
        scratch_shapes=[
            pltpu.VMEM((e_total, height, LANES), F32),
            pltpu.VMEM((e_total, height, LANES) if last else (1, 8, LANES), F32),
            pltpu.VMEM((height, LANES), F32),
            pltpu.SemaphoreType.DMA,
        ],
        compiler_params=params(),
        cost_estimate=cost(10**9 if n == NF else 10**8, 10 * 10**6),
    )(r, p, w, jac, weights, *faces)


def to_coarse(r, faces, restrict, jac, weights, diag, layers):
    e_total = r.shape[0]
    span = e_total // layers
    small = weights.shape[0] // 2
    n = NC
    group = 4

    def body(r_in, h1, h2, g1, g2, rest_ref, jac_ref, w_mat, diag_ref, rc_ref, u_ref, w_ref, c1, c2, z1, z2, r_fine, count_ref):
        count_ref[...] = half_faces(n, small)
        add_halo(NF, e_total, span, lambda e: r_in[e], r_fine, h1, h2, g1, g2)

        def some(i, carry):
            first = i * group
            wide = jnp.concatenate([r_fine[first + j] for j in range(group)], axis=1)
            product = times(rest_ref[...], wide)
            for j in range(group):
                rc_ref[first + j] = product[:, j * LANES : (j + 1) * LANES]
            return carry

        lax.fori_loop(0, e_total // group, some, 0, unroll=2)

        def u_of(e, r_here):
            w_here = DAMPING / (jac_ref[pl.ds(e, 1), :] * diag_ref[...] + count_ref[...])
            w_ref[e] = w_here
            return r_here * w_here

        correct(n, e_total, span, rc_ref, u_ref, u_of, c1, c2, z1, z2)
        subtract_operator(n, e_total, span, rc_ref, u_ref, w_mat, jac_ref, count_ref)

    field = jax.ShapeDtypeStruct((e_total, small, LANES), F32)
    return pl.pallas_call(
        body,
        out_shape=[field, field, field] + face_shapes(n, layers),
        scratch_shapes=[pltpu.VMEM(r.shape, F32), pltpu.VMEM((small, LANES), F32)],
        compiler_params=params(),
        cost_estimate=cost(5 * 10**8, 5 * 10**6),
        name="to_coarse",
    )(r, *faces, restrict, jac, weights, diag)


def to_coarsest(r, faces, restrict, layers):
    e_total = r.shape[0]
    span = e_total // layers
    group = 4

    def body(r_in, h1, h2, g1, g2, rest_ref, out_ref, r_done, kept, sem):
        add_halo(NC, e_total, span, lambda e: r_in[e], r_done, h1, h2, g1, g2)

        def some(i, carry):
            first = i * group
            wide = jnp.concatenate([r_done[first + j] for j in range(group)], axis=1)
            product = times(rest_ref[...], wide)
            for j in range(group):
                kept[first + j] = product[:LAST, j * LANES : (j + 1) * LANES]
            return carry

        lax.fori_loop(0, e_total // group, some, 0, unroll=8)
        stores = []
        for e in range(e_total):
            c = pltpu.make_async_copy(kept.at[e], out_ref.at[:, e, :], sem)
            c.start()
            stores.append(c)
        for c in stores:
            c.wait()

    whole = pl.BlockSpec()
    return pl.pallas_call(
        body,
        out_shape=jax.ShapeDtypeStruct((LAST, e_total, LANES), F32),
        in_specs=[whole] * 6,
        out_specs=any_spec(),
        scratch_shapes=[
            pltpu.VMEM(r.shape, F32),
            pltpu.VMEM((e_total, LAST, LANES), F32),
            pltpu.SemaphoreType.DMA,
        ],
        compiler_params=params(),
        cost_estimate=cost(5 * 10**7, 10**6),
        name="to_coarsest",
    )(r, *faces, restrict)


def move(x, axis, by):
    count = lax.axis_size(axis)
    return lax.ppermute(x, axis, [(i, (i + by) % count) for i in range(count)])


def swap(x, axis, odd_first):
    count = lax.axis_size(axis)
    pairs = []
    for i in range(count):
        ahead = (i % 2 == 0) != odd_first
        pairs.append((i, (i + 1) % count if ahead else (i - 1) % count))
    return lax.ppermute(x, axis, pairs)


def swap_inner(x, axis, other):
    count, beside = lax.axis_size(axis), lax.axis_size(other)
    pairs = []
    for j in range(beside):
        for i in range(count):
            to = i + 1 if i % 2 else i - 1
            target = (j, to) if 0 <= to < count else (j ^ 1, i)
            pairs.append((j * count + i, target[0] * count + target[1]))
    return lax.ppermute(x, (other, axis), pairs)


def exchange(faces):
    c1, c2, z1, z2 = faces
    c2 = swap(c2, "sector", True)
    z2 = swap_inner(z2, "block", "sector")
    z1 = swap(z1, "block", False)
    c1 = swap(c1, "sector", False)
    return c1, c2, z1, z2


def windows(pair, offsets, own):
    span = pair.shape[0] // 2
    buckets = span // STEP
    _, steps = turn_plan(offsets[0], span)

    def branch(number):
        by, bucket = number // buckets, number % buckets
        many, few = span - STEP * bucket, STEP * (bucket + 1)

        def run(pair, offsets, own):
            near = move(pair[:many], "sector", by)
            far = move(pair[span - few : span], "sector", by + 1)
            near_back = move(pair[2 * span - many :], "sector", -by)
            far_back = move(pair[span : span + few], "sector", -by - 1)
            kept, w = own_part(offsets, pair, *own)
            return join(far, near, near_back, far_back), kept, w

        return run

    branches = [branch(i) for i in range(lax.axis_size("sector") // 2 * buckets)]
    return lax.switch(lax.div(steps, STEP), branches, pair, offsets, own)


def per_device(
    source, jacobian, stiff_fine, stiff_coarse, restrict_fine, restrict_coarse, mortar_proj, rotor_trace,
    stator_trace, offsets,
):
    layers, span, axial = jacobian.shape
    e_total = layers * span
    source_rows = source.reshape(source.shape[0], e_total, axial)
    jac = jacobian.reshape(e_total, axial)
    rotor_rows = rotor_trace.reshape(-1, span, axial)
    stator_rows = stator_trace.reshape(-1, span, axial)
    pair, near1, near2, proj, back, wf, wc, rfs, rcs, df, dc = prepare(
        offsets, rotor_rows, stator_rows, mortar_proj.transpose(1, 0, 2),
        stiff_fine, stiff_coarse, restrict_fine, restrict_coarse,
    )
    near2 = swap(near2, "sector", True)
    near1 = swap(near1, "sector", False)
    wins, kept, w = windows(pair, offsets, (proj, jac, df))
    sflux, rflux, r, p, *faces = first_sweep(
        offsets, wins, pair, kept, near1, near2, proj, back, source_rows, w, jac, wf, layers
    )
    p, r, *faces = sweep(NF, r, p, w, jac, wf, exchange(faces), layers, False)
    fine, r, *faces = sweep(NF, r, p, w, jac, wf, exchange(faces), layers, True)
    r, p, w, *faces = to_coarse(r, exchange(faces), rfs, jac, wc, dc, layers)
    p, r, *faces = sweep(NC, r, p, w, jac, wc, exchange(faces), layers, False)
    coarse, r, *faces = sweep(NC, r, p, w, jac, wc, exchange(faces), layers, True)
    coarsest = to_coarsest(r, exchange(faces), rcs, layers)
    shape = (layers, span, axial)
    return (
        sflux.reshape(stator_trace.shape),
        rflux.reshape(rotor_trace.shape),
        fine.reshape((-1,) + shape),
        coarse.reshape((-1,) + shape),
        coarsest.reshape((-1,) + shape),
    )


def solution(mesh):
    cell = P(None, None, "sector", "block")

    return jax.shard_map(
        per_device,
        mesh=mesh,
        in_specs=(cell, P(None, "sector", "block"), P(), P(), P(), P(), P(), cell, cell, P("block")),
        out_specs=(cell,) * 5,
        check_vma=False,
    )
```

```python
import jax
import jax.numpy as jnp
from jax import lax
from jax.experimental import pallas as pl
from jax.experimental.pallas import tpu as pltpu
from jax.sharding import PartitionSpec as P


F32 = jnp.float32
BF16 = jnp.bfloat16
DAMPING = 0.6
PENALTY = 0.5
LANES = 128
NF = 5
NC = 3
LAST = 8
STEP = 2
HALO_UNROLL = 32
GROUP = {NF: 4, NC: 16}
GROUP_UNROLL = {NF: 4, NC: 1}
VMEM_BYTES = 12 * 1024 * 1024


def up(value, unit):
    return (value + unit - 1) // unit * unit


def any_spec():
    return pl.BlockSpec(memory_space=pl.ANY)


def hbm_spec():
    return pl.BlockSpec(memory_space=pltpu.HBM)


def in_vmem(array):
    return pltpu.with_memory_space_constraint(array, pltpu.VMEM)


def in_hbm(*arrays):
    return tuple(pltpu.with_memory_space_constraint(x, pltpu.HBM) for x in arrays)


def params(**extra):
    return pltpu.CompilerParams(vmem_limit_bytes=VMEM_BYTES, **extra)


def cost(flops, data):
    return pl.CostEstimate(flops=flops, bytes_accessed=data, transcendentals=0)


def parts_of(x):
    high = x.astype(BF16)
    low = (x - high.astype(F32)).astype(BF16)
    return high, low


def stacked(matrix):
    high, low = parts_of(matrix)
    top = jnp.concatenate([high, high], axis=1)
    bottom = jnp.concatenate([low, jnp.zeros_like(low)], axis=1)
    return jnp.concatenate([top, bottom], axis=0)


def times(weights, x):
    rows = weights.shape[0] // 2
    high, low = parts_of(x)
    both = jnp.dot(weights, jnp.concatenate([high, low], axis=0), preferred_element_type=F32)
    return both[:rows] + both[rows:]


def lane_ids(rows):
    return lax.broadcasted_iota(jnp.int32, (rows, LANES), 1)


def node_rows(shape, axis):
    return lax.broadcasted_iota(jnp.int32, shape, axis)


def digit(index, unit, most):
    found = jnp.zeros_like(index)
    for k in range(1, most + 1):
        found += jnp.where(index >= k * unit, 1, 0)
    return found


def half_faces(n, height):
    row = node_rows((height, LANES), 0)
    a = digit(row, n * n, n)
    b = digit(row - n * n * a, n, n - 1)
    on_a = jnp.where((a == 0) | (a == n - 1), PENALTY, 0.0)
    on_b = jnp.where((b == 0) | (b == n - 1), PENALTY, 0.0)
    return jnp.where(row < n**3, on_a + on_b, 0.0)


def turn_plan(offset, span):
    total = span * lax.axis_size("sector")
    flipped = jnp.where(offset >= total // 2, 1, 0)
    return flipped, jnp.where(flipped == 1, total - 1 - offset, offset)


def smem_spec():
    return pl.BlockSpec(memory_space=pltpu.SMEM)


def add_halo(n, e_total, span, source_of, r_ref, c1, c2, z1, z2):
    nn = n * n
    odd = lax.rem(lax.axis_index("sector"), 2) == 1
    block = lax.axis_index("block")
    z_odd = lax.rem(block, 2) == 1
    lowest = block == 0
    highest = block == lax.axis_size("block") - 1
    lanes = lane_ids(8)

    def slab(e, carry):
        r_ref[e] = source_of(e)
        for a in range(n):
            first, second = z1[a], z2[a]
            below = jnp.where(z_odd, first, second)
            above = jnp.where(z_odd, second, first)
            below = pltpu.roll(below, lax.rem(LANES - e, LANES), 1)
            above = pltpu.roll(above, LANES - 1 - e, 1)
            below = jnp.where((lanes == 0) & jnp.logical_not(lowest), PENALTY * below, 0.0)
            above = jnp.where((lanes == LANES - 1) & jnp.logical_not(highest), PENALTY * above, 0.0)
            r_ref[e, pl.ds(a * nn, n), :] += below[:n]
            r_ref[e, pl.ds(a * nn + nn - n, n), :] += above[:n]
        return carry

    lax.fori_loop(0, e_total, slab, 0, unroll=HALO_UNROLL)
    for layer in range(e_total // span):
        first, second = c1[layer], c2[layer]
        r_ref[layer * span, pl.ds(0, nn), :] += PENALTY * jnp.where(odd, first, second)
        r_ref[layer * span + span - 1, pl.ds((n - 1) * nn, nn), :] += PENALTY * jnp.where(odd, second, first)


def correct(n, e_total, span, r_ref, u_ref, u_of, c1, c2, z1, z2):
    nn = n * n
    lanes = lane_ids(8)

    def slab(e, carry):
        lows, highs = carry
        u_ref[e] = u_of(e, r_ref[e])
        new_lows, new_highs = [], []
        for a in range(n):
            low = u_ref[e, pl.ds(a * nn, 8), :]
            high = u_ref[e, pl.ds(a * nn + nn - n, 8), :]
            here = lanes == e
            new_lows.append(jnp.where(here, pltpu.roll(low, e, 1), lows[a]))
            new_highs.append(jnp.where(here, pltpu.roll(high, e + 1, 1), highs[a]))
        return tuple(new_lows), tuple(new_highs)

    blank = tuple(jnp.zeros((8, LANES), F32) for _ in range(n))
    lows, highs = lax.fori_loop(0, e_total, slab, (blank, blank), unroll=HALO_UNROLL)
    odd = lax.rem(lax.axis_index("sector"), 2) == 1
    z_odd = lax.rem(lax.axis_index("block"), 2) == 1
    for a in range(n):
        z1[a] = jnp.where(z_odd, lows[a], highs[a])
        z2[a] = jnp.where(z_odd, highs[a], lows[a])
    for layer in range(e_total // span):
        low = u_ref[layer * span, pl.ds(0, nn), :]
        high = u_ref[layer * span + span - 1, pl.ds((n - 1) * nn, nn), :]
        c1[layer] = jnp.where(odd, low, high)
        c2[layer] = jnp.where(odd, high, low)


def subtract_operator(n, e_total, span, r_ref, u_ref, weights, jac_ref, count_ref):
    nn = n * n
    group = GROUP[n]
    lanes = lane_ids(8)

    def some(i, carry):
        first = i * group
        wide = jnp.concatenate([u_ref[first + j] for j in range(group)], axis=1)
        product = times(weights[...], wide)
        for j in range(group):
            e = first + j
            own = product[:, j * LANES : (j + 1) * LANES]
            r_ref[e] = r_ref[e] - jac_ref[pl.ds(e, 1), :] * own - count_ref[...] * u_ref[e]
            s = lax.rem(e, span)
            before = jnp.where(s > 0, PENALTY, 0.0)
            after = jnp.where(s < span - 1, PENALTY, 0.0)
            previous = u_ref[jnp.maximum(e - 1, 0), pl.ds((n - 1) * nn, nn), :]
            following = u_ref[jnp.minimum(e + 1, e_total - 1), pl.ds(0, nn), :]
            r_ref[e, pl.ds(0, nn), :] += before * previous
            r_ref[e, pl.ds((n - 1) * nn, nn), :] += after * following
            for a in range(n):
                low = u_ref[e, pl.ds(a * nn, 8), :]
                high = u_ref[e, pl.ds(a * nn + nn - n, 8), :]
                from_below = jnp.where(lanes > 0, PENALTY * pltpu.roll(high, 1, 1), 0.0)
                from_above = jnp.where(lanes < LANES - 1, PENALTY * pltpu.roll(low, LANES - 1, 1), 0.0)
                r_ref[e, pl.ds(a * nn, n), :] += from_below[:n]
                r_ref[e, pl.ds(a * nn + nn - n, n), :] += from_above[:n]
        return carry

    lax.fori_loop(0, e_total // group, some, 0, unroll=GROUP_UNROLL[n])


def face_shapes(n, layers):
    circ = jax.ShapeDtypeStruct((layers, n * n, LANES), F32)
    axial = jax.ShapeDtypeStruct((n, 8, LANES), F32)
    return [circ, circ, axial, axial]


def prepare(offsets, rotor, stator, mortar, stiff_fine, stiff_coarse, restrict_fine, restrict_coarse):
    rows, span = rotor.shape[0], rotor.shape[1]
    tall, wide = up(rows, 8), up(rows, 16)
    big, small = up(NF**3, 16), up(NC**3, 16)
    smalls = (mortar, stiff_fine, stiff_coarse, restrict_fine, restrict_coarse)

    def body(
        offset_ref, rotor_ref, stator_ref, mortar_in, kf_in, kc_in, rf_in, rc_in,
        pair_out, near1_out, near2_out, proj_out, back_out, wf_out, wc_out, rfs_out, rcs_out, df_out, dc_out,
        mortar_ref, kf_ref, kc_ref, rf_ref, rc_ref, pad_ref, sem, small_sem,
    ):
        flipped, _ = turn_plan(offset_ref[0], span)
        copies = []
        for f in range(span):
            for source, first in ((rotor_ref, span * flipped), (stator_ref, span - span * flipped)):
                if tall > rows:
                    pair_out[first + f, pl.ds(rows, tall - rows), :] = jnp.zeros((tall - rows, LANES), F32)
                copies.append(
                    pltpu.make_async_copy(source.at[:, f, :], pair_out.at[first + f, pl.ds(0, rows), :], sem)
                )
        little = [
            pltpu.make_async_copy(source, target, small_sem)
            for source, target in (
                (mortar_in, mortar_ref), (kf_in, kf_ref), (kc_in, kc_ref), (rf_in, rf_ref), (rc_in, rc_ref)
            )
        ]
        for c in little + copies:
            c.start()
        row, col = node_rows((tall, LANES), 0), node_rows((tall, LANES), 1)
        comp_r, comp_c = digit(row, NF * NF, 4), digit(col, NF * NF, 5)
        rest_r, rest_c = row - NF * NF * comp_r, col - NF * NF * comp_c
        a_r, a_c = digit(rest_r, NF, NF - 1), digit(rest_c, NF, NF - 1)
        same = (comp_r == comp_c) & (rest_r - NF * a_r == rest_c - NF * a_c) & (row < rows) & (col < rows)
        ahead = jnp.where(same, a_r * NF + a_c, -1)
        turned = jnp.where(same, a_c * NF + a_r, -1)
        for c in little:
            c.wait()

        def both_terms(pair):
            highs, lows = zip(*[parts_of(m) for m in pair])
            return jnp.concatenate(
                [jnp.concatenate([h, h], axis=1) for h in highs]
                + [jnp.concatenate([l, jnp.zeros_like(l)], axis=1) for l in lows],
                axis=0,
            )

        for found, out in ((ahead, proj_out), (turned, back_out)):
            pair = []
            for which in range(2):
                total = jnp.zeros((tall, LANES), F32)
                matrix = mortar_ref[:, which, :]
                for i in range(NF):
                    for j in range(NF):
                        total = jnp.where(found == i * NF + j, matrix[i : i + 1, j : j + 1], total)
                pair.append(total)
            out[...] = both_terms([m[:, :wide] for m in pair])

        def padded(ref, height, width):
            pad_ref[...] = jnp.zeros_like(pad_ref)
            pad_ref[pl.ds(0, ref.shape[0]), pl.ds(0, ref.shape[1])] = ref[...]
            return pad_ref[pl.ds(0, height), :][:, :width]

        for ref, out, diag_out, size in ((kf_ref, wf_out, df_out, big), (kc_ref, wc_out, dc_out, small)):
            matrix = padded(ref, size, size)
            out[...] = stacked(matrix)
            row = lax.broadcasted_iota(jnp.int32, (size, size), 0)
            col = lax.broadcasted_iota(jnp.int32, (size, size), 1)
            diag = jnp.sum(jnp.where(row == col, matrix, 0.0), axis=1, keepdims=True)
            diag = jnp.where(row[:, :1] < ref.shape[0], diag, 1.0)
            diag_out[...] = jnp.broadcast_to(diag, (size, LANES))
        rfs_out[...] = stacked(padded(rf_ref, small, big))
        rcs_out[...] = stacked(padded(rc_ref, 16, small))
        for c in copies:
            c.wait()
        odd = lax.rem(lax.axis_index("sector"), 2) == 1
        lowest, highest = pair_out[span * flipped], pair_out[span * flipped + span - 1]
        near1_out[0] = jnp.where(odd, lowest, highest)
        near2_out[0] = jnp.where(odd, highest, lowest)

    return pl.pallas_call(
        body,
        out_shape=[
            jax.ShapeDtypeStruct((2 * span, tall, LANES), F32),
            jax.ShapeDtypeStruct((1, tall, LANES), F32),
            jax.ShapeDtypeStruct((1, tall, LANES), F32),
            jax.ShapeDtypeStruct((4 * tall, 2 * wide), BF16),
            jax.ShapeDtypeStruct((4 * tall, 2 * wide), BF16),
            jax.ShapeDtypeStruct((2 * big, 2 * big), BF16),
            jax.ShapeDtypeStruct((2 * small, 2 * small), BF16),
            jax.ShapeDtypeStruct((2 * small, 2 * big), BF16),
            jax.ShapeDtypeStruct((32, 2 * small), BF16),
            jax.ShapeDtypeStruct((big, LANES), F32),
            jax.ShapeDtypeStruct((small, LANES), F32),
        ],
        in_specs=[smem_spec()] + [hbm_spec()] * 7,
        scratch_shapes=[pltpu.VMEM(m.shape, F32) for m in smalls]
        + [pltpu.VMEM((big, LANES), F32), pltpu.SemaphoreType.DMA, pltpu.SemaphoreType.DMA],
        compiler_params=params(),
        name="prepare",
    )(offsets, *in_hbm(rotor, stator, *smalls))


def apply_faces(matrix_ref, slab_of, count, tall, wide, y0, y1, unrolled):
    group = 4
    fill = jnp.zeros((wide - tall, group * LANES), F32)

    def some(i, carry):
        first = group * i
        least = min if unrolled else jnp.minimum
        x = jnp.concatenate([slab_of(least(first + j, count - 1)) for j in range(group)], axis=1)
        if wide > tall:
            x = jnp.concatenate([x, fill], axis=0)
        high, low = parts_of(x)
        y = jnp.dot(matrix_ref[...], jnp.concatenate([high, low], axis=0), preferred_element_type=F32)
        a = y[:tall] + y[2 * tall : 3 * tall]
        b = y[tall : 2 * tall] + y[3 * tall :]
        for j in range(group):
            y0[first + j] = a[:, j * LANES : (j + 1) * LANES]
            y1[first + j] = b[:, j * LANES : (j + 1) * LANES]
        return carry

    if unrolled:
        for i in range(up(count, group) // group):
            some(i, 0)
    else:
        lax.fori_loop(0, up(count, group) // group, some, 0)


def own_part(offsets, pair, proj, jac, diag):
    span, tall = pair.shape[0] // 2, pair.shape[1]
    wide = proj.shape[1] // 2
    e_total, height = jac.shape[0], diag.shape[0]

    def body(offset_ref, pair_ref, proj_ref, jac_ref, diag_ref, kept, w_ref, y0, y1):
        first = span * turn_plan(offset_ref[0], span)[0]
        apply_faces(proj_ref, lambda f: pair_ref[first + f], span, tall, wide, y0, y1, False)
        kept[0] = y0[0]
        kept[span] = y1[span - 1]

        def face(g, carry):
            kept[g] = y0[g] + y1[g - 1]
            return carry

        lax.fori_loop(1, span, face, 0)
        count = half_faces(NF, height)

        def weight(e, carry):
            w_ref[e] = DAMPING / (jac_ref[pl.ds(e, 1), :] * diag_ref[...] + count)
            return carry

        lax.fori_loop(0, e_total, weight, 0)

    return pl.pallas_call(
        body,
        out_shape=[
            jax.ShapeDtypeStruct((span + 1, tall, LANES), F32),
            jax.ShapeDtypeStruct((e_total, height, LANES), F32),
        ],
        in_specs=[smem_spec()] + [pl.BlockSpec()] * 4,
        scratch_shapes=[pltpu.VMEM((up(span, 4), tall, LANES), F32)] * 2,
        compiler_params=params(),
        cost_estimate=cost(2 * 10**9, 10 * 10**6),
        name="own_part",
    )(offsets, pair, proj, jac, diag)


def copy_faces(source, first, out, into, count):
    def one(f, carry):
        out[into + f] = source[first + f]
        return carry

    lax.fori_loop(0, count, one, 0)


def cut(pair, many, few):
    span = pair.shape[0] // 2

    def body(pair_ref, far, near, near_back, far_back):
        copy_faces(pair_ref, span - few, far, 0, few)
        copy_faces(pair_ref, 0, near, 0, many)
        copy_faces(pair_ref, 2 * span - many, near_back, 0, many)
        copy_faces(pair_ref, span, far_back, 0, few)

    piece = [pltpu.VMEM((count,) + pair.shape[1:], F32) for count in (few, many, many, few)]
    return pl.pallas_call(body, out_shape=piece, compiler_params=params(), name="cut")(pair)


def join(far, near, near_back, far_back):
    few, many = far.shape[0], near.shape[0]
    reach = few + many

    def body(far_ref, near_ref, near_back_ref, far_back_ref, out, sem):
        first = 0
        copies = []
        for piece in (far_ref, near_ref, near_back_ref, far_back_ref):
            count = piece.shape[0]
            copies.append(pltpu.make_async_copy(piece, out.at[pl.ds(first, count)], sem))
            first += count
        for c in copies:
            c.start()
        for c in copies:
            c.wait()

    return pl.pallas_call(
        body,
        out_shape=jax.ShapeDtypeStruct((2 * reach,) + far.shape[1:], F32),
        out_specs=hbm_spec(),
        scratch_shapes=[pltpu.SemaphoreType.DMA],
        compiler_params=params(),
        name="join",
    )(far, near, near_back, far_back)


def first_sweep(offsets, wins, pair, kept, near1, near2, proj, back, source, w, jac, weights, layers):
    span, tall = pair.shape[0] // 2, pair.shape[1]
    reach = wins.shape[0] // 2
    wide = back.shape[1] // 2
    rows = 4 * NF * NF
    e_total = jac.shape[0]
    n, nn = NF, NF * NF
    nodes = n**3
    height = weights.shape[0] // 2

    def body(
        offset_ref, wins_in, pair_ref, kept_ref, near1_ref, near2_ref, proj_ref, back_ref, source_ref, w_ref,
        jac_ref, w_mat, sflux_out, rflux_out, r_ref, u_ref, c1, c2, z1, z2,
        y0, y1, x0, x1, sflux, rflux, count_ref, wins_ref, in_sem, out_sem, win_sems,
    ):
        loads = [
            pltpu.make_async_copy(source_ref.at[:, e, :], r_ref.at[e, pl.ds(0, nodes), :], in_sem)
            for e in range(e_total)
        ]
        flipped, steps = turn_plan(offset_ref[0], span)
        inner = lax.rem(steps, STEP)
        rotor_half = reach * flipped
        halves = [
            pltpu.make_async_copy(wins_in.at[pl.ds(first, reach)], wins_ref.at[pl.ds(first, reach)], win_sems.at[k])
            for k, first in enumerate((rotor_half, reach - rotor_half))
        ]
        for c in halves + loads:
            c.start()
        ahead, behind = STEP - 1 - inner, reach + inner
        first_rotor = jnp.where(flipped == 1, behind, ahead)
        first_stator = jnp.where(flipped == 1, ahead, behind)
        own_stator = span - span * flipped
        count_ref[...] = half_faces(n, height)
        odd = lax.rem(lax.axis_index("sector"), 2) == 1

        def rotor_slab(f):
            if f <= span:
                return wins_ref[first_rotor + f]
            one, two = near1_ref[0], near2_ref[0]
            return jnp.where(odd, one, two) if f == span + 1 else jnp.where(odd, two, one)

        def jump(f):
            own = kept_ref[f]
            if f == 0:
                own = own + x1[span + 1]
            if f == span:
                own = own + x0[span + 2]
            return wins_ref[first_stator + f] - own

        halves[0].wait()
        apply_faces(proj_ref, rotor_slab, span + 3, tall, wide, x0, x1, True)
        halves[1].wait()
        apply_faces(back_ref, jump, span + 1, tall, wide, y0, y1, True)
        stores = []
        for s in range(span):
            sflux[s] = pair_ref[own_stator + s] - (x0[s + 1] + x1[s])
            rflux[s] = y0[s] + y1[s + 1]
            for buffer, out in ((sflux, sflux_out), (rflux, rflux_out)):
                c = pltpu.make_async_copy(buffer.at[s, pl.ds(0, rows), :], out.at[:, s, :], out_sem)
                c.start()
                stores.append(c)
        for c in loads:
            c.wait()
        for s in range(span):
            if height > nodes:
                for layer in range(layers):
                    r_ref[layer * span + s, pl.ds(nodes, height - nodes), :] = jnp.zeros((height - nodes, LANES), F32)
            inflow = sflux[s, pl.ds(0, nn), :] + sflux[s, pl.ds(3 * nn, nn), :]
            outflow = rflux[s, pl.ds(0, nn), :] + rflux[s, pl.ds(3 * nn, nn), :]
            r_ref[span + s, pl.ds(0, nn, stride=n), :] += inflow
            r_ref[s, pl.ds(n - 1, nn, stride=n), :] += -outflow
        correct(n, e_total, span, r_ref, u_ref, lambda e, r: r * w_ref[e], c1, c2, z1, z2)
        subtract_operator(n, e_total, span, r_ref, u_ref, w_mat, jac_ref, count_ref)
        for c in stores:
            c.wait()

    whole = pl.BlockSpec()
    field = jax.ShapeDtypeStruct((e_total, height, LANES), F32)
    trace = jax.ShapeDtypeStruct((rows, span, LANES), F32)
    slabs = pltpu.VMEM((up(span + 3, 4), tall, LANES), F32)
    return pl.pallas_call(
        body,
        out_shape=[trace, trace, field, field] + face_shapes(n, layers),
        in_specs=[smem_spec(), hbm_spec()] + [whole] * 6 + [hbm_spec()] + [whole] * 3,
        out_specs=[hbm_spec()] * 2 + [whole] * 6,
        scratch_shapes=[slabs] * 4
        + [
            pltpu.VMEM((span, tall, LANES), F32),
            pltpu.VMEM((span, tall, LANES), F32),
            pltpu.VMEM((height, LANES), F32),
            pltpu.VMEM(wins.shape, F32),
            pltpu.SemaphoreType.DMA,
            pltpu.SemaphoreType.DMA,
            pltpu.SemaphoreType.DMA((2,)),
        ],
        compiler_params=params(),
        cost_estimate=cost(2 * 10**9, 20 * 10**6),
        name="first_sweep",
    )(offsets, *in_hbm(wins), pair, kept, near1, near2, proj, back, *in_hbm(source), in_vmem(w), jac, weights)


def sweep(n, r, p, w, jac, weights, faces, layers, last):
    e_total, height = r.shape[0], r.shape[1]
    span = e_total // layers
    nodes = n**3

    def body(r_in, p_in, w_in, jac_ref, w_mat, h1, h2, g1, g2, p_out, r_ref, c1, c2, z1, z2, u_ref, p_keep, count_ref, sem):
        count_ref[...] = half_faces(n, height)
        p_ref = p_keep if last else p_out
        add_halo(n, e_total, span, lambda e: r_in[e], r_ref, h1, h2, g1, g2)

        def u_of(e, r_here):
            u = r_here * w_in[e]
            p_ref[e] = p_in[e] + u
            return u

        correct(n, e_total, span, r_ref, u_ref, u_of, c1, c2, z1, z2)
        stores = []
        if last:
            for e in range(e_total):
                c = pltpu.make_async_copy(p_ref.at[e, pl.ds(0, nodes), :], p_out.at[:, e, :], sem)
                c.start()
                stores.append(c)
        subtract_operator(n, e_total, span, r_ref, u_ref, w_mat, jac_ref, count_ref)
        for c in stores:
            c.wait()

    whole = pl.BlockSpec()
    field = jax.ShapeDtypeStruct((e_total, height, LANES), F32)
    kept = jax.ShapeDtypeStruct((nodes, e_total, LANES), F32) if last else field
    return pl.pallas_call(
        body,
        out_shape=[kept, field] + face_shapes(n, layers),
        out_specs=[any_spec() if last else whole] + [whole] * 5,
        scratch_shapes=[
            pltpu.VMEM((e_total, height, LANES), F32),
            pltpu.VMEM((e_total, height, LANES) if last else (1, 8, LANES), F32),
            pltpu.VMEM((height, LANES), F32),
            pltpu.SemaphoreType.DMA,
        ],
        compiler_params=params(),
        cost_estimate=cost(10**9 if n == NF else 10**8, 10 * 10**6),
    )(r, p, w, jac, weights, *faces)


def to_coarse(r, faces, restrict, jac, weights, diag, layers):
    e_total = r.shape[0]
    span = e_total // layers
    small = weights.shape[0] // 2
    n = NC
    group = 4

    def body(r_in, h1, h2, g1, g2, rest_ref, jac_ref, w_mat, diag_ref, rc_ref, u_ref, w_ref, c1, c2, z1, z2, r_fine, count_ref):
        count_ref[...] = half_faces(n, small)
        add_halo(NF, e_total, span, lambda e: r_in[e], r_fine, h1, h2, g1, g2)

        def some(i, carry):
            first = i * group
            wide = jnp.concatenate([r_fine[first + j] for j in range(group)], axis=1)
            product = times(rest_ref[...], wide)
            for j in range(group):
                rc_ref[first + j] = product[:, j * LANES : (j + 1) * LANES]
            return carry

        lax.fori_loop(0, e_total // group, some, 0, unroll=2)

        def u_of(e, r_here):
            w_here = DAMPING / (jac_ref[pl.ds(e, 1), :] * diag_ref[...] + count_ref[...])
            w_ref[e] = w_here
            return r_here * w_here

        correct(n, e_total, span, rc_ref, u_ref, u_of, c1, c2, z1, z2)
        subtract_operator(n, e_total, span, rc_ref, u_ref, w_mat, jac_ref, count_ref)

    field = jax.ShapeDtypeStruct((e_total, small, LANES), F32)
    return pl.pallas_call(
        body,
        out_shape=[field, field, field] + face_shapes(n, layers),
        scratch_shapes=[pltpu.VMEM(r.shape, F32), pltpu.VMEM((small, LANES), F32)],
        compiler_params=params(),
        cost_estimate=cost(5 * 10**8, 5 * 10**6),
        name="to_coarse",
    )(r, *faces, restrict, jac, weights, diag)


def to_coarsest(r, faces, restrict, layers):
    e_total = r.shape[0]
    span = e_total // layers
    group = 4

    def body(r_in, h1, h2, g1, g2, rest_ref, out_ref, r_done, kept, sem):
        add_halo(NC, e_total, span, lambda e: r_in[e], r_done, h1, h2, g1, g2)

        def some(i, carry):
            first = i * group
            wide = jnp.concatenate([r_done[first + j] for j in range(group)], axis=1)
            product = times(rest_ref[...], wide)
            for j in range(group):
                kept[first + j] = product[:LAST, j * LANES : (j + 1) * LANES]
            return carry

        lax.fori_loop(0, e_total // group, some, 0, unroll=8)
        stores = []
        for e in range(e_total):
            c = pltpu.make_async_copy(kept.at[e], out_ref.at[:, e, :], sem)
            c.start()
            stores.append(c)
        for c in stores:
            c.wait()

    whole = pl.BlockSpec()
    return pl.pallas_call(
        body,
        out_shape=jax.ShapeDtypeStruct((LAST, e_total, LANES), F32),
        in_specs=[whole] * 6,
        out_specs=any_spec(),
        scratch_shapes=[
            pltpu.VMEM(r.shape, F32),
            pltpu.VMEM((e_total, LAST, LANES), F32),
            pltpu.SemaphoreType.DMA,
        ],
        compiler_params=params(),
        cost_estimate=cost(5 * 10**7, 10**6),
        name="to_coarsest",
    )(r, *faces, restrict)


def move(x, axis, by):
    count = lax.axis_size(axis)
    return lax.ppermute(x, axis, [(i, (i + by) % count) for i in range(count)])


def swap(x, axis, odd_first):
    count = lax.axis_size(axis)
    pairs = []
    for i in range(count):
        ahead = (i % 2 == 0) != odd_first
        pairs.append((i, (i + 1) % count if ahead else (i - 1) % count))
    return lax.ppermute(x, axis, pairs)


def swap_inner(x, axis, other):
    count, beside = lax.axis_size(axis), lax.axis_size(other)
    pairs = []
    for j in range(beside):
        for i in range(count):
            to = i + 1 if i % 2 else i - 1
            target = (j, to) if 0 <= to < count else (j ^ 1, i)
            pairs.append((j * count + i, target[0] * count + target[1]))
    return lax.ppermute(x, (other, axis), pairs)


def exchange(faces):
    c1, c2, z1, z2 = faces
    c2 = swap(c2, "sector", True)
    z2 = swap_inner(z2, "block", "sector")
    z1 = swap(z1, "block", False)
    c1 = swap(c1, "sector", False)
    return c1, c2, z1, z2


def windows(pair, offsets, own):
    span = pair.shape[0] // 2
    buckets = span // STEP
    _, steps = turn_plan(offsets[0], span)

    def branch(number):
        by, bucket = number // buckets, number % buckets
        many, few = span - STEP * bucket, STEP * (bucket + 1)

        def run(pair, offsets, own):
            far, near, near_back, far_back = cut(pair, many, few)
            near = move(near, "sector", by)
            far = move(far, "sector", by + 1)
            near_back = move(near_back, "sector", -by)
            far_back = move(far_back, "sector", -by - 1)
            kept, w = own_part(offsets, pair, *own)
            return kept, w, join(far, near, near_back, far_back)

        return run

    branches = [branch(i) for i in range(lax.axis_size("sector") // 2 * buckets)]
    return lax.switch(lax.div(steps, STEP), branches, pair, offsets, own)


def per_device(
    source, jacobian, stiff_fine, stiff_coarse, restrict_fine, restrict_coarse, mortar_proj, rotor_trace,
    stator_trace, offsets,
):
    layers, span, axial = jacobian.shape
    e_total = layers * span
    source_rows = source.reshape(source.shape[0], e_total, axial)
    jac = jacobian.reshape(e_total, axial)
    rotor_rows = rotor_trace.reshape(-1, span, axial)
    stator_rows = stator_trace.reshape(-1, span, axial)
    pair, near1, near2, proj, back, wf, wc, rfs, rcs, df, dc = prepare(
        offsets, rotor_rows, stator_rows, mortar_proj.transpose(1, 0, 2),
        stiff_fine, stiff_coarse, restrict_fine, restrict_coarse,
    )
    near2 = swap(near2, "sector", True)
    near1 = swap(near1, "sector", False)
    kept, w, wins = windows(pair, offsets, (proj, jac, df))
    sflux, rflux, r, p, *faces = first_sweep(
        offsets, wins, pair, kept, near1, near2, proj, back, source_rows, w, jac, wf, layers
    )
    p, r, *faces = sweep(NF, r, p, w, jac, wf, exchange(faces), layers, False)
    fine, r, *faces = sweep(NF, r, p, w, jac, wf, exchange(faces), layers, True)
    r, p, w, *faces = to_coarse(r, exchange(faces), rfs, jac, wc, dc, layers)
    p, r, *faces = sweep(NC, r, p, w, jac, wc, exchange(faces), layers, False)
    coarse, r, *faces = sweep(NC, r, p, w, jac, wc, exchange(faces), layers, True)
    coarsest = to_coarsest(r, exchange(faces), rcs, layers)
    shape = (layers, span, axial)
    return (
        sflux.reshape(stator_trace.shape),
        rflux.reshape(rotor_trace.shape),
        fine.reshape((-1,) + shape),
        coarse.reshape((-1,) + shape),
        coarsest.reshape((-1,) + shape),
    )


def solution(mesh):
    cell = P(None, None, "sector", "block")

    return jax.shard_map(
        per_device,
        mesh=mesh,
        in_specs=(cell, P(None, "sector", "block"), P(), P(), P(), P(), P(), cell, cell, P("block")),
        out_specs=(cell,) * 5,
        check_vma=False,
    )
```

```python
import jax
import jax.numpy as jnp
from jax import lax
from jax.experimental import pallas as pl
from jax.experimental.pallas import tpu as pltpu
from jax.sharding import PartitionSpec as P


F32 = jnp.float32
BF16 = jnp.bfloat16
DAMPING = 0.6
PENALTY = 0.5
LANES = 128
NF = 5
NC = 3
LAST = 8
STEP = 2
HALO_UNROLL = 32
GROUP = {NF: 4, NC: 16}
GROUP_UNROLL = {NF: 4, NC: 1}
VMEM_BYTES = 14 * 1024 * 1024


def up(value, unit):
    return (value + unit - 1) // unit * unit


def any_spec():
    return pl.BlockSpec(memory_space=pl.ANY)


def hbm_spec():
    return pl.BlockSpec(memory_space=pltpu.HBM)


def in_hbm(*arrays):
    return tuple(pltpu.with_memory_space_constraint(x, pltpu.HBM) for x in arrays)


def params(**extra):
    return pltpu.CompilerParams(vmem_limit_bytes=VMEM_BYTES, **extra)


def cost(flops, data):
    return pl.CostEstimate(flops=flops, bytes_accessed=data, transcendentals=0)


def parts_of(x):
    high = x.astype(BF16)
    low = (x - high.astype(F32)).astype(BF16)
    return high, low


def stacked(matrix):
    high, low = parts_of(matrix)
    top = jnp.concatenate([high, high], axis=1)
    bottom = jnp.concatenate([low, jnp.zeros_like(low)], axis=1)
    return jnp.concatenate([top, bottom], axis=0)


def times(weights, x):
    rows = weights.shape[0] // 2
    high, low = parts_of(x)
    both = jnp.dot(weights, jnp.concatenate([high, low], axis=0), preferred_element_type=F32)
    return both[:rows] + both[rows:]


def lane_ids(rows):
    return lax.broadcasted_iota(jnp.int32, (rows, LANES), 1)


def node_rows(shape, axis):
    return lax.broadcasted_iota(jnp.int32, shape, axis)


def digit(index, unit, most):
    found = jnp.zeros_like(index)
    for k in range(1, most + 1):
        found += jnp.where(index >= k * unit, 1, 0)
    return found


def half_faces(n, height):
    row = node_rows((height, LANES), 0)
    a = digit(row, n * n, n)
    b = digit(row - n * n * a, n, n - 1)
    on_a = jnp.where((a == 0) | (a == n - 1), PENALTY, 0.0)
    on_b = jnp.where((b == 0) | (b == n - 1), PENALTY, 0.0)
    return jnp.where(row < n**3, on_a + on_b, 0.0)


def turn_plan(offset, span):
    total = span * lax.axis_size("sector")
    flipped = jnp.where(offset >= total // 2, 1, 0)
    return flipped, jnp.where(flipped == 1, total - 1 - offset, offset)


def smem_spec():
    return pl.BlockSpec(memory_space=pltpu.SMEM)


def add_halo(n, e_total, span, source_of, r_ref, c1, c2, z1, z2):
    nn = n * n
    odd = lax.rem(lax.axis_index("sector"), 2) == 1
    block = lax.axis_index("block")
    z_odd = lax.rem(block, 2) == 1
    lowest = block == 0
    highest = block == lax.axis_size("block") - 1
    lanes = lane_ids(8)

    def slab(e, carry):
        r_ref[e] = source_of(e)
        for a in range(n):
            first, second = z1[a], z2[a]
            below = jnp.where(z_odd, first, second)
            above = jnp.where(z_odd, second, first)
            below = pltpu.roll(below, lax.rem(LANES - e, LANES), 1)
            above = pltpu.roll(above, LANES - 1 - e, 1)
            below = jnp.where((lanes == 0) & jnp.logical_not(lowest), PENALTY * below, 0.0)
            above = jnp.where((lanes == LANES - 1) & jnp.logical_not(highest), PENALTY * above, 0.0)
            r_ref[e, pl.ds(a * nn, n), :] += below[:n]
            r_ref[e, pl.ds(a * nn + nn - n, n), :] += above[:n]
        return carry

    lax.fori_loop(0, e_total, slab, 0, unroll=HALO_UNROLL)
    for layer in range(e_total // span):
        first, second = c1[layer], c2[layer]
        r_ref[layer * span, pl.ds(0, nn), :] += PENALTY * jnp.where(odd, first, second)
        r_ref[layer * span + span - 1, pl.ds((n - 1) * nn, nn), :] += PENALTY * jnp.where(odd, second, first)


def correct(n, e_total, span, r_ref, u_ref, u_of, c1, c2, z1, z2):
    nn = n * n
    lanes = lane_ids(8)

    def slab(e, carry):
        lows, highs = carry
        u_ref[e] = u_of(e, r_ref[e])
        new_lows, new_highs = [], []
        for a in range(n):
            low = u_ref[e, pl.ds(a * nn, 8), :]
            high = u_ref[e, pl.ds(a * nn + nn - n, 8), :]
            here = lanes == e
            new_lows.append(jnp.where(here, pltpu.roll(low, e, 1), lows[a]))
            new_highs.append(jnp.where(here, pltpu.roll(high, e + 1, 1), highs[a]))
        return tuple(new_lows), tuple(new_highs)

    blank = tuple(jnp.zeros((8, LANES), F32) for _ in range(n))
    lows, highs = lax.fori_loop(0, e_total, slab, (blank, blank), unroll=HALO_UNROLL)
    odd = lax.rem(lax.axis_index("sector"), 2) == 1
    z_odd = lax.rem(lax.axis_index("block"), 2) == 1
    for a in range(n):
        z1[a] = jnp.where(z_odd, lows[a], highs[a])
        z2[a] = jnp.where(z_odd, highs[a], lows[a])
    for layer in range(e_total // span):
        low = u_ref[layer * span, pl.ds(0, nn), :]
        high = u_ref[layer * span + span - 1, pl.ds((n - 1) * nn, nn), :]
        c1[layer] = jnp.where(odd, low, high)
        c2[layer] = jnp.where(odd, high, low)


def subtract_operator(n, e_total, span, r_ref, u_ref, weights, jac_ref, count_ref):
    nn = n * n
    group = GROUP[n]
    lanes = lane_ids(8)

    def some(i, carry):
        first = i * group
        wide = jnp.concatenate([u_ref[first + j] for j in range(group)], axis=1)
        product = times(weights[...], wide)
        for j in range(group):
            e = first + j
            own = product[:, j * LANES : (j + 1) * LANES]
            r_ref[e] = r_ref[e] - jac_ref[pl.ds(e, 1), :] * own - count_ref[...] * u_ref[e]
            s = lax.rem(e, span)
            before = jnp.where(s > 0, PENALTY, 0.0)
            after = jnp.where(s < span - 1, PENALTY, 0.0)
            previous = u_ref[jnp.maximum(e - 1, 0), pl.ds((n - 1) * nn, nn), :]
            following = u_ref[jnp.minimum(e + 1, e_total - 1), pl.ds(0, nn), :]
            r_ref[e, pl.ds(0, nn), :] += before * previous
            r_ref[e, pl.ds((n - 1) * nn, nn), :] += after * following
            for a in range(n):
                low = u_ref[e, pl.ds(a * nn, 8), :]
                high = u_ref[e, pl.ds(a * nn + nn - n, 8), :]
                from_below = jnp.where(lanes > 0, PENALTY * pltpu.roll(high, 1, 1), 0.0)
                from_above = jnp.where(lanes < LANES - 1, PENALTY * pltpu.roll(low, LANES - 1, 1), 0.0)
                r_ref[e, pl.ds(a * nn, n), :] += from_below[:n]
                r_ref[e, pl.ds(a * nn + nn - n, n), :] += from_above[:n]
        return carry

    lax.fori_loop(0, e_total // group, some, 0, unroll=GROUP_UNROLL[n])


def face_shapes(n, layers):
    circ = jax.ShapeDtypeStruct((layers, n * n, LANES), F32)
    axial = jax.ShapeDtypeStruct((n, 8, LANES), F32)
    return [circ, circ, axial, axial]


def prepare(offsets, rotor, stator, mortar, stiff_fine, stiff_coarse, restrict_fine, restrict_coarse):
    rows, span = rotor.shape[0], rotor.shape[1]
    tall, wide = up(rows, 8), up(rows, 16)
    big, small = up(NF**3, 16), up(NC**3, 16)
    smalls = (mortar, stiff_fine, stiff_coarse, restrict_fine, restrict_coarse)

    def body(
        offset_ref, rotor_ref, stator_ref, mortar_in, kf_in, kc_in, rf_in, rc_in,
        pair_out, near1_out, near2_out, proj_out, back_out, wf_out, wc_out, rfs_out, rcs_out, df_out, dc_out,
        mortar_ref, kf_ref, kc_ref, rf_ref, rc_ref, pad_ref, sem, small_sem,
    ):
        flipped, _ = turn_plan(offset_ref[0], span)
        copies = []
        for f in range(span):
            for source, first in ((rotor_ref, span * flipped), (stator_ref, span - span * flipped)):
                if tall > rows:
                    pair_out[first + f, pl.ds(rows, tall - rows), :] = jnp.zeros((tall - rows, LANES), F32)
                copies.append(
                    pltpu.make_async_copy(source.at[:, f, :], pair_out.at[first + f, pl.ds(0, rows), :], sem)
                )
        little = [
            pltpu.make_async_copy(source, target, small_sem)
            for source, target in (
                (mortar_in, mortar_ref), (kf_in, kf_ref), (kc_in, kc_ref), (rf_in, rf_ref), (rc_in, rc_ref)
            )
        ]
        for c in little + copies:
            c.start()
        row, col = node_rows((tall, LANES), 0), node_rows((tall, LANES), 1)
        comp_r, comp_c = digit(row, NF * NF, 4), digit(col, NF * NF, 5)
        rest_r, rest_c = row - NF * NF * comp_r, col - NF * NF * comp_c
        a_r, a_c = digit(rest_r, NF, NF - 1), digit(rest_c, NF, NF - 1)
        same = (comp_r == comp_c) & (rest_r - NF * a_r == rest_c - NF * a_c) & (row < rows) & (col < rows)
        ahead = jnp.where(same, a_r * NF + a_c, -1)
        turned = jnp.where(same, a_c * NF + a_r, -1)
        for c in little:
            c.wait()

        def both_terms(pair):
            highs, lows = zip(*[parts_of(m) for m in pair])
            return jnp.concatenate(
                [jnp.concatenate([h, h], axis=1) for h in highs]
                + [jnp.concatenate([l, jnp.zeros_like(l)], axis=1) for l in lows],
                axis=0,
            )

        for found, out in ((ahead, proj_out), (turned, back_out)):
            pair = []
            for which in range(2):
                total = jnp.zeros((tall, LANES), F32)
                matrix = mortar_ref[:, which, :]
                for i in range(NF):
                    for j in range(NF):
                        total = jnp.where(found == i * NF + j, matrix[i : i + 1, j : j + 1], total)
                pair.append(total)
            out[...] = both_terms([m[:, :wide] for m in pair])

        def padded(ref, height, width):
            pad_ref[...] = jnp.zeros_like(pad_ref)
            pad_ref[pl.ds(0, ref.shape[0]), pl.ds(0, ref.shape[1])] = ref[...]
            return pad_ref[pl.ds(0, height), :][:, :width]

        for ref, out, diag_out, size in ((kf_ref, wf_out, df_out, big), (kc_ref, wc_out, dc_out, small)):
            matrix = padded(ref, size, size)
            out[...] = stacked(matrix)
            row = lax.broadcasted_iota(jnp.int32, (size, size), 0)
            col = lax.broadcasted_iota(jnp.int32, (size, size), 1)
            diag = jnp.sum(jnp.where(row == col, matrix, 0.0), axis=1, keepdims=True)
            diag = jnp.where(row[:, :1] < ref.shape[0], diag, 1.0)
            diag_out[...] = jnp.broadcast_to(diag, (size, LANES))
        rfs_out[...] = stacked(padded(rf_ref, small, big))
        rcs_out[...] = stacked(padded(rc_ref, 16, small))
        for c in copies:
            c.wait()
        odd = lax.rem(lax.axis_index("sector"), 2) == 1
        lowest, highest = pair_out[span * flipped], pair_out[span * flipped + span - 1]
        near1_out[0] = jnp.where(odd, lowest, highest)
        near2_out[0] = jnp.where(odd, highest, lowest)

    return pl.pallas_call(
        body,
        out_shape=[
            pltpu.VMEM((2 * span, tall, LANES), F32),
            jax.ShapeDtypeStruct((1, tall, LANES), F32),
            jax.ShapeDtypeStruct((1, tall, LANES), F32),
            jax.ShapeDtypeStruct((4 * tall, 2 * wide), BF16),
            jax.ShapeDtypeStruct((4 * tall, 2 * wide), BF16),
            jax.ShapeDtypeStruct((2 * big, 2 * big), BF16),
            jax.ShapeDtypeStruct((2 * small, 2 * small), BF16),
            jax.ShapeDtypeStruct((2 * small, 2 * big), BF16),
            jax.ShapeDtypeStruct((32, 2 * small), BF16),
            jax.ShapeDtypeStruct((big, LANES), F32),
            jax.ShapeDtypeStruct((small, LANES), F32),
        ],
        in_specs=[smem_spec()] + [hbm_spec()] * 7,
        scratch_shapes=[pltpu.VMEM(m.shape, F32) for m in smalls]
        + [pltpu.VMEM((big, LANES), F32), pltpu.SemaphoreType.DMA, pltpu.SemaphoreType.DMA],
        compiler_params=params(),
        name="prepare",
    )(offsets, *in_hbm(rotor, stator, *smalls))


def apply_faces(matrix_ref, slab_of, count, tall, wide, y0, y1, unrolled):
    group = 4
    fill = jnp.zeros((wide - tall, group * LANES), F32)

    def some(i, carry):
        first = group * i
        least = min if unrolled else jnp.minimum
        x = jnp.concatenate([slab_of(least(first + j, count - 1)) for j in range(group)], axis=1)
        if wide > tall:
            x = jnp.concatenate([x, fill], axis=0)
        high, low = parts_of(x)
        y = jnp.dot(matrix_ref[...], jnp.concatenate([high, low], axis=0), preferred_element_type=F32)
        a = y[:tall] + y[2 * tall : 3 * tall]
        b = y[tall : 2 * tall] + y[3 * tall :]
        for j in range(group):
            y0[first + j] = a[:, j * LANES : (j + 1) * LANES]
            y1[first + j] = b[:, j * LANES : (j + 1) * LANES]
        return carry

    if unrolled:
        for i in range(up(count, group) // group):
            some(i, 0)
    else:
        lax.fori_loop(0, up(count, group) // group, some, 0)


def own_part(offsets, pair, proj, jac, diag):
    span, tall = pair.shape[0] // 2, pair.shape[1]
    wide = proj.shape[1] // 2
    e_total, height = jac.shape[0], diag.shape[0]

    def body(offset_ref, pair_ref, proj_ref, jac_ref, diag_ref, kept, w_ref, y0, y1):
        first = span * turn_plan(offset_ref[0], span)[0]
        apply_faces(proj_ref, lambda f: pair_ref[first + f], span, tall, wide, y0, y1, False)
        kept[0] = y0[0]
        kept[span] = y1[span - 1]

        def face(g, carry):
            kept[g] = y0[g] + y1[g - 1]
            return carry

        lax.fori_loop(1, span, face, 0)
        count = half_faces(NF, height)

        def weight(e, carry):
            w_ref[e] = DAMPING / (jac_ref[pl.ds(e, 1), :] * diag_ref[...] + count)
            return carry

        lax.fori_loop(0, e_total, weight, 0)

    return pl.pallas_call(
        body,
        out_shape=[
            jax.ShapeDtypeStruct((span + 1, tall, LANES), F32),
            jax.ShapeDtypeStruct((e_total, height, LANES), F32),
        ],
        in_specs=[smem_spec()] + [pl.BlockSpec()] * 4,
        scratch_shapes=[pltpu.VMEM((up(span, 4), tall, LANES), F32)] * 2,
        compiler_params=params(),
        cost_estimate=cost(2 * 10**9, 10 * 10**6),
        name="own_part",
    )(offsets, pair, proj, jac, diag)


def copy_faces(source, first, out, into, count):
    def one(f, carry):
        out[into + f] = source[first + f]
        return carry

    lax.fori_loop(0, count, one, 0, unroll=2)


def cut(pair, many, few):
    span = pair.shape[0] // 2

    def body(pair_ref, far, near, near_back, far_back):
        copy_faces(pair_ref, span - few, far, 0, few)
        copy_faces(pair_ref, 0, near, 0, many)
        copy_faces(pair_ref, 2 * span - many, near_back, 0, many)
        copy_faces(pair_ref, span, far_back, 0, few)

    piece = [pltpu.VMEM((count,) + pair.shape[1:], F32) for count in (few, many, many, few)]
    return pl.pallas_call(body, out_shape=piece, compiler_params=params(), name="cut")(pair)


def join(far, near, near_back, far_back):
    few, many = far.shape[0], near.shape[0]
    reach = few + many

    def body(far_ref, near_ref, near_back_ref, far_back_ref, out, sem):
        first = 0
        copies = []
        for piece in (far_ref, near_ref, near_back_ref, far_back_ref):
            count = piece.shape[0]
            copies.append(pltpu.make_async_copy(piece, out.at[pl.ds(first, count)], sem))
            first += count
        for c in copies:
            c.start()
        for c in copies:
            c.wait()

    return pl.pallas_call(
        body,
        out_shape=pltpu.HBM((2 * reach,) + far.shape[1:], F32),
        out_specs=hbm_spec(),
        scratch_shapes=[pltpu.SemaphoreType.DMA],
        compiler_params=params(),
        name="join",
    )(far, near, near_back, far_back)


def first_sweep(offsets, wins, pair, kept, near1, near2, proj, back, source, w, jac, weights, layers):
    span, tall = pair.shape[0] // 2, pair.shape[1]
    reach = wins.shape[0] // 2
    wide = back.shape[1] // 2
    rows = 4 * NF * NF
    e_total = jac.shape[0]
    n, nn = NF, NF * NF
    nodes = n**3
    height = weights.shape[0] // 2

    def body(
        offset_ref, wins_in, pair_ref, kept_ref, near1_ref, near2_ref, proj_ref, back_ref, source_ref, w_in,
        jac_ref, w_mat, sflux_out, rflux_out, r_ref, u_ref, c1, c2, z1, z2,
        y0, y1, x0, x1, sflux, rflux, count_ref, wins_ref, w_ref, in_sem, out_sem, win_sems,
    ):
        loads = [
            pltpu.make_async_copy(source_ref.at[:, e, :], r_ref.at[e, pl.ds(0, nodes), :], in_sem)
            for e in range(e_total)
        ]
        flipped, steps = turn_plan(offset_ref[0], span)
        inner = lax.rem(steps, STEP)
        rotor_half = reach * flipped
        halves = [
            pltpu.make_async_copy(wins_in.at[pl.ds(first, reach)], wins_ref.at[pl.ds(first, reach)], win_sems.at[k])
            for k, first in enumerate((rotor_half, reach - rotor_half))
        ]
        loads.append(pltpu.make_async_copy(w_in, w_ref, win_sems.at[2]))
        for c in halves + loads:
            c.start()
        ahead, behind = STEP - 1 - inner, reach + inner
        first_rotor = jnp.where(flipped == 1, behind, ahead)
        first_stator = jnp.where(flipped == 1, ahead, behind)
        own_stator = span - span * flipped
        count_ref[...] = half_faces(n, height)
        odd = lax.rem(lax.axis_index("sector"), 2) == 1

        def rotor_slab(f):
            if f <= span:
                return wins_ref[first_rotor + f]
            one, two = near1_ref[0], near2_ref[0]
            return jnp.where(odd, one, two) if f == span + 1 else jnp.where(odd, two, one)

        def jump(f):
            own = kept_ref[f]
            if f == 0:
                own = own + x1[span + 1]
            if f == span:
                own = own + x0[span + 2]
            return wins_ref[first_stator + f] - own

        halves[0].wait()
        apply_faces(proj_ref, rotor_slab, span + 3, tall, wide, x0, x1, True)
        halves[1].wait()
        apply_faces(back_ref, jump, span + 1, tall, wide, y0, y1, True)
        stores = []
        for s in range(span):
            sflux[s] = pair_ref[own_stator + s] - (x0[s + 1] + x1[s])
            rflux[s] = y0[s] + y1[s + 1]
            for buffer, out in ((sflux, sflux_out), (rflux, rflux_out)):
                c = pltpu.make_async_copy(buffer.at[s, pl.ds(0, rows), :], out.at[:, s, :], out_sem)
                c.start()
                stores.append(c)
        for c in loads:
            c.wait()
        for s in range(span):
            if height > nodes:
                for layer in range(layers):
                    r_ref[layer * span + s, pl.ds(nodes, height - nodes), :] = jnp.zeros((height - nodes, LANES), F32)
            inflow = sflux[s, pl.ds(0, nn), :] + sflux[s, pl.ds(3 * nn, nn), :]
            outflow = rflux[s, pl.ds(0, nn), :] + rflux[s, pl.ds(3 * nn, nn), :]
            r_ref[span + s, pl.ds(0, nn, stride=n), :] += inflow
            r_ref[s, pl.ds(n - 1, nn, stride=n), :] += -outflow
        correct(n, e_total, span, r_ref, u_ref, lambda e, r: r * w_ref[e], c1, c2, z1, z2)
        subtract_operator(n, e_total, span, r_ref, u_ref, w_mat, jac_ref, count_ref)
        for c in stores:
            c.wait()

    whole = pl.BlockSpec()
    field = jax.ShapeDtypeStruct((e_total, height, LANES), F32)
    trace = jax.ShapeDtypeStruct((rows, span, LANES), F32)
    slabs = pltpu.VMEM((up(span + 3, 4), tall, LANES), F32)
    return pl.pallas_call(
        body,
        out_shape=[trace, trace, field, field] + face_shapes(n, layers),
        in_specs=[smem_spec(), hbm_spec()] + [whole] * 6 + [hbm_spec()] * 2 + [whole] * 2,
        out_specs=[hbm_spec()] * 2 + [whole] * 6,
        scratch_shapes=[slabs] * 4
        + [
            pltpu.VMEM((span, tall, LANES), F32),
            pltpu.VMEM((span, tall, LANES), F32),
            pltpu.VMEM((height, LANES), F32),
            pltpu.VMEM(wins.shape, F32),
            pltpu.VMEM(w.shape, F32),
            pltpu.SemaphoreType.DMA,
            pltpu.SemaphoreType.DMA,
            pltpu.SemaphoreType.DMA((3,)),
        ],
        compiler_params=params(),
        cost_estimate=cost(2 * 10**9, 20 * 10**6),
        name="first_sweep",
    )(offsets, *in_hbm(wins), pair, kept, near1, near2, proj, back, *in_hbm(source, w), jac, weights)


def sweep(n, r, p, w, jac, weights, faces, layers, last):
    e_total, height = r.shape[0], r.shape[1]
    span = e_total // layers
    nodes = n**3

    def body(r_in, p_in, w_in, jac_ref, w_mat, h1, h2, g1, g2, p_out, r_ref, c1, c2, z1, z2, u_ref, p_keep, count_ref, sem):
        count_ref[...] = half_faces(n, height)
        p_ref = p_keep if last else p_out
        add_halo(n, e_total, span, lambda e: r_in[e], r_ref, h1, h2, g1, g2)

        def u_of(e, r_here):
            u = r_here * w_in[e]
            p_ref[e] = p_in[e] + u
            return u

        correct(n, e_total, span, r_ref, u_ref, u_of, c1, c2, z1, z2)
        stores = []
        if last:
            for e in range(e_total):
                c = pltpu.make_async_copy(p_ref.at[e, pl.ds(0, nodes), :], p_out.at[:, e, :], sem)
                c.start()
                stores.append(c)
        subtract_operator(n, e_total, span, r_ref, u_ref, w_mat, jac_ref, count_ref)
        for c in stores:
            c.wait()

    whole = pl.BlockSpec()
    field = jax.ShapeDtypeStruct((e_total, height, LANES), F32)
    kept = jax.ShapeDtypeStruct((nodes, e_total, LANES), F32) if last else field
    return pl.pallas_call(
        body,
        out_shape=[kept, field] + face_shapes(n, layers),
        out_specs=[any_spec() if last else whole] + [whole] * 5,
        scratch_shapes=[
            pltpu.VMEM((e_total, height, LANES), F32),
            pltpu.VMEM((e_total, height, LANES) if last else (1, 8, LANES), F32),
            pltpu.VMEM((height, LANES), F32),
            pltpu.SemaphoreType.DMA,
        ],
        compiler_params=params(),
        cost_estimate=cost(10**9 if n == NF else 10**8, 10 * 10**6),
    )(r, p, w, jac, weights, *faces)


def to_coarse(r, faces, restrict, jac, weights, diag, layers):
    e_total = r.shape[0]
    span = e_total // layers
    small = weights.shape[0] // 2
    n = NC
    group = 4

    def body(r_in, h1, h2, g1, g2, rest_ref, jac_ref, w_mat, diag_ref, rc_ref, u_ref, w_ref, c1, c2, z1, z2, r_fine, count_ref):
        count_ref[...] = half_faces(n, small)
        add_halo(NF, e_total, span, lambda e: r_in[e], r_fine, h1, h2, g1, g2)

        def some(i, carry):
            first = i * group
            wide = jnp.concatenate([r_fine[first + j] for j in range(group)], axis=1)
            product = times(rest_ref[...], wide)
            for j in range(group):
                rc_ref[first + j] = product[:, j * LANES : (j + 1) * LANES]
            return carry

        lax.fori_loop(0, e_total // group, some, 0, unroll=2)

        def u_of(e, r_here):
            w_here = DAMPING / (jac_ref[pl.ds(e, 1), :] * diag_ref[...] + count_ref[...])
            w_ref[e] = w_here
            return r_here * w_here

        correct(n, e_total, span, rc_ref, u_ref, u_of, c1, c2, z1, z2)
        subtract_operator(n, e_total, span, rc_ref, u_ref, w_mat, jac_ref, count_ref)

    field = jax.ShapeDtypeStruct((e_total, small, LANES), F32)
    return pl.pallas_call(
        body,
        out_shape=[field, field, field] + face_shapes(n, layers),
        scratch_shapes=[pltpu.VMEM(r.shape, F32), pltpu.VMEM((small, LANES), F32)],
        compiler_params=params(),
        cost_estimate=cost(5 * 10**8, 5 * 10**6),
        name="to_coarse",
    )(r, *faces, restrict, jac, weights, diag)


def to_coarsest(r, faces, restrict, layers):
    e_total = r.shape[0]
    span = e_total // layers
    group = 4

    def body(r_in, h1, h2, g1, g2, rest_ref, out_ref, r_done, kept, sem):
        add_halo(NC, e_total, span, lambda e: r_in[e], r_done, h1, h2, g1, g2)

        def some(i, carry):
            first = i * group
            wide = jnp.concatenate([r_done[first + j] for j in range(group)], axis=1)
            product = times(rest_ref[...], wide)
            for j in range(group):
                kept[first + j] = product[:LAST, j * LANES : (j + 1) * LANES]
            return carry

        lax.fori_loop(0, e_total // group, some, 0, unroll=8)
        stores = []
        for e in range(e_total):
            c = pltpu.make_async_copy(kept.at[e], out_ref.at[:, e, :], sem)
            c.start()
            stores.append(c)
        for c in stores:
            c.wait()

    whole = pl.BlockSpec()
    return pl.pallas_call(
        body,
        out_shape=jax.ShapeDtypeStruct((LAST, e_total, LANES), F32),
        in_specs=[whole] * 6,
        out_specs=any_spec(),
        scratch_shapes=[
            pltpu.VMEM(r.shape, F32),
            pltpu.VMEM((e_total, LAST, LANES), F32),
            pltpu.SemaphoreType.DMA,
        ],
        compiler_params=params(),
        cost_estimate=cost(5 * 10**7, 10**6),
        name="to_coarsest",
    )(r, *faces, restrict)


def move(x, axis, by):
    count = lax.axis_size(axis)
    return lax.ppermute(x, axis, [(i, (i + by) % count) for i in range(count)])


def swap(x, axis, odd_first):
    count = lax.axis_size(axis)
    pairs = []
    for i in range(count):
        ahead = (i % 2 == 0) != odd_first
        pairs.append((i, (i + 1) % count if ahead else (i - 1) % count))
    return lax.ppermute(x, axis, pairs)


def swap_inner(x, axis, other):
    count, beside = lax.axis_size(axis), lax.axis_size(other)
    pairs = []
    for j in range(beside):
        for i in range(count):
            to = i + 1 if i % 2 else i - 1
            target = (j, to) if 0 <= to < count else (j ^ 1, i)
            pairs.append((j * count + i, target[0] * count + target[1]))
    return lax.ppermute(x, (other, axis), pairs)


def exchange(faces):
    c1, c2, z1, z2 = faces
    c2 = swap(c2, "sector", True)
    z2 = swap_inner(z2, "block", "sector")
    z1 = swap(z1, "block", False)
    c1 = swap(c1, "sector", False)
    return c1, c2, z1, z2


def windows(pair, offsets, own):
    span = pair.shape[0] // 2
    buckets = span // STEP
    _, steps = turn_plan(offsets[0], span)

    def branch(number):
        by, bucket = number // buckets, number % buckets
        many, few = span - STEP * bucket, STEP * (bucket + 1)

        def run(pair, offsets, own):
            far, near, near_back, far_back = cut(pair, many, few)
            near = move(near, "sector", by)
            far = move(far, "sector", by + 1)
            near_back = move(near_back, "sector", -by)
            far_back = move(far_back, "sector", -by - 1)
            kept, w = own_part(offsets, pair, *own)
            return kept, w, join(far, near, near_back, far_back)

        return run

    branches = [branch(i) for i in range(lax.axis_size("sector") // 2 * buckets)]
    return lax.switch(lax.div(steps, STEP), branches, pair, offsets, own)


def per_device(
    source, jacobian, stiff_fine, stiff_coarse, restrict_fine, restrict_coarse, mortar_proj, rotor_trace,
    stator_trace, offsets,
):
    layers, span, axial = jacobian.shape
    e_total = layers * span
    source_rows = source.reshape(source.shape[0], e_total, axial)
    jac = jacobian.reshape(e_total, axial)
    rotor_rows = rotor_trace.reshape(-1, span, axial)
    stator_rows = stator_trace.reshape(-1, span, axial)
    pair, near1, near2, proj, back, wf, wc, rfs, rcs, df, dc = prepare(
        offsets, rotor_rows, stator_rows, mortar_proj.transpose(1, 0, 2),
        stiff_fine, stiff_coarse, restrict_fine, restrict_coarse,
    )
    near2 = swap(near2, "sector", True)
    near1 = swap(near1, "sector", False)
    kept, w, wins = windows(pair, offsets, (proj, jac, df))
    sflux, rflux, r, p, *faces = first_sweep(
        offsets, wins, pair, kept, near1, near2, proj, back, source_rows, w, jac, wf, layers
    )
    p, r, *faces = sweep(NF, r, p, w, jac, wf, exchange(faces), layers, False)
    fine, r, *faces = sweep(NF, r, p, w, jac, wf, exchange(faces), layers, True)
    r, p, w, *faces = to_coarse(r, exchange(faces), rfs, jac, wc, dc, layers)
    p, r, *faces = sweep(NC, r, p, w, jac, wc, exchange(faces), layers, False)
    coarse, r, *faces = sweep(NC, r, p, w, jac, wc, exchange(faces), layers, True)
    coarsest = to_coarsest(r, exchange(faces), rcs, layers)
    shape = (layers, span, axial)
    return (
        sflux.reshape(stator_trace.shape),
        rflux.reshape(rotor_trace.shape),
        fine.reshape((-1,) + shape),
        coarse.reshape((-1,) + shape),
        coarsest.reshape((-1,) + shape),
    )


def solution(mesh):
    cell = P(None, None, "sector", "block")

    return jax.shard_map(
        per_device,
        mesh=mesh,
        in_specs=(cell, P(None, "sector", "block"), P(), P(), P(), P(), P(), cell, cell, P("block")),
        out_specs=(cell,) * 5,
        check_vma=False,
    )
```

```python
import jax
import jax.numpy as jnp
from jax import lax
from jax.experimental import pallas as pl
from jax.experimental.pallas import tpu as pltpu
from jax.sharding import PartitionSpec as P


F32 = jnp.float32
BF16 = jnp.bfloat16
DAMPING = 0.6
PENALTY = 0.5
LANES = 128
NF = 5
NC = 3
LAST = 8
STEP = 2
HALO_UNROLL = 32
GROUP = {NF: 4, NC: 16}
GROUP_UNROLL = {NF: 8, NC: 2}
VMEM_BYTES = 14 * 1024 * 1024


def up(value, unit):
    return (value + unit - 1) // unit * unit


def any_spec():
    return pl.BlockSpec(memory_space=pl.ANY)


def hbm_spec():
    return pl.BlockSpec(memory_space=pltpu.HBM)


def in_hbm(*arrays):
    return tuple(pltpu.with_memory_space_constraint(x, pltpu.HBM) for x in arrays)


def params(**extra):
    return pltpu.CompilerParams(vmem_limit_bytes=VMEM_BYTES, **extra)


def cost(flops, data):
    return pl.CostEstimate(flops=flops, bytes_accessed=data, transcendentals=0)


def parts_of(x):
    high = x.astype(BF16)
    low = (x - high.astype(F32)).astype(BF16)
    return high, low


def stacked(matrix):
    high, low = parts_of(matrix)
    top = jnp.concatenate([high, high], axis=1)
    bottom = jnp.concatenate([low, jnp.zeros_like(low)], axis=1)
    return jnp.concatenate([top, bottom], axis=0)


def times(weights, x):
    rows = weights.shape[0] // 2
    high, low = parts_of(x)
    both = jnp.dot(weights, jnp.concatenate([high, low], axis=0), preferred_element_type=F32)
    return both[:rows] + both[rows:]


def lane_ids(rows):
    return lax.broadcasted_iota(jnp.int32, (rows, LANES), 1)


def node_rows(shape, axis):
    return lax.broadcasted_iota(jnp.int32, shape, axis)


def digit(index, unit, most):
    found = jnp.zeros_like(index)
    for k in range(1, most + 1):
        found += jnp.where(index >= k * unit, 1, 0)
    return found


def half_faces(n, height):
    row = node_rows((height, LANES), 0)
    a = digit(row, n * n, n)
    b = digit(row - n * n * a, n, n - 1)
    on_a = jnp.where((a == 0) | (a == n - 1), PENALTY, 0.0)
    on_b = jnp.where((b == 0) | (b == n - 1), PENALTY, 0.0)
    return jnp.where(row < n**3, on_a + on_b, 0.0)


def turn_plan(offset, span):
    total = span * lax.axis_size("sector")
    flipped = jnp.where(offset >= total // 2, 1, 0)
    return flipped, jnp.where(flipped == 1, total - 1 - offset, offset)


def smem_spec():
    return pl.BlockSpec(memory_space=pltpu.SMEM)


def add_halo(n, e_total, span, source_of, r_ref, c1, c2, z1, z2):
    nn = n * n
    odd = lax.rem(lax.axis_index("sector"), 2) == 1
    block = lax.axis_index("block")
    z_odd = lax.rem(block, 2) == 1
    lowest = block == 0
    highest = block == lax.axis_size("block") - 1
    lanes = lane_ids(8)

    def slab(e, carry):
        r_ref[e] = source_of(e)
        for a in range(n):
            first, second = z1[a], z2[a]
            below = jnp.where(z_odd, first, second)
            above = jnp.where(z_odd, second, first)
            below = pltpu.roll(below, lax.rem(LANES - e, LANES), 1)
            above = pltpu.roll(above, LANES - 1 - e, 1)
            below = jnp.where((lanes == 0) & jnp.logical_not(lowest), PENALTY * below, 0.0)
            above = jnp.where((lanes == LANES - 1) & jnp.logical_not(highest), PENALTY * above, 0.0)
            r_ref[e, pl.ds(a * nn, n), :] += below[:n]
            r_ref[e, pl.ds(a * nn + nn - n, n), :] += above[:n]
        return carry

    lax.fori_loop(0, e_total, slab, 0, unroll=HALO_UNROLL)
    for layer in range(e_total // span):
        first, second = c1[layer], c2[layer]
        r_ref[layer * span, pl.ds(0, nn), :] += PENALTY * jnp.where(odd, first, second)
        r_ref[layer * span + span - 1, pl.ds((n - 1) * nn, nn), :] += PENALTY * jnp.where(odd, second, first)


def correct(n, e_total, span, r_ref, u_ref, u_of, c1, c2, z1, z2):
    nn = n * n
    lanes = lane_ids(8)

    def slab(e, carry):
        lows, highs = carry
        u_ref[e] = u_of(e, r_ref[e])
        new_lows, new_highs = [], []
        for a in range(n):
            low = u_ref[e, pl.ds(a * nn, 8), :]
            high = u_ref[e, pl.ds(a * nn + nn - n, 8), :]
            here = lanes == e
            new_lows.append(jnp.where(here, pltpu.roll(low, e, 1), lows[a]))
            new_highs.append(jnp.where(here, pltpu.roll(high, e + 1, 1), highs[a]))
        return tuple(new_lows), tuple(new_highs)

    blank = tuple(jnp.zeros((8, LANES), F32) for _ in range(n))
    lows, highs = lax.fori_loop(0, e_total, slab, (blank, blank), unroll=HALO_UNROLL)
    odd = lax.rem(lax.axis_index("sector"), 2) == 1
    z_odd = lax.rem(lax.axis_index("block"), 2) == 1
    for a in range(n):
        z1[a] = jnp.where(z_odd, lows[a], highs[a])
        z2[a] = jnp.where(z_odd, highs[a], lows[a])
    for layer in range(e_total // span):
        low = u_ref[layer * span, pl.ds(0, nn), :]
        high = u_ref[layer * span + span - 1, pl.ds((n - 1) * nn, nn), :]
        c1[layer] = jnp.where(odd, low, high)
        c2[layer] = jnp.where(odd, high, low)


def subtract_operator(n, e_total, span, r_ref, u_ref, weights, jac_ref, count_ref):
    nn = n * n
    group = GROUP[n]
    lanes = lane_ids(8)

    def some(i, carry):
        first = i * group
        wide = jnp.concatenate([u_ref[first + j] for j in range(group)], axis=1)
        product = times(weights[...], wide)
        for j in range(group):
            e = first + j
            own = product[:, j * LANES : (j + 1) * LANES]
            r_ref[e] = r_ref[e] - jac_ref[pl.ds(e, 1), :] * own - count_ref[...] * u_ref[e]
            s = lax.rem(e, span)
            before = jnp.where(s > 0, PENALTY, 0.0)
            after = jnp.where(s < span - 1, PENALTY, 0.0)
            previous = u_ref[jnp.maximum(e - 1, 0), pl.ds((n - 1) * nn, nn), :]
            following = u_ref[jnp.minimum(e + 1, e_total - 1), pl.ds(0, nn), :]
            r_ref[e, pl.ds(0, nn), :] += before * previous
            r_ref[e, pl.ds((n - 1) * nn, nn), :] += after * following
            for a in range(n):
                low = u_ref[e, pl.ds(a * nn, 8), :]
                high = u_ref[e, pl.ds(a * nn + nn - n, 8), :]
                from_below = jnp.where(lanes > 0, PENALTY * pltpu.roll(high, 1, 1), 0.0)
                from_above = jnp.where(lanes < LANES - 1, PENALTY * pltpu.roll(low, LANES - 1, 1), 0.0)
                r_ref[e, pl.ds(a * nn, n), :] += from_below[:n]
                r_ref[e, pl.ds(a * nn + nn - n, n), :] += from_above[:n]
        return carry

    lax.fori_loop(0, e_total // group, some, 0, unroll=GROUP_UNROLL[n])


def face_shapes(n, layers):
    circ = jax.ShapeDtypeStruct((layers, n * n, LANES), F32)
    axial = jax.ShapeDtypeStruct((n, 8, LANES), F32)
    return [circ, circ, axial, axial]


def prepare(offsets, rotor, stator, mortar, stiff_fine, stiff_coarse, restrict_fine, restrict_coarse):
    rows, span = rotor.shape[0], rotor.shape[1]
    tall, wide = up(rows, 8), up(rows, 16)
    big, small = up(NF**3, 16), up(NC**3, 16)
    smalls = (mortar, stiff_fine, stiff_coarse, restrict_fine, restrict_coarse)

    def body(
        offset_ref, rotor_ref, stator_ref, mortar_in, kf_in, kc_in, rf_in, rc_in,
        pair_out, near1_out, near2_out, proj_out, back_out, wf_out, wc_out, rfs_out, rcs_out, df_out, dc_out,
        mortar_ref, kf_ref, kc_ref, rf_ref, rc_ref, pad_ref, sem, small_sem,
    ):
        flipped, _ = turn_plan(offset_ref[0], span)
        copies = []
        for f in range(span):
            for source, first in ((rotor_ref, span * flipped), (stator_ref, span - span * flipped)):
                if tall > rows:
                    pair_out[first + f, pl.ds(rows, tall - rows), :] = jnp.zeros((tall - rows, LANES), F32)
                copies.append(
                    pltpu.make_async_copy(source.at[:, f, :], pair_out.at[first + f, pl.ds(0, rows), :], sem)
                )
        little = [
            pltpu.make_async_copy(source, target, small_sem)
            for source, target in (
                (mortar_in, mortar_ref), (kf_in, kf_ref), (kc_in, kc_ref), (rf_in, rf_ref), (rc_in, rc_ref)
            )
        ]
        for c in little + copies:
            c.start()
        row, col = node_rows((tall, LANES), 0), node_rows((tall, LANES), 1)
        comp_r, comp_c = digit(row, NF * NF, 4), digit(col, NF * NF, 5)
        rest_r, rest_c = row - NF * NF * comp_r, col - NF * NF * comp_c
        a_r, a_c = digit(rest_r, NF, NF - 1), digit(rest_c, NF, NF - 1)
        same = (comp_r == comp_c) & (rest_r - NF * a_r == rest_c - NF * a_c) & (row < rows) & (col < rows)
        ahead = jnp.where(same, a_r * NF + a_c, -1)
        turned = jnp.where(same, a_c * NF + a_r, -1)
        for c in little:
            c.wait()

        def both_terms(pair):
            highs, lows = zip(*[parts_of(m) for m in pair])
            return jnp.concatenate(
                [jnp.concatenate([h, h], axis=1) for h in highs]
                + [jnp.concatenate([l, jnp.zeros_like(l)], axis=1) for l in lows],
                axis=0,
            )

        for found, out in ((ahead, proj_out), (turned, back_out)):
            pair = []
            for which in range(2):
                total = jnp.zeros((tall, LANES), F32)
                matrix = mortar_ref[:, which, :]
                for i in range(NF):
                    for j in range(NF):
                        total = jnp.where(found == i * NF + j, matrix[i : i + 1, j : j + 1], total)
                pair.append(total)
            out[...] = both_terms([m[:, :wide] for m in pair])

        def padded(ref, height, width):
            pad_ref[...] = jnp.zeros_like(pad_ref)
            pad_ref[pl.ds(0, ref.shape[0]), pl.ds(0, ref.shape[1])] = ref[...]
            return pad_ref[pl.ds(0, height), :][:, :width]

        for ref, out, diag_out, size in ((kf_ref, wf_out, df_out, big), (kc_ref, wc_out, dc_out, small)):
            matrix = padded(ref, size, size)
            out[...] = stacked(matrix)
            row = lax.broadcasted_iota(jnp.int32, (size, size), 0)
            col = lax.broadcasted_iota(jnp.int32, (size, size), 1)
            diag = jnp.sum(jnp.where(row == col, matrix, 0.0), axis=1, keepdims=True)
            diag = jnp.where(row[:, :1] < ref.shape[0], diag, 1.0)
            diag_out[...] = jnp.broadcast_to(diag, (size, LANES))
        rfs_out[...] = stacked(padded(rf_ref, small, big))
        rcs_out[...] = stacked(padded(rc_ref, 16, small))
        for c in copies:
            c.wait()
        odd = lax.rem(lax.axis_index("sector"), 2) == 1
        lowest, highest = pair_out[span * flipped], pair_out[span * flipped + span - 1]
        near1_out[0] = jnp.where(odd, lowest, highest)
        near2_out[0] = jnp.where(odd, highest, lowest)

    return pl.pallas_call(
        body,
        out_shape=[
            pltpu.VMEM((2 * span, tall, LANES), F32),
            jax.ShapeDtypeStruct((1, tall, LANES), F32),
            jax.ShapeDtypeStruct((1, tall, LANES), F32),
            jax.ShapeDtypeStruct((4 * tall, 2 * wide), BF16),
            jax.ShapeDtypeStruct((4 * tall, 2 * wide), BF16),
            jax.ShapeDtypeStruct((2 * big, 2 * big), BF16),
            jax.ShapeDtypeStruct((2 * small, 2 * small), BF16),
            jax.ShapeDtypeStruct((2 * small, 2 * big), BF16),
            jax.ShapeDtypeStruct((32, 2 * small), BF16),
            jax.ShapeDtypeStruct((big, LANES), F32),
            jax.ShapeDtypeStruct((small, LANES), F32),
        ],
        in_specs=[smem_spec()] + [hbm_spec()] * 7,
        scratch_shapes=[pltpu.VMEM(m.shape, F32) for m in smalls]
        + [pltpu.VMEM((big, LANES), F32), pltpu.SemaphoreType.DMA, pltpu.SemaphoreType.DMA],
        compiler_params=params(),
        name="prepare",
    )(offsets, *in_hbm(rotor, stator, *smalls))


def apply_faces(matrix_ref, slab_of, count, tall, wide, y0, y1, unrolled):
    group = 4
    fill = jnp.zeros((wide - tall, group * LANES), F32)

    def some(i, carry):
        first = group * i
        least = min if unrolled else jnp.minimum
        x = jnp.concatenate([slab_of(least(first + j, count - 1)) for j in range(group)], axis=1)
        if wide > tall:
            x = jnp.concatenate([x, fill], axis=0)
        high, low = parts_of(x)
        y = jnp.dot(matrix_ref[...], jnp.concatenate([high, low], axis=0), preferred_element_type=F32)
        a = y[:tall] + y[2 * tall : 3 * tall]
        b = y[tall : 2 * tall] + y[3 * tall :]
        for j in range(group):
            y0[first + j] = a[:, j * LANES : (j + 1) * LANES]
            y1[first + j] = b[:, j * LANES : (j + 1) * LANES]
        return carry

    if unrolled:
        for i in range(up(count, group) // group):
            some(i, 0)
    else:
        lax.fori_loop(0, up(count, group) // group, some, 0)


def own_part(offsets, pair, proj, jac, diag):
    span, tall = pair.shape[0] // 2, pair.shape[1]
    wide = proj.shape[1] // 2
    e_total, height = jac.shape[0], diag.shape[0]

    def body(offset_ref, pair_ref, proj_ref, jac_ref, diag_ref, kept, w_ref, y0, y1):
        first = span * turn_plan(offset_ref[0], span)[0]
        apply_faces(proj_ref, lambda f: pair_ref[first + f], span, tall, wide, y0, y1, False)
        kept[0] = y0[0]
        kept[span] = y1[span - 1]

        def face(g, carry):
            kept[g] = y0[g] + y1[g - 1]
            return carry

        lax.fori_loop(1, span, face, 0)
        count = half_faces(NF, height)

        def weight(e, carry):
            w_ref[e] = DAMPING / (jac_ref[pl.ds(e, 1), :] * diag_ref[...] + count)
            return carry

        lax.fori_loop(0, e_total, weight, 0)

    return pl.pallas_call(
        body,
        out_shape=[
            jax.ShapeDtypeStruct((span + 1, tall, LANES), F32),
            jax.ShapeDtypeStruct((e_total, height, LANES), F32),
        ],
        in_specs=[smem_spec()] + [pl.BlockSpec()] * 4,
        scratch_shapes=[pltpu.VMEM((up(span, 4), tall, LANES), F32)] * 2,
        compiler_params=params(),
        cost_estimate=cost(2 * 10**9, 10 * 10**6),
        name="own_part",
    )(offsets, pair, proj, jac, diag)


def cut(pair, many, few, rows):
    span = pair.shape[0] // 2

    def body(pair_ref, far, near, near_back, far_back):
        def copy(first, out):
            def two(i, carry):
                for j in range(2):
                    out[i, pl.ds(j * rows, rows), :] = pair_ref[first + 2 * i + j, pl.ds(0, rows), :]
                return carry

            lax.fori_loop(0, out.shape[0], two, 0)

        copy(span - few, far)
        copy(0, near)
        copy(2 * span - many, near_back)
        copy(span, far_back)

    piece = [pltpu.VMEM((count // 2, 2 * rows, LANES), F32) for count in (few, many, many, few)]
    return pl.pallas_call(body, out_shape=piece, compiler_params=params(), name="cut")(pair)


def join(*pieces):
    def body(far_ref, near_ref, near_back_ref, far_back_ref, out, sem):
        first = 0
        copies = []
        for piece in (far_ref, near_ref, near_back_ref, far_back_ref):
            count = piece.shape[0]
            copies.append(pltpu.make_async_copy(piece, out.at[pl.ds(first, count)], sem))
            first += count
        for c in copies:
            c.start()
        for c in copies:
            c.wait()

    return pl.pallas_call(
        body,
        out_shape=pltpu.HBM((sum(p.shape[0] for p in pieces),) + pieces[0].shape[1:], F32),
        out_specs=hbm_spec(),
        scratch_shapes=[pltpu.SemaphoreType.DMA],
        compiler_params=params(),
        name="join",
    )(*pieces)


def first_sweep(offsets, wins, pair, kept, near1, near2, proj, back, source, w, jac, weights, layers):
    span, tall = pair.shape[0] // 2, pair.shape[1]
    wide = back.shape[1] // 2
    rows = 4 * NF * NF
    reach = wins.shape[0] // (2 * rows)
    e_total = jac.shape[0]
    n, nn = NF, NF * NF
    nodes = n**3
    height = weights.shape[0] // 2

    def body(
        offset_ref, wins_in, pair_ref, kept_ref, near1_ref, near2_ref, proj_ref, back_ref, source_ref, w_in,
        jac_ref, w_mat, sflux_out, rflux_out, r_ref, u_ref, c1, c2, z1, z2,
        y0, y1, x0, x1, sflux, rflux, count_ref, wins_ref, w_ref, in_sem, out_sem, win_sems,
    ):
        loads = [
            pltpu.make_async_copy(source_ref.at[:, e, :], r_ref.at[e, pl.ds(0, nodes), :], in_sem)
            for e in range(e_total)
        ]
        flipped, steps = turn_plan(offset_ref[0], span)
        inner = lax.rem(steps, STEP)
        rotor_half = reach * flipped
        halves = []
        for k, first in enumerate((rotor_half, reach - rotor_half)):
            half = []
            for f in range(reach):
                if tall > rows:
                    wins_ref[first + f, pl.ds(rows, tall - rows), :] = jnp.zeros((tall - rows, LANES), F32)
                half.append(
                    pltpu.make_async_copy(
                        wins_in.at[pl.ds(rows * (first + f), rows), 0, :],
                        wins_ref.at[first + f, pl.ds(0, rows), :],
                        win_sems.at[k],
                    )
                )
            halves.append(half)
        loads.append(pltpu.make_async_copy(w_in, w_ref, win_sems.at[2]))
        for c in halves[0] + halves[1] + loads:
            c.start()
        ahead, behind = STEP - 1 - inner, reach + inner
        first_rotor = jnp.where(flipped == 1, behind, ahead)
        first_stator = jnp.where(flipped == 1, ahead, behind)
        own_stator = span - span * flipped
        count_ref[...] = half_faces(n, height)
        odd = lax.rem(lax.axis_index("sector"), 2) == 1

        def rotor_slab(f):
            if f <= span:
                return wins_ref[first_rotor + f]
            one, two = near1_ref[0], near2_ref[0]
            return jnp.where(odd, one, two) if f == span + 1 else jnp.where(odd, two, one)

        def jump(f):
            own = kept_ref[f]
            if f == 0:
                own = own + x1[span + 1]
            if f == span:
                own = own + x0[span + 2]
            return wins_ref[first_stator + f] - own

        for c in halves[0]:
            c.wait()
        apply_faces(proj_ref, rotor_slab, span + 3, tall, wide, x0, x1, True)
        for c in halves[1]:
            c.wait()
        apply_faces(back_ref, jump, span + 1, tall, wide, y0, y1, True)
        stores = []
        for s in range(span):
            sflux[s] = pair_ref[own_stator + s] - (x0[s + 1] + x1[s])
            rflux[s] = y0[s] + y1[s + 1]
            for buffer, out in ((sflux, sflux_out), (rflux, rflux_out)):
                c = pltpu.make_async_copy(buffer.at[s, pl.ds(0, rows), :], out.at[:, s, :], out_sem)
                c.start()
                stores.append(c)
        for c in loads:
            c.wait()
        for s in range(span):
            if height > nodes:
                for layer in range(layers):
                    r_ref[layer * span + s, pl.ds(nodes, height - nodes), :] = jnp.zeros((height - nodes, LANES), F32)
            inflow = sflux[s, pl.ds(0, nn), :] + sflux[s, pl.ds(3 * nn, nn), :]
            outflow = rflux[s, pl.ds(0, nn), :] + rflux[s, pl.ds(3 * nn, nn), :]
            r_ref[span + s, pl.ds(0, nn, stride=n), :] += inflow
            r_ref[s, pl.ds(n - 1, nn, stride=n), :] += -outflow
        correct(n, e_total, span, r_ref, u_ref, lambda e, r: r * w_ref[e], c1, c2, z1, z2)
        subtract_operator(n, e_total, span, r_ref, u_ref, w_mat, jac_ref, count_ref)
        for c in stores:
            c.wait()

    whole = pl.BlockSpec()
    field = jax.ShapeDtypeStruct((e_total, height, LANES), F32)
    trace = jax.ShapeDtypeStruct((rows, span, LANES), F32)
    slabs = pltpu.VMEM((up(span + 3, 4), tall, LANES), F32)
    return pl.pallas_call(
        body,
        out_shape=[trace, trace, field, field] + face_shapes(n, layers),
        in_specs=[smem_spec(), hbm_spec()] + [whole] * 6 + [hbm_spec()] * 2 + [whole] * 2,
        out_specs=[hbm_spec()] * 2 + [whole] * 6,
        scratch_shapes=[slabs] * 4
        + [
            pltpu.VMEM((span, tall, LANES), F32),
            pltpu.VMEM((span, tall, LANES), F32),
            pltpu.VMEM((height, LANES), F32),
            pltpu.VMEM((2 * reach, tall, LANES), F32),
            pltpu.VMEM(w.shape, F32),
            pltpu.SemaphoreType.DMA,
            pltpu.SemaphoreType.DMA,
            pltpu.SemaphoreType.DMA((3,)),
        ],
        compiler_params=params(),
        cost_estimate=cost(2 * 10**9, 20 * 10**6),
        name="first_sweep",
    )(offsets, *in_hbm(wins), pair, kept, near1, near2, proj, back, *in_hbm(source, w), jac, weights)


def sweep(n, r, p, w, jac, weights, faces, layers, last):
    e_total, height = r.shape[0], r.shape[1]
    span = e_total // layers
    nodes = n**3

    def body(r_in, p_in, w_in, jac_ref, w_mat, h1, h2, g1, g2, p_out, r_ref, c1, c2, z1, z2, u_ref, p_keep, count_ref, sem):
        count_ref[...] = half_faces(n, height)
        p_ref = p_keep if last else p_out
        add_halo(n, e_total, span, lambda e: r_in[e], r_ref, h1, h2, g1, g2)

        def u_of(e, r_here):
            u = r_here * w_in[e]
            p_ref[e] = p_in[e] + u
            return u

        correct(n, e_total, span, r_ref, u_ref, u_of, c1, c2, z1, z2)
        stores = []
        if last:
            for e in range(e_total):
                c = pltpu.make_async_copy(p_ref.at[e, pl.ds(0, nodes), :], p_out.at[:, e, :], sem)
                c.start()
                stores.append(c)
        subtract_operator(n, e_total, span, r_ref, u_ref, w_mat, jac_ref, count_ref)
        for c in stores:
            c.wait()

    whole = pl.BlockSpec()
    field = jax.ShapeDtypeStruct((e_total, height, LANES), F32)
    kept = jax.ShapeDtypeStruct((nodes, e_total, LANES), F32) if last else field
    return pl.pallas_call(
        body,
        out_shape=[kept, field] + face_shapes(n, layers),
        out_specs=[any_spec() if last else whole] + [whole] * 5,
        scratch_shapes=[
            pltpu.VMEM((e_total, height, LANES), F32),
            pltpu.VMEM((e_total, height, LANES) if last else (1, 8, LANES), F32),
            pltpu.VMEM((height, LANES), F32),
            pltpu.SemaphoreType.DMA,
        ],
        compiler_params=params(),
        cost_estimate=cost(10**9 if n == NF else 10**8, 10 * 10**6),
    )(r, p, w, jac, weights, *faces)


def to_coarse(r, faces, restrict, jac, weights, diag, layers):
    e_total = r.shape[0]
    span = e_total // layers
    small = weights.shape[0] // 2
    n = NC
    group = 4

    def body(r_in, h1, h2, g1, g2, rest_ref, jac_ref, w_mat, diag_ref, rc_ref, u_ref, w_ref, c1, c2, z1, z2, r_fine, count_ref):
        count_ref[...] = half_faces(n, small)
        add_halo(NF, e_total, span, lambda e: r_in[e], r_fine, h1, h2, g1, g2)

        def some(i, carry):
            first = i * group
            wide = jnp.concatenate([r_fine[first + j] for j in range(group)], axis=1)
            product = times(rest_ref[...], wide)
            for j in range(group):
                rc_ref[first + j] = product[:, j * LANES : (j + 1) * LANES]
            return carry

        lax.fori_loop(0, e_total // group, some, 0, unroll=2)

        def u_of(e, r_here):
            w_here = DAMPING / (jac_ref[pl.ds(e, 1), :] * diag_ref[...] + count_ref[...])
            w_ref[e] = w_here
            return r_here * w_here

        correct(n, e_total, span, rc_ref, u_ref, u_of, c1, c2, z1, z2)
        subtract_operator(n, e_total, span, rc_ref, u_ref, w_mat, jac_ref, count_ref)

    field = jax.ShapeDtypeStruct((e_total, small, LANES), F32)
    return pl.pallas_call(
        body,
        out_shape=[field, field, field] + face_shapes(n, layers),
        scratch_shapes=[pltpu.VMEM(r.shape, F32), pltpu.VMEM((small, LANES), F32)],
        compiler_params=params(),
        cost_estimate=cost(5 * 10**8, 5 * 10**6),
        name="to_coarse",
    )(r, *faces, restrict, jac, weights, diag)


def to_coarsest(r, faces, restrict, layers):
    e_total = r.shape[0]
    span = e_total // layers
    group = 4

    def body(r_in, h1, h2, g1, g2, rest_ref, out_ref, r_done, kept, sem):
        add_halo(NC, e_total, span, lambda e: r_in[e], r_done, h1, h2, g1, g2)

        def some(i, carry):
            first = i * group
            wide = jnp.concatenate([r_done[first + j] for j in range(group)], axis=1)
            product = times(rest_ref[...], wide)
            for j in range(group):
                kept[first + j] = product[:LAST, j * LANES : (j + 1) * LANES]
            return carry

        lax.fori_loop(0, e_total // group, some, 0, unroll=8)
        stores = []
        for e in range(e_total):
            c = pltpu.make_async_copy(kept.at[e], out_ref.at[:, e, :], sem)
            c.start()
            stores.append(c)
        for c in stores:
            c.wait()

    whole = pl.BlockSpec()
    return pl.pallas_call(
        body,
        out_shape=jax.ShapeDtypeStruct((LAST, e_total, LANES), F32),
        in_specs=[whole] * 6,
        out_specs=any_spec(),
        scratch_shapes=[
            pltpu.VMEM(r.shape, F32),
            pltpu.VMEM((e_total, LAST, LANES), F32),
            pltpu.SemaphoreType.DMA,
        ],
        compiler_params=params(),
        cost_estimate=cost(5 * 10**7, 10**6),
        name="to_coarsest",
    )(r, *faces, restrict)


def move(x, axis, by):
    count = lax.axis_size(axis)
    return lax.ppermute(x, axis, [(i, (i + by) % count) for i in range(count)])


def swap(x, axis, odd_first):
    count = lax.axis_size(axis)
    pairs = []
    for i in range(count):
        ahead = (i % 2 == 0) != odd_first
        pairs.append((i, (i + 1) % count if ahead else (i - 1) % count))
    return lax.ppermute(x, axis, pairs)


def swap_inner(x, axis, other):
    count, beside = lax.axis_size(axis), lax.axis_size(other)
    pairs = []
    for j in range(beside):
        for i in range(count):
            to = i + 1 if i % 2 else i - 1
            target = (j, to) if 0 <= to < count else (j ^ 1, i)
            pairs.append((j * count + i, target[0] * count + target[1]))
    return lax.ppermute(x, (other, axis), pairs)


def exchange(faces):
    c1, c2, z1, z2 = faces
    c2 = swap(c2, "sector", True)
    z2 = swap_inner(z2, "block", "sector")
    z1 = swap(z1, "block", False)
    c1 = swap(c1, "sector", False)
    return c1, c2, z1, z2


def windows(pair, offsets, own):
    span = pair.shape[0] // 2
    buckets = span // STEP
    _, steps = turn_plan(offsets[0], span)

    def branch(number):
        by, bucket = number // buckets, number % buckets
        many, few = span - STEP * bucket, STEP * (bucket + 1)

        def run(pair, offsets, own):
            far, near, near_back, far_back = cut(pair, many, few, 4 * NF * NF)
            near = move(near, "sector", by)
            far = move(far, "sector", by + 1)
            near_back = move(near_back, "sector", -by)
            far_back = move(far_back, "sector", -by - 1)
            kept, w = own_part(offsets, pair, *own)
            return kept, w, join(far, near, near_back, far_back)

        return run

    branches = [branch(i) for i in range(lax.axis_size("sector") // 2 * buckets)]
    return lax.switch(lax.div(steps, STEP), branches, pair, offsets, own)


def per_device(
    source, jacobian, stiff_fine, stiff_coarse, restrict_fine, restrict_coarse, mortar_proj, rotor_trace,
    stator_trace, offsets,
):
    layers, span, axial = jacobian.shape
    e_total = layers * span
    source_rows = source.reshape(source.shape[0], e_total, axial)
    jac = jacobian.reshape(e_total, axial)
    rotor_rows = rotor_trace.reshape(-1, span, axial)
    stator_rows = stator_trace.reshape(-1, span, axial)
    pair, near1, near2, proj, back, wf, wc, rfs, rcs, df, dc = prepare(
        offsets, rotor_rows, stator_rows, mortar_proj.transpose(1, 0, 2),
        stiff_fine, stiff_coarse, restrict_fine, restrict_coarse,
    )
    near2 = swap(near2, "sector", True)
    near1 = swap(near1, "sector", False)
    kept, w, wins = windows(pair, offsets, (proj, jac, df))
    wins = wins.reshape(-1, 1, wins.shape[-1])
    sflux, rflux, r, p, *faces = first_sweep(
        offsets, wins, pair, kept, near1, near2, proj, back, source_rows, w, jac, wf, layers
    )
    p, r, *faces = sweep(NF, r, p, w, jac, wf, exchange(faces), layers, False)
    fine, r, *faces = sweep(NF, r, p, w, jac, wf, exchange(faces), layers, True)
    r, p, w, *faces = to_coarse(r, exchange(faces), rfs, jac, wc, dc, layers)
    p, r, *faces = sweep(NC, r, p, w, jac, wc, exchange(faces), layers, False)
    coarse, r, *faces = sweep(NC, r, p, w, jac, wc, exchange(faces), layers, True)
    coarsest = to_coarsest(r, exchange(faces), rcs, layers)
    shape = (layers, span, axial)
    return (
        sflux.reshape(stator_trace.shape),
        rflux.reshape(rotor_trace.shape),
        fine.reshape((-1,) + shape),
        coarse.reshape((-1,) + shape),
        coarsest.reshape((-1,) + shape),
    )


def solution(mesh):
    cell = P(None, None, "sector", "block")

    return jax.shard_map(
        per_device,
        mesh=mesh,
        in_specs=(cell, P(None, "sector", "block"), P(), P(), P(), P(), P(), cell, cell, P("block")),
        out_specs=(cell,) * 5,
        check_vma=False,
    )
```
